1024 devices in a mesh: lat: 128 (over z, x, core), lon: 8 (over y).
Axes of the slice: x: 4, y: 8, z: 16, core: 2. Of those that a mesh axis runs over, the one named last changes fastest.
Arguments:
- courant: float32 [2, 16, 2048, 1024], P(None, None, 'lat', 'lon'), may hold values from -0.45 to 0.45
- obs_matrix: float32 [128, 64, 128, 128], P('lat', 'lon'), may hold values from -0.5 to 0.5
- obs_weight: float32 [128, 64, 128], P('lat', 'lon'), may hold values from 0.5 to 4
- innovation: float32 [128, 64, 128], P('lat', 'lon'), may hold values from -6 to 6
- block_owner: int32 [128, 64, 1], P('lat', 'lon'), may hold values from 0 to 7; in each aligned block of 8 rows (0 to 7, 8 to 15, ..., all dimensions but the last counted through in order) at most 2 rows name the same one
- block_row: int32 [128, 64], P('lat', 'lon'), may hold values from 0 to 255
- block_count: int32 [128, 8], P('lat', 'lon'), may hold values from 1 to 8, as said below
Outputs:
- increment: float32 [16, 2048, 1024], P(None, 'lat', 'lon')
- residual: float32 [16, 2048, 1024], P(None, 'lat', 'lon')
The draws below stay inside these ranges and needn't reach their ends.
Inputs may be any that keep to these rules, and one draw needn't show every extreme that they name: `block_owner`: among one device's 8 block slots no lon index is named more than 2 times, a bound that some block reaches. A device's first block_count slots are live, the rest are padding; some device has all 8 live.
All inputs are finite; a program needn't handle non-finite values.
Results may differ from the reference program's by a relative error of at most 0.0003.
Values sent between devices are 32-bit elements; how exact they have to be, the bound alone decides.
No kernel may reach another device: no remote copies, remote signals or barrier semaphores. Data moves between devices by JAX's collectives and lax.ppermute only.
A program may use at most 32 MiB of HBM per device.

```python
import math
import jax
import jax.numpy as jnp
import numpy as np
from jax import lax

LEVELS = 16
CLAT = 16
CLON = 128
OBS = 128
CAP = 8
SLOT = 2
STEPS = 4
ITERS = 2
NLAT = 2048
NLON = 1024
BLOCKS = 64
N_LAT = 128
N_LON = 8


def draw_block_count(key, part):
    first_key, second_key = jax.random.split(jax.random.fold_in(key, 11))
    counted = jax.random.randint(first_key, (N_LAT * N_LON,), 1, CAP + 1)
    chosen = jax.random.randint(second_key, (), 0, N_LAT * N_LON)
    counted = jnp.where(jnp.arange(N_LAT * N_LON) == chosen, CAP, counted)
    return counted.reshape(N_LAT, N_LON).astype(jnp.int32)


def place_ends(drawn, key, smallest, high):
    dims = drawn.shape
    place = [jax.random.randint(jax.random.fold_in(key, axis), (), 0, dims[axis]) for axis in range(len(dims))]
    drawn = drawn.at[tuple(place)].set(smallest)
    longest = dims.index(max(dims))
    place[longest] = (place[longest] + 1) % dims[longest]
    return drawn.at[tuple(place)].set(high)


def block_scale(own_key, dims, cuts, smallest, high):
    def one(position, blocks):
        draws = jax.random.uniform(jax.random.fold_in(jax.random.fold_in(own_key, 6), position), (blocks,), jnp.float32, smallest / len(cuts), high / len(cuts))
        return jnp.repeat(jnp.exp(draws), dims[position] // blocks).reshape((-1,) + (1,) * (len(dims) - position - 1))

    level = one(*cuts[0])
    for cut in cuts[1:]:
        level = level * one(*cut)
    return level


def routed_block(rng, own, number, rows, number_of, top, reach, slope):
    sequence = jax.random.permutation(rng, number_of)
    heavy_load, usual = portions_of(number_of, rows * top, reach, slope, True), portions_of(number_of, rows * top, reach, slope, False)
    places = jnp.arange(number_of)

    def named(lengths, offset_by):
        used = int((lengths > 0).sum())
        fixed = max(1, used // 4)
        moved = fixed + (places - fixed + offset_by * (used - fixed)) % max(1, number_of - fixed)
        return jnp.zeros((number_of,), jnp.int32).at[sequence[jnp.where(places < fixed, places, moved)]].set(jnp.asarray(lengths, jnp.int32))

    lengths = jnp.where(number % 4 == 0, named(heavy_load, number // 4), named(usual, number - number // 4 - 1))
    mixed = jax.random.permutation(jax.random.fold_in(own, 3), number_of)
    donor, sink = mixed[0:number_of // 2 * 2:2], mixed[1:number_of // 2 * 2:2]
    room = jnp.minimum(lengths[donor] - 1, reach - lengths[sink]) // 2
    room = jnp.where((donor == sequence[0]) | (sink == sequence[0]) | (lengths[sink] == 0), 0, jnp.maximum(room, 0))
    moved = jax.random.randint(jax.random.fold_in(own, 4), (number_of // 2,), 0, 1 << 20) % (room + 1)
    lengths = lengths.at[donor].add(-moved).at[sink].add(moved)
    items = jnp.searchsorted(jnp.cumsum(lengths), jnp.arange(rows * top), side="right").astype(jnp.int32)
    listing = items.reshape(top, rows).T
    listing = listing[jax.random.permutation(jax.random.fold_in(own, 1), rows)]
    offset_by = jax.random.randint(jax.random.fold_in(own, 2), (rows, 1), 0, top)
    return jnp.take_along_axis(listing, (jnp.arange(top)[None, :] + offset_by) % top, axis=1)


def portions_of(number_of, total, limit, slope, full):
    weights = [(1 << 20) // math.isqrt(rank ** slope) + 1 for rank in range(1, number_of + 1)]
    largest = limit if full else min(limit, max(-(-total // number_of), total * weights[0] // sum(weights)))
    least = 1 if total - largest >= number_of - 1 else 0
    given, spare = [largest] + [least] * (number_of - 1), total - largest - least * (number_of - 1)
    while spare > 0:
        movable = [i for i in range(1, number_of) if given[i] < largest] or [i for i in range(1, number_of) if given[i] < limit]
        pool, remaining = sum([weights[i] for i in movable]), spare
        for i in movable:
            addition = min(limit - given[i], max(1, remaining * weights[i] // pool), spare)
            given[i] = given[i] + addition
            spare = spare - addition
    return np.array(given)


def scatter_about(rng, extent, scale, limit, cuts=(), kind=jnp.bfloat16):
    level = block_scale(rng, extent, cuts, -0.22, 0.18) if cuts else 1.0
    array = jax.random.normal(rng, extent, jnp.float32) * scale * level
    return jnp.minimum(jnp.maximum(array, -limit), limit).astype(kind)


def setup_inputs(seed: int = 0) -> dict:
    splits = jax.random.split(jax.random.key(seed), 8)
    courant = jnp.clip(jax.random.uniform(splits[0], (2, LEVELS, NLAT, NLON), jnp.float32, -0.45, 0.45) * block_scale(splits[0], (2, LEVELS, NLAT, NLON), ((2, 128), (3, 8)), -0.4, 0.0), -0.45, 0.45)
    obs_matrix = scatter_about(splits[1], (N_LAT, BLOCKS, OBS, CLON), CLON ** -0.5, 0.5, ((0, 128), (1, 8)), jnp.float32)
    obs_weight = jnp.clip(jnp.exp(math.log(4.0) - 2.0794415 * jax.random.uniform(splits[2], (N_LAT, BLOCKS, OBS), jnp.float32) ** block_scale(splits[2], (N_LAT, BLOCKS, OBS), ((0, 128), (1, 8)), -0.2, 0.2)), 0.5, 4.0)
    innovation = scatter_about(splits[3], (N_LAT, BLOCKS, OBS), 1.0, 6.0, ((0, 128), (1, 8)), jnp.float32)
    block_owner_keys = jax.random.split(jax.random.fold_in(splits[4], 1), N_LAT * BLOCKS // CAP)
    block_owner_turns = jax.random.permutation(jax.random.fold_in(splits[4], 3), N_LAT * BLOCKS // CAP)
    block_owner = jax.vmap(lambda own, number: routed_block(jax.random.fold_in(splits[4], 2), own, number, CAP, N_LON, 1, SLOT, 2))(block_owner_keys, block_owner_turns).reshape((N_LAT, BLOCKS, 1))
    block_row = place_ends(jax.random.randint(splits[5], (N_LAT, BLOCKS), 0, LEVELS * CLAT), jax.random.fold_in(splits[5], 1), 0, (LEVELS * CLAT) - 1).astype(jnp.int32)
    block_count = draw_block_count(jax.random.fold_in(splits[7], 71), 0)
    return dict(courant=courant, obs_matrix=obs_matrix, obs_weight=obs_weight, innovation=innovation, block_owner=block_owner, block_row=block_row, block_count=block_count)


def from_south(grid_field):
    return jnp.pad(grid_field[:, :-1, :], ((0, 0), (1, 0), (0, 0)))


def from_north(grid_field):
    return jnp.pad(grid_field[:, 1:, :], ((0, 0), (0, 1), (0, 0)))


def tangent_step(grid_field, rate_parts, keep_self):
    return (keep_self * grid_field + rate_parts[0] * from_south(grid_field) + rate_parts[1] * from_north(grid_field)
            + rate_parts[2] * jnp.roll(grid_field, 1, axis=2) + rate_parts[3] * jnp.roll(grid_field, -1, axis=2))


def adjoint_step(grid_field, rate_parts, keep_self):
    return (keep_self * grid_field + from_north(rate_parts[0] * grid_field) + from_south(rate_parts[1] * grid_field)
            + jnp.roll(rate_parts[2] * grid_field, -1, axis=2) + jnp.roll(rate_parts[3] * grid_field, 1, axis=2))


def reference(courant, obs_matrix, obs_weight, innovation, block_owner, block_row, block_count):
    rate_parts = (jnp.maximum(courant[0], 0.0), jnp.maximum(-courant[0], 0.0),
                  jnp.maximum(courant[1], 0.0), jnp.maximum(-courant[1], 0.0))
    keep_self = 1.0 - rate_parts[0] - rate_parts[1] - rate_parts[2] - rate_parts[3]
    owner_lon = block_owner[:, :, 0]
    level_idx = block_row // CLAT
    lat_idx = jnp.arange(N_LAT, dtype=jnp.int32)[:, None] * CLAT + block_row % CLAT
    lon_idx = owner_lon[:, :, None] * CLON + jnp.arange(CLON, dtype=jnp.int32)[None, None, :]
    cell_index = ((level_idx * NLAT + lat_idx) * NLON)[:, :, None] + lon_idx
    slot_index = jnp.arange(BLOCKS, dtype=jnp.int32) % CAP
    live_mask = slot_index[None, :] < jnp.repeat(block_count, CAP, axis=1)
    weighted = jnp.where(live_mask[:, :, None], obs_weight, 0.0)

    def observe(grid_field):
        seen_rows = grid_field.reshape(-1)[cell_index]
        return jnp.einsum("ibok,ibk->ibo", obs_matrix, seen_rows, precision=lax.Precision.HIGHEST)

    def observe_adjoint(block_terms):
        spread = jnp.einsum("ibok,ibo->ibk", obs_matrix, block_terms, precision=lax.Precision.HIGHEST)
        flat_out = jnp.zeros((LEVELS * NLAT * NLON,), jnp.float32).at[cell_index].add(spread)
        return flat_out.reshape(LEVELS, NLAT, NLON)

    def model_adjoint(grid_field):
        for sweep in range(STEPS):
            grid_field = adjoint_step(grid_field, rate_parts, keep_self)
        return grid_field

    def hessian(vector):
        moved = vector
        for sweep in range(STEPS):
            moved = tangent_step(moved, rate_parts, keep_self)
        return vector + model_adjoint(observe_adjoint(weighted * observe(moved)))

    right_side = model_adjoint(observe_adjoint(weighted * innovation))
    increment = jnp.zeros_like(right_side)
    residual = right_side
    direction = right_side
    norm_now = jnp.sum(residual * residual)
    for sweep in range(ITERS):
        image_vec = hessian(direction)
        step_size = norm_now / jnp.sum(direction * image_vec)
        increment = increment + step_size * direction
        residual = residual - step_size * image_vec
        if sweep + 1 < ITERS:
            norm_next = jnp.sum(residual * residual)
            direction = residual + (norm_next / norm_now) * direction
            norm_now = norm_next
    return increment, residual
```

```python
import jax
import jax.numpy as jnp
from jax import lax
from jax.sharding import Mesh
from jax.sharding import PartitionSpec as P

SLOT = 2
STEPS = 4
HALO = 2 * STEPS
LAT = ("lat_0", "lat_1", "lat_2")
HIGHEST = lax.Precision.HIGHEST


def from_sides(cells, axis, dim, width, wrap):
    count = lax.axis_size(axis)
    head = lax.slice_in_dim(cells, 0, width, axis=dim)
    tail = lax.slice_in_dim(cells, cells.shape[dim] - width, cells.shape[dim], axis=dim)
    last = count if wrap else count - 1
    before = lax.ppermute(tail, axis, [(i, (i + 1) % count) for i in range(last)])
    after = lax.ppermute(head, axis, [((i + 1) % count, i) for i in range(last)])
    return jnp.concatenate([before, cells, after], axis=dim)


def exchanged(cells, lat_dim, width):
    cells = from_sides(cells, LAT, lat_dim, width, False)
    return from_sides(cells, "lon", lat_dim + 1, width, True)


def cut(a, width):
    return a[..., width:-width, width:-width] if width else a


def total(values):
    for axes in (("lat_1", "lon"), ("lat_0", "lat_2")):
        count = lax.axis_size(axes)
        spread = jnp.broadcast_to(values[None], (count,) + values.shape)
        values = jnp.sum(lax.all_to_all(spread, axes, split_axis=0, concat_axis=0, tiled=True), axis=0)
    return values


def shards(courant, obs_matrix, obs_weight, innovation, block_owner, block_row, block_count):
    levels, lat_rows, lon_cells = courant.shape[1:]
    capacity = block_row.shape[1]
    lon_count = lax.axis_size("lon")
    lat_index = lax.axis_index(LAT)
    lat_total = lax.axis_size(LAT)

    owner_lon = block_owner[0, :, 0]
    onehot = (owner_lon[:, None] == jnp.arange(lon_count, dtype=jnp.int32)[None, :]).astype(jnp.int32)
    before = jnp.cumsum(onehot, axis=0) - onehot
    target = owner_lon * SLOT + jnp.sum(before * onehot, axis=1)
    live = jnp.arange(capacity, dtype=jnp.int32) < block_count[0, 0]
    weighted = jnp.where(live[:, None], obs_weight[0], 0.0)
    matrix = obs_matrix[0]
    gram = jnp.einsum("bok,bol->bkl", weighted[:, :, None] * matrix, matrix, precision=HIGHEST)
    pulled = jnp.einsum("bok,bo->bk", matrix, weighted * innovation[0], precision=HIGHEST)
    named = jnp.broadcast_to(block_row[0].astype(jnp.float32)[:, None], (capacity, lon_cells))
    parcel = jnp.concatenate([gram, pulled[:, None], named[:, None]], axis=1)
    parcels = jnp.zeros((lon_count * SLOT,) + parcel.shape[1:], jnp.float32).at[target].set(parcel)
    arrived = lax.all_to_all(parcels, "lon", split_axis=0, concat_axis=0, tiled=True)
    gram, pulled, rows = arrived[:, :lon_cells], arrived[:, lon_cells], arrived[:, lon_cells + 1, 0].astype(jnp.int32)

    def spread(terms):
        flat = jnp.zeros((levels * lat_rows, lon_cells), jnp.float32).at[rows].add(terms)
        return flat.reshape(levels, lat_rows, lon_cells)

    def seen(field):
        return field.reshape(levels * lat_rows, lon_cells)[rows]

    def weigh(terms):
        return jnp.einsum("bkl,bl->bk", gram, terms, precision=HIGHEST)

    first = exchanged(jnp.concatenate([courant, spread(pulled)[None]], axis=0), 2, HALO)
    flow, departure = first[:2], first[2]
    rates = (jnp.maximum(flow[0], 0.0), jnp.maximum(-flow[0], 0.0), jnp.maximum(flow[1], 0.0), jnp.maximum(-flow[1], 0.0))
    keep = 1.0 - rates[0] - rates[1] - rates[2] - rates[3]

    def inside(field):
        margin = (field.shape[1] - lat_rows) // 2
        at = jnp.arange(field.shape[1], dtype=jnp.int32) + lat_index * lat_rows - margin
        return jnp.where(((at >= 0) & (at < lat_rows * lat_total))[:, None], field, 0.0)

    def adjoint(field, reach):
        for _ in range(STEPS):
            a, b, e, f = (cut(r, HALO - reach) * field for r in rates)
            field = (
                cut(keep, HALO - reach + 1) * field[:, 1:-1, 1:-1]
                + a[:, 2:, 1:-1] + b[:, :-2, 1:-1] + e[:, 1:-1, 2:] + f[:, 1:-1, :-2]
            )
            reach -= 1
        return field

    def tangent(field, reach):
        for _ in range(STEPS):
            reach -= 1
            a, b, e, f = (cut(r, HALO - reach) for r in rates)
            field = (
                cut(keep, HALO - reach) * field[:, 1:-1, 1:-1]
                + a * field[:, :-2, 1:-1] + b * field[:, 2:, 1:-1] + e * field[:, 1:-1, :-2] + f * field[:, 1:-1, 2:]
            )
        return field

    right_wide = inside(adjoint(departure, HALO))
    right = cut(right_wide, STEPS)
    seen_1 = seen(tangent(right_wide, STEPS))
    terms_1 = weigh(seen_1)
    image_wide = right_wide + inside(adjoint(exchanged(spread(terms_1), 1, HALO), HALO))
    image = cut(image_wide, STEPS)
    seen_2 = seen(tangent(image_wide, STEPS))
    terms_2 = weigh(seen_2)
    sums = total(jnp.stack([jnp.sum(right * right), jnp.sum(seen_1 * terms_1), jnp.sum(image * image), jnp.sum(seen_2 * terms_2)]))
    second = image + adjoint(exchanged(spread(terms_2), 1, STEPS), STEPS)

    bb, b_ab, ab_ab, ab_aab = sums[0], sums[0] + sums[1], sums[2], sums[2] + sums[3]
    step_0 = bb / b_ab
    norm_1 = bb - 2.0 * step_0 * b_ab + step_0 * step_0 * ab_ab
    beta = norm_1 / bb
    curve = b_ab - 2.0 * step_0 * ab_ab + step_0 * step_0 * ab_aab - beta * beta * b_ab
    step_1 = norm_1 / curve
    main = step_0 + step_1 * (1.0 + beta)
    cross = step_0 * step_1
    return main * right - cross * image, right - main * image + cross * second


def solution(mesh):
    torus = Mesh(
        mesh.devices.reshape(16, 4, 2, mesh.shape["lon"]), ("lat_0", "lat_1", "lat_2", "lon")
    )
    placed = (
        P(None, None, LAT, "lon"),
        P(LAT, "lon", None, None),
        P(LAT, "lon", None),
        P(LAT, "lon", None),
        P(LAT, "lon", None),
        P(LAT, "lon"),
        P(LAT, "lon"),
    )
    return jax.shard_map(
        shards,
        mesh=torus,
        in_specs=placed,
        out_specs=(P(None, LAT, "lon"), P(None, LAT, "lon")),
        check_vma=False,
    )
```

```python
import functools

import jax
import jax.numpy as jnp
from jax import lax
from jax.experimental import pallas as pl
from jax.experimental.pallas import tpu as pltpu
from jax.sharding import Mesh
from jax.sharding import PartitionSpec as P

LAT = ("lat_0", "lat_1", "lat_2")
LEVELS = 16
ROWS = 16
LANES = 128
CAP = 8
SLOT = 2
STEPS = 4
HALO = 2 * STEPS
WIDE = ROWS + 2 * HALO
LON = 8
HALF = LANES // 2
OWN = LON * SLOT
NEAR = 3 * OWN
BULK = 2 * HALF + 8
LIST = 24
SMALL = LIST + 64
NOWHERE = -4096.0
HIGHEST = lax.Precision.HIGHEST
F32 = jnp.float32
VMEM = pl.BlockSpec(memory_space=pltpu.VMEM)
SMEM = pl.BlockSpec(memory_space=pltpu.SMEM)


def lanes(rows):
    return lax.broadcasted_iota(jnp.int32, (rows, LANES), 1)


def places(rows):
    return lax.broadcasted_iota(jnp.int32, (rows, LANES), 0)


def roll(x, shift):
    shift %= LANES
    return pltpu.roll(x, shift, axis=1) if shift else x


def call(body, outs, args, flops, scratch=()):
    outs = [jax.ShapeDtypeStruct(s, F32) for s in outs]
    return pl.pallas_call(
        body,
        out_shape=outs,
        in_specs=[SMEM if a.dtype == jnp.int32 else VMEM for a in args],
        out_specs=[VMEM] * len(outs),
        scratch_shapes=list(scratch),
        compiler_params=pltpu.CompilerParams(vmem_limit_bytes=24 << 20),
        cost_estimate=pl.CostEstimate(flops=flops, bytes_accessed=0, transcendentals=0),
        name=body.__name__ if hasattr(body, "__name__") else body.func.__name__,
    )(*args)


def prepare(owner, row, count, flow, matrix, weight, innovation, up, down, bulk):
    for i in range(HALO):
        for f in range(2):
            for h in range(2):
                at = (i * 2 + f) * LEVELS + h * 8
                start = f * LEVELS * ROWS + h * 8 * ROWS
                up[at : at + 8, :] = flow[pl.ds(start + ROWS - HALO + i, 8, stride=ROWS), :]
                down[at : at + 8, :] = flow[pl.ds(start + i, 8, stride=ROWS), :]
    base = HALO * 2 * LEVELS
    up[base : base + OWN, :] = jnp.zeros((OWN, LANES), F32)
    bulk[...] = jnp.zeros(bulk.shape, F32)
    owners = [owner[j] for j in range(CAP)]
    turns = [sum([(owners[i] == owners[j]).astype(jnp.int32) for i in range(j)], jnp.int32(0)) for j in range(CAP)]
    column = jnp.transpose(weight[...] * innovation[...])
    ln, rw = lanes(HALF), places(HALF)
    where_to = jnp.full((8, LANES), NOWHERE, F32)
    for j in range(CAP):
        live = j < count[0]
        total = jnp.zeros((8, LANES), F32)
        for k in range(LANES // 8):
            total += matrix[j, k * 8 : k * 8 + 8, :] * column[k * 8 : k * 8 + 8, j : j + 1]
        pulled = jnp.where(live, jnp.sum(total, axis=0, keepdims=True), 0.0)
        slot = owners[j] * SLOT + turns[j]
        up[pl.ds(base + slot, 1), :] = pulled
        place = jnp.where(live, (lax.rem(row[j], ROWS) + HALO) * LEVELS + lax.div(row[j], ROWS), int(NOWHERE)).astype(F32)
        where_to = jnp.where(lanes(8) == slot, place, where_to)
    up[base + OWN :, :] = where_to
    down[base:, :] = up[base:, :]
    for j in range(CAP):
        block = matrix[j]
        scaled = jnp.transpose(block) * jnp.where(j < count[0], weight[j : j + 1, :], 0.0)
        gram = jnp.dot(scaled, block, precision=HIGHEST, preferred_element_type=F32)
        top, low = gram[:HALF], gram[HALF:]
        packed = jnp.where((ln >= HALF) & (ln - HALF <= rw), roll(top, HALF), low)
        diagonal = jnp.sum(jnp.where(ln - HALF == rw, low, 0.0), axis=0, keepdims=True)
        at = owners[j] * BULK + turns[j] * HALF
        bulk[pl.ds(pl.multiple_of(at, 8), HALF), :] = packed
        bulk[pl.ds(owners[j] * BULK + 2 * HALF + turns[j], 1), :] = diagonal


def widen(where, flow, below, above, own, wide, small):
    base = HALO * 2 * LEVELS
    wide[:base, :] = below[:base, :]
    wide[(HALO + ROWS) * 2 * LEVELS :, :] = above[:base, :]
    for r in range(ROWS):
        for f in range(2):
            for h in range(2):
                at = ((HALO + r) * 2 + f) * LEVELS + h * 8
                wide[at : at + 8, :] = flow[pl.ds(f * LEVELS * ROWS + h * 8 * ROWS + r, 8, stride=ROWS), :]
    me = where[0]
    right = lax.rem(me + 1, LON) * SMALL + LIST
    left = lax.rem(me + LON - 1, LON) * SMALL + LIST
    ln = lanes(8)
    lists = [below, own, above]
    spots = []
    for n, ref in enumerate(lists):
        p = ref[base + OWN : base + OWN + 8, :] + float((n - 1) * ROWS * LEVELS)
        spots.append(jnp.where(ln < OWN, p, roll(p, OWN)))
    for d in range(LON):
        first = 2 * (d - 1) % OWN
        spot = jnp.full((8, LANES), NOWHERE, F32)
        for n, ref in enumerate(lists):
            at = d * SMALL + n * 6
            fit = min(6, OWN - first)
            small[at : at + fit, :] = ref[base + first : base + first + fit, :]
            if fit < 6:
                small[at + fit : at + 6, :] = ref[base : base + 6 - fit, :]
            spot = jnp.where((ln >= n * 6) & (ln < n * 6 + 6), roll(spots[n], n * 6 - first), spot)
        small[d * SMALL + 18 : d * SMALL + LIST, :] = spot[:6]
        small[d * SMALL + LIST : (d + 1) * SMALL, :] = jnp.zeros((64, LANES), F32)
    for f in range(2):
        for g in range(WIDE // 8):
            to_right = jnp.zeros((8, LANES), F32)
            to_left = jnp.zeros((8, LANES), F32)
            for k in range(8):
                at = ((g * 8 + k) * 2 + f) * LEVELS
                low, high = wide[at : at + 8, :], wide[at + 8 : at + 16, :]
                mine_low = (ln >= 16 * k) & (ln < 16 * k + 8)
                mine_high = (ln >= 16 * k + 8) & (ln < 16 * k + 16)
                to_right = jnp.where(mine_low, roll(low, 16 * k + 8), jnp.where(mine_high, roll(high, 16 * k + 16), to_right))
                to_left = jnp.where(mine_low, roll(low, 16 * k), jnp.where(mine_high, roll(high, 16 * k + 8), to_left))
            at = (f * 4 + g) * 8
            small[pl.ds(pl.multiple_of(right + at, 8), 8), :] = to_right
            small[pl.ds(pl.multiple_of(left + at, 8), 8), :] = to_left


def unpack(bulk, grams):
    ln, rw = lanes(HALF), places(HALF)
    upper, diagonal, first = ln - HALF > rw, ln - HALF == rw, ln < HALF
    for s in range(LON):
        both = bulk[s * BULK : s * BULK + 2 * HALF, :]
        turned = jnp.transpose(both)
        ct, et = turned[:HALF], turned[HALF:]
        ct_rolled, et_rolled = roll(ct, HALF), roll(et, HALF)
        for o in range(SLOT):
            q = both[o * HALF : (o + 1) * HALF]
            d = bulk[s * BULK + 2 * HALF + o : s * BULK + 2 * HALF + o + 1, :]
            e_first, e_last = (et, et_rolled) if o == 0 else (et_rolled, et)
            c_last = ct_rolled if o == 0 else ct
            top = jnp.where(first, jnp.where(ln <= rw, roll(q, HALF), e_first), c_last)
            low = jnp.where(first | upper, q, jnp.where(diagonal, d, e_last))
            at = (o * LON + s) * LANES
            grams[at : at + HALF, :] = top
            grams[at + HALF : at + LANES, :] = low


def split(x):
    high = x.astype(jnp.bfloat16)
    rest = x - high.astype(F32)
    middle = rest.astype(jnp.bfloat16)
    low = (rest - middle.astype(F32)).astype(jnp.bfloat16)
    return jnp.concatenate([high, middle, low], axis=1)


def chosen(one_hot, parts):
    out = jnp.dot(one_hot, parts, preferred_element_type=F32)
    return out[:, :LANES] + out[:, LANES : 2 * LANES] + out[:, 2 * LANES :]


def one_hot(index, at):
    return jnp.where(index == at, 1.0, 0.0).astype(jnp.bfloat16)


def padded(x, rows):
    return jnp.concatenate([x, jnp.zeros((rows - x.shape[0], LANES), F32)], axis=0)


def lay_out(spot, own, sides, field, strips, low, high):
    spot = spot.astype(jnp.int32)
    by_lane = [jnp.transpose(spot[i * LANES : (i + 1) * LANES].astype(F32))[:8].astype(jnp.int32) for i in range(2)]
    ln = lanes(LANES)
    own_strip = jnp.where(ln < 32, jnp.where(ln >= 8, roll(own, 8), 0.0), jnp.where(ln < 56, roll(own, 56), 0.0))
    left = (places(LANES) < NEAR) & (ln < 8)
    right = (places(LANES) >= NEAR) & (ln >= 56) & (ln < 64)
    side_strip = jnp.where(left, roll(sides, 8), jnp.where(right, roll(sides, 56), 0.0))
    pieces = []
    for i, strip in enumerate((own_strip, side_strip)):
        upper = (spot[i * LANES : (i + 1) * LANES] & 8) != 0
        pieces.append(split(jnp.where(upper, roll(strip, HALF), strip)))
    own_parts = split(own)
    p = jnp.broadcast_to(by_lane[0][:1], (LANES, LANES))
    for start in range(low * LEVELS, high * LEVELS, LANES):
        field[start : start + LANES, :] = chosen(one_hot(places(LANES) + start, p), own_parts)
    folded = [jnp.broadcast_to((((b >> 4) << 3) + (b & 7))[:1], (64, LANES)) for b in by_lane]
    for start in range(low * 8, high * 8, 64):
        at = places(64) + start
        strips[start : start + 64, :] = chosen(one_hot(at, folded[0]), pieces[0]) + chosen(one_hot(at, folded[1]), pieces[1])


def adjoint(rates, source, target, first, last, height):
    before = kept = None
    for r in range(first, last + 1):
        y = source[r * height : (r + 1) * height, :]
        lat, lon = rates(r)
        t = lat * y
        a = jnp.where(lat > 0.0, t, 0.0)
        b = a - t
        s = lon * y
        e = jnp.where(lon > 0.0, s, 0.0)
        f = e - s
        if r > first + 1:
            target[(r - 1) * height : r * height, :] = kept + a
        if r > first:
            kept = y - (a + b) - (e + f) + roll(e, -1) + roll(f, 1) + before
        before = b


def tangent(rates, source, target, first, last, height):
    for r in range(first + 1, last):
        x = source[r * height : (r + 1) * height, :]
        south = source[(r - 1) * height : r * height, :]
        north = source[(r + 1) * height : (r + 2) * height, :]
        lat, lon = rates(r)
        out = x + jnp.abs(lat) * (jnp.where(lat > 0.0, south, north) - x)
        target[r * height : (r + 1) * height, :] = out + jnp.abs(lon) * (jnp.where(lon > 0.0, roll(x, 1), roll(x, -1)) - x)


def merged(field, strips, r):
    ln = lanes(8)
    t = strips[r * 8 : (r + 1) * 8, :]
    low, high = field[r * LEVELS : r * LEVELS + 8, :], field[r * LEVELS + 8 : (r + 1) * LEVELS, :]
    low = jnp.where(ln < 8, roll(t, -8), jnp.where(ln >= 120, roll(t, 72), low))
    high = jnp.where(ln < 8, roll(t, -72), jnp.where(ln >= 120, roll(t, 8), high))
    return low, high


def wide_rates(wide):
    return lambda r: (wide[r * 2 * LEVELS : (r * 2 + 1) * LEVELS, :], wide[(r * 2 + 1) * LEVELS : (r + 1) * 2 * LEVELS, :])


def edge_rates(edge):
    return lambda r: (edge[r * 16 : r * 16 + 8, :], edge[r * 16 + 8 : (r + 1) * 16, :])


def hessian_half(where, spot, own, sides, wide, edge, grams, kept, terms, fields, strips, image):
    field, other = fields
    strip, other_strip = strips
    lay_out(spot, own, sides, field, strip, 0, WIDE)
    full, narrow = wide_rates(wide), edge_rates(edge)
    pair, strip_pair = (field, other), (strip, other_strip)
    for k in range(STEPS):
        adjoint(full, *pair, k, WIDE - 1 - k, LEVELS)
        adjoint(narrow, *strip_pair, k, WIDE - 1 - k, 8)
        pair, strip_pair = pair[::-1], strip_pair[::-1]
    for flag, start in ((where[1], STEPS), (where[2], HALO + ROWS)):
        for ref, height in ((pair[0], LEVELS), (strip_pair[0], 8)):
            block = ref[start * height : (start + STEPS) * height, :]
            ref[start * height : (start + STEPS) * height, :] = jnp.where(flag == 1, 0.0, block)
    square = jnp.zeros((8, LANES), F32)
    for r in range(ROWS):
        low, high = merged(pair[0], strip_pair[0], r + HALO)
        kept[r * LEVELS : r * LEVELS + 8, :] = low
        kept[r * LEVELS + 8 : (r + 1) * LEVELS, :] = high
        square += low * low + high * high
    for k in range(STEPS, 2 * STEPS):
        tangent(full, *pair, k, WIDE - 1 - k, LEVELS)
        tangent(narrow, *strip_pair, k, WIDE - 1 - k, 8)
        pair, strip_pair = pair[::-1], strip_pair[::-1]
    for r in range(ROWS):
        low, high = merged(pair[0], strip_pair[0], r + HALO)
        image[r * LEVELS : r * LEVELS + 8, :] = low
        image[r * LEVELS + 8 : (r + 1) * LEVELS, :] = high
    mine = spot[OWN : 2 * OWN].astype(jnp.int32) - HALO * LEVELS
    hit = jnp.concatenate([one_hot(lanes(OWN), mine), one_hot(lanes(OWN) + LANES, mine)], axis=1)
    seen = chosen(hit, split(image[...]))
    column = jnp.transpose(seen)
    for t in range(OWN):
        total = jnp.zeros((8, LANES), F32)
        for k in range(LANES // 8):
            at = t * LANES + k * 8
            total += grams[at : at + 8, :] * column[k * 8 : k * 8 + 8, t : t + 1]
        terms[t : t + 1, :] = jnp.sum(total, axis=0, keepdims=True)
    return jnp.sum(square, keepdims=True), jnp.sum(seen * terms[...], keepdims=True)


def first_half(where, small, wide, grams, edge, spots, kept, terms, sums, field, other, strip, other_strip, image):
    ln = lanes(8)
    me = where[0]
    from_left = lax.rem(me + LON - 1, LON) * SMALL + LIST
    from_right = lax.rem(me + 1, LON) * SMALL + LIST
    for f in range(2):
        for g in range(WIDE // 8):
            at = (f * 4 + g) * 8
            left = small[pl.ds(pl.multiple_of(from_left + at, 8), 8), :]
            right = small[pl.ds(pl.multiple_of(from_right + at, 8), 8), :]
            for k in range(8):
                r = g * 8 + k
                at = (r * 2 + f) * LEVELS
                low, high = wide[at : at + 8, :], wide[at + 8 : at + 16, :]
                a = jnp.where(ln < 8, roll(left, -16 * k), jnp.where(ln < 32, roll(low, 8), jnp.where(ln < 56, roll(low, 56), roll(right, 56 - 16 * k))))
                b = jnp.where(ln < 72, roll(left, 56 - 16 * k), jnp.where(ln < 96, roll(high, 72), jnp.where(ln < 120, roll(high, 120), roll(right, 112 - 16 * k))))
                edge[(r * 2 + f) * 8 : (r * 2 + f + 1) * 8, :] = jnp.where(ln < HALF, a, b)
    named = small[pl.ds(18, LON, stride=SMALL), :]

    def spot_of(n, k):
        return jnp.broadcast_to(named[:, n * 6 + k : n * 6 + k + 1], (LON, LANES))

    def row_of(n, k):
        return small[pl.ds(n * 6 + k, LON, stride=SMALL), :]

    order = [[(n, k + o) for n in range(3) for o in range(SLOT)] for k in (2, 0, 4)]
    nowhere = jnp.full((LANES - NEAR, LANES), NOWHERE, F32)
    spot = jnp.concatenate(
        [spot_of(*i) for i in order[0]] + [nowhere] + [spot_of(*i) for i in order[1] + order[2]] + [nowhere[: LANES - 2 * NEAR]], axis=0
    )
    spots[...] = spot
    own = padded(jnp.concatenate([row_of(*i) for i in order[0]], axis=0), LANES)
    sides = padded(jnp.concatenate([row_of(*i) for i in order[1] + order[2]], axis=0), LANES)
    square, product = hessian_half(where, spot, own, sides, wide, edge, grams, kept, terms, (field, other), (strip, other_strip), image)
    sums[...] = jnp.where(ln == 0, square, jnp.where(ln == 1, product, 0.0))


def second_half(where, spots, own, left, right, wide, edge, grams, before, kept, terms, sums, field, other, strip, other_strip, image):
    own = padded(own[...], LANES)
    sides = padded(jnp.concatenate([left[...], right[...]], axis=0), LANES)
    square, product = hessian_half(where, spots[...], own, sides, wide, edge, grams, kept, terms, (field, other), (strip, other_strip), image)
    ln = lanes(8)
    mine = before[...] + jnp.where(ln == 2, square, jnp.where(ln == 3, product, 0.0))
    sums[...] = jnp.concatenate([mine] * (sums.shape[0] // 8), axis=0)


def gathered(parts, sums):
    sums[...] = jnp.broadcast_to(jnp.sum(parts[...], axis=0, keepdims=True), sums.shape)


def finish(spots, own, left, right, wide, edge, parts, right_side, image, increment, residual, field, other, strip, other_strip):
    own = padded(own[...], LANES)
    sides = padded(jnp.concatenate([left[...], right[...]], axis=0), LANES)
    lay_out(spots[...], own, sides, field, strip, HALO - STEPS, HALO + ROWS + STEPS)
    full, narrow = wide_rates(wide), edge_rates(edge)
    pair, strip_pair = (field, other), (strip, other_strip)
    for k in range(STEPS, 2 * STEPS):
        adjoint(full, *pair, k, WIDE - 1 - k, LEVELS)
        adjoint(narrow, *strip_pair, k, WIDE - 1 - k, 8)
        pair, strip_pair = pair[::-1], strip_pair[::-1]
    total = jnp.sum(parts[...], axis=0, keepdims=True)
    m0, m1, m2, m3 = (jnp.sum(jnp.where(lanes(1) == i, total, 0.0), keepdims=True) for i in range(4))
    step_0 = m0 / (m0 + m1)
    rho = m1 / m0
    spread = m2 - rho * m1
    curve = (m3 - rho * m2) - rho * (m2 - rho * m1)
    gamma = step_0 * spread / m0
    step_1 = spread / (spread + curve - gamma * spread)
    on_b = step_0 * (1.0 + step_1 * (gamma + rho))
    on_k = -step_0 * step_1
    rest_b = step_0 * ((1.0 - step_1) * rho - step_1 * gamma)
    rest_k = -step_0 * ((1.0 - step_1) + step_1 * (rho + gamma))
    rest_kk = step_0 * step_1
    on_b, on_k, rest_b, rest_k, rest_kk = (jnp.broadcast_to(v, (8, LANES)) for v in (on_b, on_k, rest_b, rest_k, rest_kk))
    for r in range(ROWS):
        for h, second in enumerate(merged(pair[0], strip_pair[0], r + HALO)):
            at = r * LEVELS + h * 8
            b, first = right_side[at : at + 8, :], image[at : at + 8, :]
            to = pl.ds(h * 8 * ROWS + r, 8, stride=ROWS)
            increment[to, :] = on_b * b + on_k * first
            residual[to, :] = rest_b * b + rest_k * first + rest_kk * second


def shift(x, axis, step, wrap):
    count = lax.axis_size(axis)
    pairs = [(i, (i + step) % count) for i in range(count) if wrap or 0 <= i + step < count]
    return lax.ppermute(x, axis, pairs)


def beside(terms):
    own = jnp.concatenate([shift(terms, LAT, 1, False), terms, shift(terms, LAT, -1, False)], axis=0)
    return own, shift(own, "lon", 1, True), shift(own, "lon", -1, True)


def spread_out(sums, axes):
    return lax.all_to_all(sums[:, None, :], axes, split_axis=0, concat_axis=0, tiled=True)[:, 0, :]


def shards(courant, obs_matrix, obs_weight, innovation, block_owner, block_row, block_count):
    lat_index = lax.axis_index(LAT)
    lat_total = lax.axis_size(LAT)
    where = jnp.stack([lax.axis_index("lon"), (lat_index == 0).astype(jnp.int32), (lat_index == lat_total - 1).astype(jnp.int32)]).astype(jnp.int32)
    flow = courant.reshape(-1, LANES)
    message = HALO * 2 * LEVELS + OWN + 8
    up, down, bulk = call(
        prepare,
        [(message, LANES), (message, LANES), (LON * BULK, LANES)],
        (block_owner.reshape(-1), block_row.reshape(-1), block_count.reshape(-1), flow, obs_matrix[0], obs_weight[0], innovation[0]),
        4_000_000,
    )
    packed = lax.all_to_all(bulk.reshape(LON, BULK, LANES), "lon", split_axis=0, concat_axis=0, tiled=True)
    below, above = shift(up, LAT, 1, False), shift(down, LAT, -1, False)
    wide, small = call(
        widen, [(WIDE * 2 * LEVELS, LANES), (LON * SMALL, LANES)], (where, flow, below, above, up), 2_000_000
    )
    small = lax.all_to_all(small.reshape(LON, SMALL, LANES), "lon", split_axis=0, concat_axis=0, tiled=True)
    (grams,) = call(unpack, [(OWN * LANES, LANES)], (packed.reshape(LON * BULK, LANES),), 2_000_000)
    cells = (ROWS * LEVELS, LANES)
    work = [pltpu.VMEM((WIDE * LEVELS, LANES), F32)] * 2 + [pltpu.VMEM((WIDE * 8, LANES), F32)] * 2
    image = pltpu.VMEM(cells, F32)
    edge, spots, right_side, terms, sums = call(
        first_half,
        [(WIDE * 2 * 8, LANES), (2 * LANES, LANES), cells, (OWN, LANES), (8, LANES)],
        (where, small.reshape(LON * SMALL, LANES), wide, grams),
        4_000_000,
        work + [image],
    )
    plane = lax.axis_size(("lat_1", "lon"))
    towers = lax.axis_size(("lat_0", "lat_2"))
    kept, terms, sums = call(
        second_half,
        [cells, (OWN, LANES), (plane, LANES)],
        (where, spots, *beside(terms), wide, edge, grams, sums),
        4_000_000,
        work + [image],
    )
    (sums,) = call(gathered, [(towers, LANES)], (spread_out(sums, ("lat_1", "lon")),), 10_000)
    parts = spread_out(sums, ("lat_0", "lat_2"))
    increment, residual = call(
        finish, [cells, cells], (spots, *beside(terms), wide, edge, parts, right_side, kept), 2_000_000, work
    )
    shape = courant.shape[1:]
    return increment.reshape(shape), residual.reshape(shape)


def solution(mesh):
    torus = Mesh(
        mesh.devices.reshape(-1, 4, 2, mesh.shape["lon"]), ("lat_0", "lat_1", "lat_2", "lon")
    )
    placed = (
        P(None, None, LAT, "lon"),
        P(LAT, "lon", None, None),
        P(LAT, "lon", None),
        P(LAT, "lon", None),
        P(LAT, "lon", None),
        P(LAT, "lon"),
        P(LAT, "lon"),
    )
    return jax.shard_map(
        shards,
        mesh=torus,
        in_specs=placed,
        out_specs=(P(None, LAT, "lon"), P(None, LAT, "lon")),
        check_vma=False,
    )
```

```python
import jax
import jax.numpy as jnp
from jax import lax
from jax.experimental import pallas as pl
from jax.experimental.pallas import tpu as pltpu
from jax.sharding import Mesh
from jax.sharding import PartitionSpec as P

LAT = ("lat_0", "lat_1", "lat_2")
LEVELS = 16
ROWS = 16
LANES = 128
CAP = 8
SLOT = 2
STEPS = 4
HALO = 2 * STEPS
WIDE = ROWS + 2 * HALO
LON = 8
HALF = LANES // 2
OWN = LON * SLOT
NEAR = 3 * OWN
BULK = 2 * HALF + 8
LIST = 8
SMALL = LIST + 32
EDGES = HALO * 2 * LEVELS
OWNS = EDGES + HALO * 2 * 8
LEFTS = OWNS + OWN
RIGHTS = LEFTS + OWN
SPOTS = RIGHTS + OWN
MESSAGE = SPOTS + 8
NOWHERE = -4096.0
HIGHEST = lax.Precision.HIGHEST
F32 = jnp.float32
VMEM = pl.BlockSpec(memory_space=pltpu.VMEM)
SMEM = pl.BlockSpec(memory_space=pltpu.SMEM)


def lanes(rows):
    return lax.broadcasted_iota(jnp.int32, (rows, LANES), 1)


def places(rows):
    return lax.broadcasted_iota(jnp.int32, (rows, LANES), 0)


def roll(x, shift):
    shift %= LANES
    return pltpu.roll(x, shift, axis=1) if shift else x


def call(body, outs, args, flops, scratch=(), specs=None, room=24):
    return pl.pallas_call(
        body,
        out_shape=[jax.ShapeDtypeStruct(s, F32) for s in outs],
        in_specs=specs or [SMEM if a.dtype == jnp.int32 else VMEM for a in args],
        out_specs=[VMEM] * len(outs),
        scratch_shapes=list(scratch),
        compiler_params=pltpu.CompilerParams(vmem_limit_bytes=room << 20),
        cost_estimate=pl.CostEstimate(flops=flops, bytes_accessed=0, transcendentals=0),
        name=body.__name__,
    )(*args)


def turns_of(owners):
    return [sum([(o == owners[j]).astype(jnp.int32) for o in owners[:j]], jnp.int32(0)) for j in range(CAP)]


def packed_edges(pick, shift):
    ln = lanes(8)
    out = jnp.zeros((8, LANES), F32)
    for k in range(8):
        low, high = pick(k)
        out = jnp.where((ln >= 16 * k) & (ln < 16 * k + 8), roll(low, 16 * k + shift), out)
        out = jnp.where((ln >= 16 * k + 8) & (ln < 16 * k + 16), roll(high, 16 * k + 8 + shift), out)
    return out


def prepare(where, owner_at, row_at, count_at, flow_at, matrix_at, weight_at, innovation_at, small, owner, row, count, flow, matrix, weight, innovation, lists, sems):
    pairs = ((owner_at, owner), (row_at, row), (count_at, count), (flow_at, flow), (weight_at, weight), (innovation_at, innovation), (matrix_at, matrix))
    copies = [pltpu.make_async_copy(a, b, sems.at[i]) for i, (a, b) in enumerate(pairs)]
    for copy in copies:
        copy.start()
    copies[3].wait()
    me = where[0]
    to_right = lax.rem(me + 1, LON) * SMALL + LIST
    to_left = lax.rem(me + LON - 1, LON) * SMALL + LIST
    for f in range(2):
        for g in range(2):

            def pick(k, f=f, g=g):
                at = f * LEVELS * ROWS + g * 8 + k
                return flow[pl.ds(at, 8, stride=ROWS), :], flow[pl.ds(at + 8 * ROWS, 8, stride=ROWS), :]

            at = (f * 2 + g) * 8
            small[pl.ds(pl.multiple_of(to_right + at, 8), 8), :] = packed_edges(pick, 8)
            small[pl.ds(pl.multiple_of(to_left + at, 8), 8), :] = packed_edges(pick, 0)
    for i in (0, 1, 2, 4, 5, 6):
        copies[i].wait()
    owners = [owner[j] for j in range(CAP)]
    turns = turns_of(owners)
    lists[...] = jnp.zeros(lists.shape, F32)
    column = jnp.transpose(weight[...] * innovation[...])
    ln = lanes(8)
    named = jnp.full((8, LANES), NOWHERE, F32)
    for j in range(CAP):
        live = j < count[0]
        total = jnp.zeros((8, LANES), F32)
        for k in range(LANES // 8):
            total += matrix[j, k * 8 : k * 8 + 8, :] * column[k * 8 : k * 8 + 8, j : j + 1]
        slot = owners[j] * SLOT + turns[j]
        lists[pl.ds(slot, 1), :] = jnp.where(live, jnp.sum(total, axis=0, keepdims=True), 0.0)
        place = jnp.where(live, (lax.rem(row[j], ROWS) + HALO) * LEVELS + lax.div(row[j], ROWS), int(NOWHERE)).astype(F32)
        named = jnp.where(ln == slot, place, named)
    named = jnp.where(ln < OWN, named, roll(named, OWN))
    line = lanes(1)
    for d in range(LON):
        left, right = 2 * (d - 1) % OWN, 2 * (d + 1) % OWN
        small[d * SMALL : d * SMALL + 2, :] = lists[2 * d : 2 * d + 2, :]
        edge = jnp.where(line < 8, roll(lists[left : left + 1, :], 8), roll(lists[left + 1 : left + 2, :], 16))
        edge = jnp.where(line < 16, edge, jnp.where(line < 24, roll(lists[right : right + 1, :], 16), roll(lists[right + 1 : right + 2, :], 24)))
        small[d * SMALL + 2 : d * SMALL + 3, :] = edge
        small[d * SMALL + 3 : d * SMALL + 4, :] = roll(named, -left)[:1]


def weigh_blocks(owner, row, count, matrix, weight, bulk):
    bulk[...] = jnp.zeros(bulk.shape, F32)
    owners = [owner[j] for j in range(CAP)]
    turns = turns_of(owners)
    ln, rw = lanes(HALF), places(HALF)
    for j in range(CAP):
        block = matrix[j]
        scaled = jnp.transpose(block) * jnp.where(j < count[0], weight[j : j + 1, :], 0.0)
        gram = jnp.dot(scaled, block, precision=HIGHEST, preferred_element_type=F32)
        top, low = gram[:HALF], gram[HALF:]
        packed = jnp.where((ln >= HALF) & (ln - HALF <= rw), roll(top, HALF), low)
        diagonal = jnp.sum(jnp.where(ln - HALF == rw, low, 0.0), axis=0, keepdims=True)
        at = owners[j] * BULK + turns[j] * HALF
        bulk[pl.ds(pl.multiple_of(at, 8), HALF), :] = packed
        bulk[pl.ds(owners[j] * BULK + 2 * HALF + turns[j], 1), :] = diagonal


def arrange(where, flow, small, up, down):
    ln = lanes(8)
    me = where[0]
    from_left = lax.rem(me + LON - 1, LON) * SMALL + LIST
    from_right = lax.rem(me + 1, LON) * SMALL + LIST
    for f in range(2):
        for g, out in enumerate((down, up)):
            at = (f * 2 + g) * 8
            left = small[pl.ds(pl.multiple_of(from_left + at, 8), 8), :]
            right = small[pl.ds(pl.multiple_of(from_right + at, 8), 8), :]
            for k in range(8):
                at = f * LEVELS * ROWS + g * 8 + k
                low, high = flow[pl.ds(at, 8, stride=ROWS), :], flow[pl.ds(at + 8 * ROWS, 8, stride=ROWS), :]
                at = (k * 2 + f) * LEVELS
                out[at : at + 8, :] = low
                out[at + 8 : at + 16, :] = high
                a = jnp.where(ln < 8, roll(left, -16 * k), jnp.where(ln < 32, roll(low, 8), jnp.where(ln < 56, roll(low, 56), roll(right, 56 - 16 * k))))
                b = jnp.where(ln < 72, roll(left, 56 - 16 * k), jnp.where(ln < 96, roll(high, 72), jnp.where(ln < 120, roll(high, 120), roll(right, 112 - 16 * k))))
                at = EDGES + (k * 2 + f) * 8
                out[at : at + 8, :] = jnp.where(ln < HALF, a, b)
    edge = small[pl.ds(2, LON, stride=SMALL), :]
    named = small[pl.ds(3, LON, stride=SMALL), :]
    turned = jnp.transpose(named)
    spot = jnp.full((1, LANES), NOWHERE, F32)
    line = lanes(1)
    for i, k in enumerate((2, 3, 0, 1, 4, 5)):
        line_k = jnp.concatenate([turned[k : k + 1, :], jnp.zeros((1, LANES - LON), F32)], axis=1)
        spot = jnp.where((line >= 8 * i) & (line < 8 * i + 8), roll(line_k, 8 * i), spot)
    for o in range(SLOT):
        own = small[pl.ds(o, LON, stride=SMALL), :]
        left = jnp.where(ln < 8, roll(edge, -8 * o), 0.0)
        right = jnp.where((ln >= 56) & (ln < 64), roll(edge, 40 - 8 * o), 0.0)
        for out in (up, down):
            out[OWNS + o * LON : OWNS + (o + 1) * LON, :] = own
            out[LEFTS + o * LON : LEFTS + (o + 1) * LON, :] = left
            out[RIGHTS + o * LON : RIGHTS + (o + 1) * LON, :] = right
    for out in (up, down):
        out[SPOTS:, :] = jnp.broadcast_to(spot, (8, LANES))


def unpack(bulk, grams):
    ln, rw = lanes(HALF), places(HALF)
    upper, diagonal, first = ln - HALF > rw, ln - HALF == rw, ln < HALF
    for s in range(LON):
        both = bulk[s * BULK : s * BULK + 2 * HALF, :]
        turned = jnp.transpose(both)
        ct, et = turned[:HALF], turned[HALF:]
        ct_rolled, et_rolled = roll(ct, HALF), roll(et, HALF)
        for o in range(SLOT):
            q = both[o * HALF : (o + 1) * HALF]
            d = bulk[s * BULK + 2 * HALF + o : s * BULK + 2 * HALF + o + 1, :]
            e_first, e_last = (et, et_rolled) if o == 0 else (et_rolled, et)
            c_last = ct_rolled if o == 0 else ct
            top = jnp.where(first, jnp.where(ln <= rw, roll(q, HALF), e_first), c_last)
            low = jnp.where(first | upper, q, jnp.where(diagonal, d, e_last))
            at = (o * LON + s) * LANES
            grams[at : at + HALF, :] = top
            grams[at + HALF : at + LANES, :] = low


def split(x):
    high = x.astype(jnp.bfloat16)
    rest = x - high.astype(F32)
    middle = rest.astype(jnp.bfloat16)
    low = (rest - middle.astype(F32)).astype(jnp.bfloat16)
    return jnp.concatenate([high, middle, low], axis=1)


def chosen(one_hot, parts):
    out = jnp.dot(one_hot, parts, preferred_element_type=F32)
    return out[:, :LANES] + out[:, LANES : 2 * LANES] + out[:, 2 * LANES :]


def one_hot(index, at):
    return jnp.where(index == at, 1.0, 0.0).astype(jnp.bfloat16)


def padded(x, rows):
    return jnp.concatenate([x, jnp.zeros((rows - x.shape[0], LANES), F32)], axis=0)


def left_strips(x):
    return jnp.where(lanes(x.shape[0]) < 8, roll(x, 8), 0.0)


def right_strips(x):
    ln = lanes(x.shape[0])
    return jnp.where((ln >= 56) & (ln < 64), roll(x, 56), 0.0)


def lay_out(spots, by_lane, own, sides, field, strips, low, high):
    ln = lanes(LANES)
    own_strip = jnp.where(ln < 32, jnp.where(ln >= 8, roll(own, 8), 0.0), jnp.where(ln < 56, roll(own, 56), 0.0))
    pieces = []
    for i, strip in enumerate((own_strip, sides)):
        upper = (spots[i * LANES : (i + 1) * LANES, :].astype(jnp.int32) & 8) != 0
        pieces.append(split(jnp.where(upper, roll(strip, HALF), strip)))
    own_parts = split(own)
    lane_spots = [by_lane[i * 8 : i * 8 + 1, :].astype(jnp.int32) for i in range(2)]
    p = jnp.broadcast_to(lane_spots[0], (LANES, LANES))
    for start in range(low * LEVELS, high * LEVELS, LANES):
        field[start : start + LANES, :] = chosen(one_hot(places(LANES) + start, p), own_parts)
    folded = [jnp.broadcast_to(((b >> 4) << 3) + (b & 7), (64, LANES)) for b in lane_spots]
    for start in range(low * 8, high * 8, 64):
        at = places(64) + start
        strips[start : start + 64, :] = chosen(one_hot(at, folded[0]), pieces[0]) + chosen(one_hot(at, folded[1]), pieces[1])


def adjoint(rates, source, target, first, last, height):
    before = kept = None
    for r in range(first, last + 1):
        y = source[r * height : (r + 1) * height, :]
        lat, lon = rates(r)
        t = lat * y
        a = jnp.where(lat > 0.0, t, 0.0)
        b = a - t
        s = lon * y
        e = jnp.where(lon > 0.0, s, 0.0)
        f = e - s
        if r > first + 1:
            target[(r - 1) * height : r * height, :] = kept + a
        if r > first:
            kept = y - (a + b) - (e + f) + roll(e, -1) + roll(f, 1) + before
        before = b


def tangent(rates, source, target, first, last, height):
    for r in range(first + 1, last):
        x = source[r * height : (r + 1) * height, :]
        south = source[(r - 1) * height : r * height, :]
        north = source[(r + 1) * height : (r + 2) * height, :]
        lat, lon = rates(r)
        out = x + jnp.abs(lat) * (jnp.where(lat > 0.0, south, north) - x)
        target[r * height : (r + 1) * height, :] = out + jnp.abs(lon) * (jnp.where(lon > 0.0, roll(x, 1), roll(x, -1)) - x)


def merged(field, strips, r):
    ln = lanes(8)
    t = strips[r * 8 : (r + 1) * 8, :]
    low, high = field[r * LEVELS : r * LEVELS + 8, :], field[r * LEVELS + 8 : (r + 1) * LEVELS, :]
    low = jnp.where(ln < 8, roll(t, -8), jnp.where(ln >= 120, roll(t, 72), low))
    high = jnp.where(ln < 8, roll(t, -72), jnp.where(ln >= 120, roll(t, 8), high))
    return low, high


def rates_of(below, down, up, above, start, height):
    def rates(r):
        part, r = (below, down, up, above)[r // HALO], r % HALO
        at = start + r * 2 * height
        return part[at : at + height, :], part[at + height : at + 2 * height, :]

    return rates


def steps_back(messages, fields, strips, first):
    full, narrow = rates_of(*messages, 0, LEVELS), rates_of(*messages, EDGES, 8)
    for k in range(first, first + STEPS):
        adjoint(full, *fields, k, WIDE - 1 - k, LEVELS)
        adjoint(narrow, *strips, k, WIDE - 1 - k, 8)
        fields, strips = fields[::-1], strips[::-1]
    return fields, strips


def steps_on(messages, fields, strips, first):
    full, narrow = rates_of(*messages, 0, LEVELS), rates_of(*messages, EDGES, 8)
    for k in range(first, first + STEPS):
        tangent(full, *fields, k, WIDE - 1 - k, LEVELS)
        tangent(narrow, *strips, k, WIDE - 1 - k, 8)
        fields, strips = fields[::-1], strips[::-1]
    return fields, strips


def back_and_on(where, spots, by_lane, own, sides, messages, kept, fields, strips, image):
    lay_out(spots, by_lane, own, sides, fields[0], strips[0], 0, WIDE)
    fields, strips = steps_back(messages, fields, strips, 0)
    for flag, start in ((where[1], STEPS), (where[2], HALO + ROWS)):
        for ref, height in ((fields[0], LEVELS), (strips[0], 8)):
            block = ref[start * height : (start + STEPS) * height, :]
            ref[start * height : (start + STEPS) * height, :] = jnp.where(flag == 1, 0.0, block)
    square = jnp.zeros((8, LANES), F32)
    for r in range(ROWS):
        low, high = merged(fields[0], strips[0], r + HALO)
        kept[r * LEVELS : r * LEVELS + 8, :] = low
        kept[r * LEVELS + 8 : (r + 1) * LEVELS, :] = high
        square += low * low + high * high
    fields, strips = steps_on(messages, fields, strips, STEPS)
    for r in range(ROWS):
        low, high = merged(fields[0], strips[0], r + HALO)
        image[r * LEVELS : r * LEVELS + 8, :] = low
        image[r * LEVELS + 8 : (r + 1) * LEVELS, :] = high
    mine = spots[OWN : 2 * OWN, :].astype(jnp.int32) - HALO * LEVELS
    hit = jnp.concatenate([one_hot(lanes(OWN), mine), one_hot(lanes(OWN) + LANES, mine)], axis=1)
    return jnp.sum(square, keepdims=True), chosen(hit, split(image[...]))


def weigh(seen, grams):
    column = jnp.transpose(seen)
    out = []
    for t in range(OWN):
        total = jnp.zeros((8, LANES), F32)
        for k in range(LANES // 8):
            at = t * LANES + k * 8
            total += grams[at : at + 8, :] * column[k * 8 : k * 8 + 8, t : t + 1]
        out.append(jnp.sum(total, axis=0, keepdims=True))
    return jnp.concatenate(out, axis=0)


def in_lanes(first, values):
    ln = lanes(8)
    out = jnp.zeros((8, LANES), F32)
    for i, v in enumerate(values):
        out = jnp.where(ln == first + i, v, out)
    return out


def first_half(where, below, down, up, above, spots, by_lane, kept, seen, sums, field, other, strip, other_strip, image):
    ln = lanes(8)
    b, o, a = below[SPOTS:, :] - float(ROWS * LEVELS), up[SPOTS:, :], above[SPOTS:, :] + float(ROWS * LEVELS)
    tables = (((b, 0), (o, 0), (a, 0)), ((b, 16), (o, 16), (a, 16), (b, 32), (o, 32), (a, 32)))
    for i, table in enumerate(tables):
        spot = jnp.full((8, LANES), NOWHERE, F32)
        for n, (x, at) in enumerate(table):
            spot = jnp.where((ln >= OWN * n) & (ln < OWN * (n + 1)), roll(x, OWN * n - at), spot)
        by_lane[i * 8 : i * 8 + 8, :] = spot
        spots[i * LANES : (i + 1) * LANES, :] = jnp.transpose(jnp.broadcast_to(spot[:1], (LANES, LANES)))
    parts = (below, up, above)
    own = padded(jnp.concatenate([x[OWNS:LEFTS, :] for x in parts], axis=0), LANES)
    sides = padded(jnp.concatenate([x[LEFTS:RIGHTS, :] for x in parts] + [x[RIGHTS:SPOTS, :] for x in parts], axis=0), LANES)
    messages = (below, down, up, above)
    square, rows = back_and_on(where, spots, by_lane, own, sides, messages, kept, (field, other), (strip, other_strip), image)
    seen[...] = rows
    sums[...] = in_lanes(0, [square])


def first_terms(bulk, seen, before, grams, terms, sums):
    unpack(bulk, grams)
    rows = weigh(seen[...], grams)
    terms[...] = rows
    sums[...] = before[...] + in_lanes(1, [jnp.sum(seen[...] * rows, keepdims=True)])


def stepped(x, unit):
    row = places(OWN)
    for bit in range(4):
        x = jnp.where((row & (1 << bit)) != 0, roll(x, unit << bit), x)
    return x


def second_half(where, spots, by_lane, own, left, right, below, down, up, above, grams, before, kept, terms, parcels, field, other, strip, other_strip, image):
    own = padded(own[...], LANES)
    sides = padded(jnp.concatenate([left_strips(left[...]), right_strips(right[...])], axis=0), LANES)
    messages = (below, down, up, above)
    square, seen = back_and_on(where, spots, by_lane, own, sides, messages, kept, (field, other), (strip, other_strip), image)
    rows = weigh(seen, grams)
    terms[...] = rows
    sums = before[...] + in_lanes(2, [square, jnp.sum(seen * rows, keepdims=True)])
    parcels[...] = jnp.concatenate([sums] * (parcels.shape[0] // 8), axis=0)
    mine = (lanes(OWN) >> 3) == places(OWN)
    to_left = jnp.sum(jnp.where(mine, stepped(rows, 8), 0.0), axis=0, keepdims=True)
    to_right = jnp.sum(jnp.where(mine, stepped(roll(rows, 8), 8), 0.0), axis=0, keepdims=True)
    base = where[3] * LON
    parcels[pl.ds((base + lax.rem(where[0] + 1, LON)) * 2 + 1, 1), :] = to_right
    parcels[pl.ds((base + lax.rem(where[0] + LON - 1, LON)) * 2 + 1, 1), :] = to_left


def gathered(where, parts, terms, sums, message):
    count = parts.shape[0] // 2
    sums[...] = jnp.broadcast_to(jnp.sum(parts[pl.ds(0, count, stride=2), :], axis=0, keepdims=True), sums.shape)
    base = where[3] * LON
    message[:OWN, :] = terms[...]
    message[OWN : OWN + 1, :] = parts[pl.ds((base + lax.rem(where[0] + LON - 1, LON)) * 2 + 1, 1), :]
    message[OWN + 1 : OWN + 2, :] = parts[pl.ds((base + lax.rem(where[0] + 1, LON)) * 2 + 1, 1), :]
    message[OWN + 2 :, :] = jnp.zeros((6, LANES), F32)


def finish(spots, by_lane, south, mine, north, below, down, up, above, parts, right_side, image, increment, residual, field, other, strip, other_strip):
    lists = (south, mine, north)
    own = padded(jnp.concatenate([x[:OWN, :] for x in lists], axis=0), LANES)
    ln = lanes(OWN)
    rows = [stepped(jnp.broadcast_to(x[OWN : OWN + 1, :], (OWN, LANES)), -8) for x in lists]
    lefts = [jnp.where(ln < 8, x, 0.0) for x in rows]
    rows = [stepped(jnp.broadcast_to(x[OWN + 1 : OWN + 2, :], (OWN, LANES)), -8) for x in lists]
    rights = [right_strips(x) for x in rows]
    sides = padded(jnp.concatenate(lefts + rights, axis=0), LANES)
    lay_out(spots, by_lane, own, sides, field, strip, HALO - STEPS, HALO + ROWS + STEPS)
    fields, strips = steps_back((below, down, up, above), (field, other), (strip, other_strip), STEPS)
    total = jnp.sum(parts[...], axis=0, keepdims=True)
    m0, m1, m2, m3 = (jnp.sum(jnp.where(lanes(1) == i, total, 0.0), keepdims=True) for i in range(4))
    step_0 = m0 / (m0 + m1)
    rho = m1 / m0
    spread = m2 - rho * m1
    curve = (m3 - rho * m2) - rho * (m2 - rho * m1)
    gamma = step_0 * spread / m0
    step_1 = spread / (spread + curve - gamma * spread)
    on_b = step_0 * (1.0 + step_1 * (gamma + rho))
    on_k = -step_0 * step_1
    rest_b = step_0 * ((1.0 - step_1) * rho - step_1 * gamma)
    rest_k = -step_0 * ((1.0 - step_1) + step_1 * (rho + gamma))
    rest_kk = step_0 * step_1
    on_b, on_k, rest_b, rest_k, rest_kk = (jnp.broadcast_to(v, (8, LANES)) for v in (on_b, on_k, rest_b, rest_k, rest_kk))
    for r in range(ROWS):
        for h, second in enumerate(merged(fields[0], strips[0], r + HALO)):
            at = r * LEVELS + h * 8
            b, first = right_side[at : at + 8, :], image[at : at + 8, :]
            to = pl.ds(h * 8 * ROWS + r, 8, stride=ROWS)
            increment[to, :] = on_b * b + on_k * first
            residual[to, :] = rest_b * b + rest_k * first + rest_kk * second


def shift(x, axis, step, wrap):
    count = lax.axis_size(axis)
    pairs = [(i, (i + step) % count) for i in range(count) if wrap or 0 <= i + step < count]
    return lax.ppermute(x, axis, pairs)


def spread_out(x, axes):
    return lax.all_to_all(x, axes, split_axis=0, concat_axis=0, tiled=True)


def shards(courant, obs_matrix, obs_weight, innovation, block_owner, block_row, block_count):
    lat_index = lax.axis_index(LAT)
    lat_total = lax.axis_size(LAT)
    ends = [(lat_index == at).astype(jnp.int32) for at in (0, lat_total - 1)]
    where = jnp.stack([lax.axis_index("lon"), *ends, lax.axis_index("lat_1")]).astype(jnp.int32)
    flow = courant.reshape(-1, LANES)
    owner, row, count = block_owner.reshape(-1), block_row.reshape(-1), block_count.reshape(-1)
    matrix, weight = obs_matrix[0], obs_weight[0]
    wholes = (flow, matrix, weight, innovation[0])
    (small,) = call(
        prepare,
        [(LON * SMALL, LANES)],
        (where, owner, row, count, *wholes),
        1_000_000,
        [pltpu.SMEM((CAP,), jnp.int32), pltpu.SMEM((CAP,), jnp.int32), pltpu.SMEM((1,), jnp.int32)]
        + [pltpu.VMEM(x.shape, F32) for x in wholes]
        + [pltpu.VMEM((OWN, LANES), F32), pltpu.SemaphoreType.DMA((7,))],
        [SMEM] + [pl.BlockSpec(memory_space=pltpu.HBM)] * 7,
        62,
    )
    small = spread_out(small.reshape(LON, SMALL, LANES), "lon").reshape(LON * SMALL, LANES)
    (bulk,) = call(weigh_blocks, [(LON * BULK, LANES)], (owner, row, count, matrix, weight), 4_000_000)
    bulk = spread_out(bulk.reshape(LON, BULK, LANES), "lon").reshape(LON * BULK, LANES)
    up, down = call(arrange, [(MESSAGE, LANES)] * 2, (where, flow, small), 2_000_000)
    below, above = shift(up, LAT, 1, False), shift(down, LAT, -1, False)
    messages = (below, down, up, above)
    cells, listed = (ROWS * LEVELS, LANES), (OWN, LANES)
    work = [pltpu.VMEM((WIDE * LEVELS, LANES), F32)] * 2 + [pltpu.VMEM((WIDE * 8, LANES), F32)] * 2
    image = pltpu.VMEM(cells, F32)
    spots, by_lane, right_side, seen, sums = call(
        first_half, [(2 * LANES, LANES), (16, LANES), cells, listed, (8, LANES)], (where, *messages), 4_000_000, work + [image]
    )
    grams, terms, sums = call(first_terms, [(OWN * LANES, LANES), listed, (8, LANES)], (bulk, seen, sums), 2_000_000)
    own = jnp.concatenate([shift(terms, LAT, 1, False), terms, shift(terms, LAT, -1, False)], axis=0)
    sides = (shift(own, "lon", 1, True), shift(own, "lon", -1, True))
    plane = lax.axis_size(("lat_1", "lon"))
    towers = lax.axis_size(("lat_0", "lat_2"))
    kept, terms, parcels = call(
        second_half,
        [cells, listed, (plane * 2, LANES)],
        (where, spots, by_lane, own, *sides, *messages, grams, sums),
        4_000_000,
        work + [image],
    )
    parcels = spread_out(parcels.reshape(plane, 2, LANES), ("lat_1", "lon")).reshape(plane * 2, LANES)
    sums, mine = call(gathered, [(towers, LANES), (OWN + 8, LANES)], (where, parcels, terms), 10_000)
    south, north = shift(mine, LAT, 1, False), shift(mine, LAT, -1, False)
    parts = spread_out(sums.reshape(towers, 1, LANES), ("lat_0", "lat_2")).reshape(towers, LANES)
    increment, residual = call(
        finish, [cells, cells], (spots, by_lane, south, mine, north, *messages, parts, right_side, kept), 2_000_000, work
    )
    shape = courant.shape[1:]
    return increment.reshape(shape), residual.reshape(shape)


def solution(mesh):
    torus = Mesh(
        mesh.devices.reshape(-1, 4, 2, mesh.shape["lon"]), ("lat_0", "lat_1", "lat_2", "lon")
    )
    placed = (
        P(None, None, LAT, "lon"),
        P(LAT, "lon", None, None),
        P(LAT, "lon", None),
        P(LAT, "lon", None),
        P(LAT, "lon", None),
        P(LAT, "lon"),
        P(LAT, "lon"),
    )
    return jax.shard_map(
        shards,
        mesh=torus,
        in_specs=placed,
        out_specs=(P(None, LAT, "lon"), P(None, LAT, "lon")),
        check_vma=False,
    )
```

```python
import jax
import jax.numpy as jnp
from jax import lax
from jax.experimental import pallas as pl
from jax.experimental.pallas import tpu as pltpu
from jax.sharding import Mesh
from jax.sharding import PartitionSpec as P

LAT = ("lat_0", "lat_1", "lat_2")
LEVELS = 16
ROWS = 16
LANES = 128
CAP = 8
SLOT = 2
STEPS = 4
HALO = 2 * STEPS
WIDE = ROWS + 2 * HALO
LON = 8
HALF = LANES // 2
OWN = LON * SLOT
NEAR = 3 * OWN
BULK = 2 * HALF + 8
LIST = BULK + 8
PARCEL = LIST + 32
EDGE = HALO * 2 * LEVELS
STRIP = HALO * 2 * 8
LEFTS = STRIP + OWN
RIGHTS = LEFTS + OWN
SPOTS = RIGHTS + OWN
MESSAGE = SPOTS + 8
HERALD = OWN + 8
NOWHERE = -4096.0
HIGHEST = lax.Precision.HIGHEST
F32 = jnp.float32
VMEM = pl.BlockSpec(memory_space=pltpu.VMEM)
SMEM = pl.BlockSpec(memory_space=pltpu.SMEM)


def lanes(rows):
    return lax.broadcasted_iota(jnp.int32, (rows, LANES), 1)


def places(rows):
    return lax.broadcasted_iota(jnp.int32, (rows, LANES), 0)


def roll(x, shift):
    shift %= LANES
    return pltpu.roll(x, shift, axis=1) if shift else x


def call(body, outs, args, flops, scratch=(), specs=None, room=24):
    return pl.pallas_call(
        body,
        out_shape=[jax.ShapeDtypeStruct(s, F32) for s in outs],
        in_specs=specs or [SMEM if a.dtype == jnp.int32 else VMEM for a in args],
        out_specs=[VMEM] * len(outs),
        scratch_shapes=list(scratch),
        compiler_params=pltpu.CompilerParams(vmem_limit_bytes=room << 20),
        cost_estimate=pl.CostEstimate(flops=flops, bytes_accessed=0, transcendentals=0),
        name=body.__name__,
    )(*args)


def turns_of(owners):
    return [sum([(o == owners[j]).astype(jnp.int32) for o in owners[:j]], jnp.int32(0)) for j in range(CAP)]


def packed_edges(pick, shift):
    ln = lanes(8)
    out = jnp.zeros((8, LANES), F32)
    for k in range(8):
        low, high = pick(k)
        out = jnp.where((ln >= 16 * k) & (ln < 16 * k + 8), roll(low, 16 * k + shift), out)
        out = jnp.where((ln >= 16 * k + 8) & (ln < 16 * k + 16), roll(high, 16 * k + 8 + shift), out)
    return out


def weigh_blocks(owners, turns, count, matrix, weight, parcels):
    ln, rw = lanes(HALF), places(HALF)
    for j in range(CAP):
        block = matrix[j]
        scaled = jnp.transpose(block) * jnp.where(j < count[0], weight[j : j + 1, :], 0.0)
        gram = jnp.dot(scaled, block, precision=HIGHEST, preferred_element_type=F32)
        top, low = gram[:HALF], gram[HALF:]
        packed = jnp.where((ln >= HALF) & (ln - HALF <= rw), roll(top, HALF), low)
        diagonal = jnp.sum(jnp.where(ln - HALF == rw, low, 0.0), axis=0, keepdims=True)
        at = owners[j] * PARCEL + turns[j] * HALF
        parcels[pl.ds(pl.multiple_of(at, 8), HALF), :] = packed
        parcels[pl.ds(owners[j] * PARCEL + 2 * HALF + turns[j], 1), :] = diagonal


def prepare(owner_at, row_at, count_at, flow_at, matrix_at, weight_at, innovation_at, parcels, to_core, to_inter, owner, row, count, flow, matrix, weight, innovation, lists, sems):
    pairs = ((owner_at, owner), (row_at, row), (count_at, count), (flow_at, flow), (weight_at, weight), (innovation_at, innovation), (matrix_at, matrix))
    copies = [pltpu.make_async_copy(a, b, sems.at[i]) for i, (a, b) in enumerate(pairs)]
    for copy in copies:
        copy.start()
    for d in range(LON):
        parcels[d * PARCEL : d * PARCEL + BULK, :] = jnp.zeros((BULK, LANES), F32)
    lists[...] = jnp.zeros(lists.shape, F32)
    me = lax.axis_index("lon")
    even = lax.axis_index("lat_2") == 0
    to_right = lax.rem(me + 1, LON) * PARCEL + LIST
    to_left = lax.rem(me + LON - 1, LON) * PARCEL + LIST
    copies[3].wait()
    for f in range(2):
        for g in range(2):

            def pick(k, f=f, g=g):
                at = f * LEVELS * ROWS + g * 8 + k
                return flow[pl.ds(at, 8, stride=ROWS), :], flow[pl.ds(at + 8 * ROWS, 8, stride=ROWS), :]

            at = (f * 2 + g) * 8
            parcels[pl.ds(pl.multiple_of(to_right + at, 8), 8), :] = packed_edges(pick, 8)
            parcels[pl.ds(pl.multiple_of(to_left + at, 8), 8), :] = packed_edges(pick, 0)
        for i in range(HALO):
            for h in range(2):
                at = f * LEVELS * ROWS + h * 8 * ROWS + i
                up, down = flow[pl.ds(at + ROWS - HALO, 8, stride=ROWS), :], flow[pl.ds(at, 8, stride=ROWS), :]
                at = (i * 2 + f) * LEVELS + h * 8
                to_core[at : at + 8, :] = jnp.where(even, up, down)
                to_inter[at : at + 8, :] = jnp.where(even, down, up)
    for i in (0, 1, 2, 4, 5, 6):
        copies[i].wait()
    owners = [owner[j] for j in range(CAP)]
    turns = turns_of(owners)
    column = jnp.transpose(weight[...] * innovation[...])
    ln = lanes(8)
    named = jnp.full((8, LANES), NOWHERE, F32)
    for j in range(CAP):
        live = j < count[0]
        total = jnp.zeros((8, LANES), F32)
        for k in range(LANES // 8):
            total += matrix[j, k * 8 : k * 8 + 8, :] * column[k * 8 : k * 8 + 8, j : j + 1]
        slot = owners[j] * SLOT + turns[j]
        lists[pl.ds(slot, 1), :] = jnp.where(live, jnp.sum(total, axis=0, keepdims=True), 0.0)
        place = jnp.where(live, (lax.rem(row[j], ROWS) + HALO) * LEVELS + lax.div(row[j], ROWS), int(NOWHERE)).astype(F32)
        named = jnp.where(ln == slot, place, named)
    weigh_blocks(owners, turns, count, matrix, weight, parcels)
    named = jnp.where(ln < OWN, named, roll(named, OWN))
    line = lanes(1)
    for d in range(LON):
        left, right = 2 * (d - 1) % OWN, 2 * (d + 1) % OWN
        at = d * PARCEL + BULK
        parcels[at : at + 2, :] = lists[2 * d : 2 * d + 2, :]
        edge = jnp.where(line < 8, roll(lists[left : left + 1, :], 8), roll(lists[left + 1 : left + 2, :], 16))
        edge = jnp.where(line < 16, edge, jnp.where(line < 24, roll(lists[right : right + 1, :], 16), roll(lists[right + 1 : right + 2, :], 24)))
        parcels[at + 2 : at + 3, :] = edge
        parcels[at + 3 : at + 4, :] = roll(named, -left)[:1]


def arrange(flow, parcels, core, inter, wide, strips, to_core, to_inter):
    ln = lanes(8)
    me = lax.axis_index("lon")
    even = lax.axis_index("lat_2") == 0
    wide[:EDGE, :] = jnp.where(even, inter[...], core[...])
    wide[EDGE + ROWS * 2 * LEVELS :, :] = jnp.where(even, core[...], inter[...])
    from_left = lax.rem(me + LON - 1, LON) * PARCEL + LIST
    from_right = lax.rem(me + 1, LON) * PARCEL + LIST
    for f in range(2):
        for g in range(2):
            at = (f * 2 + g) * 8
            left = parcels[pl.ds(pl.multiple_of(from_left + at, 8), 8), :]
            right = parcels[pl.ds(pl.multiple_of(from_right + at, 8), 8), :]
            for k in range(8):
                at = f * LEVELS * ROWS + g * 8 + k
                low, high = flow[pl.ds(at, 8, stride=ROWS), :], flow[pl.ds(at + 8 * ROWS, 8, stride=ROWS), :]
                at = EDGE + ((g * 8 + k) * 2 + f) * LEVELS
                wide[at : at + 8, :] = low
                wide[at + 8 : at + 16, :] = high
                a = jnp.where(ln < 8, roll(left, -16 * k), jnp.where(ln < 32, roll(low, 8), jnp.where(ln < 56, roll(low, 56), roll(right, 56 - 16 * k))))
                b = jnp.where(ln < 72, roll(left, 56 - 16 * k), jnp.where(ln < 96, roll(high, 72), jnp.where(ln < 120, roll(high, 120), roll(right, 112 - 16 * k))))
                strip = jnp.where(ln < HALF, a, b)
                at = ((g * 8 + k) * 2 + f) * 8
                strips[at : at + 8, :] = strip
    lower, upper = strips[:STRIP, :], strips[STRIP:, :]
    to_core[:STRIP, :] = jnp.where(even, upper, lower)
    to_inter[:STRIP, :] = jnp.where(even, lower, upper)
    edge = parcels[pl.ds(BULK + 2, LON, stride=PARCEL), :]
    named = parcels[pl.ds(BULK + 3, LON, stride=PARCEL), :]
    turned = jnp.transpose(named)
    spot = jnp.full((1, LANES), NOWHERE, F32)
    line = lanes(1)
    for i, k in enumerate((2, 3, 0, 1, 4, 5)):
        line_k = jnp.concatenate([turned[k : k + 1, :], jnp.zeros((1, LANES - LON), F32)], axis=1)
        spot = jnp.where((line >= 8 * i) & (line < 8 * i + 8), roll(line_k, 8 * i), spot)
    for o in range(SLOT):
        own = parcels[pl.ds(BULK + o, LON, stride=PARCEL), :]
        left = jnp.where(ln < 8, roll(edge, -8 * o), 0.0)
        right = jnp.where((ln >= 56) & (ln < 64), roll(edge, 40 - 8 * o), 0.0)
        for out in (to_core, to_inter):
            out[STRIP + o * LON : STRIP + (o + 1) * LON, :] = own
            out[LEFTS + o * LON : LEFTS + (o + 1) * LON, :] = left
            out[RIGHTS + o * LON : RIGHTS + (o + 1) * LON, :] = right
    for out in (to_core, to_inter):
        out[SPOTS:, :] = jnp.broadcast_to(spot, (8, LANES))


def unpack(parcels, grams):
    ln, rw = lanes(HALF), places(HALF)
    upper, diagonal, first = ln - HALF > rw, ln - HALF == rw, ln < HALF
    for s in range(LON):
        both = parcels[s * PARCEL : s * PARCEL + 2 * HALF, :]
        turned = jnp.transpose(both)
        ct, et = turned[:HALF], turned[HALF:]
        ct_rolled, et_rolled = roll(ct, HALF), roll(et, HALF)
        for o in range(SLOT):
            q = both[o * HALF : (o + 1) * HALF]
            d = parcels[s * PARCEL + 2 * HALF + o : s * PARCEL + 2 * HALF + o + 1, :]
            e_first, e_last = (et, et_rolled) if o == 0 else (et_rolled, et)
            c_last = ct_rolled if o == 0 else ct
            top = jnp.where(first, jnp.where(ln <= rw, roll(q, HALF), e_first), c_last)
            low = jnp.where(first | upper, q, jnp.where(diagonal, d, e_last))
            at = (o * LON + s) * LANES
            grams[at : at + HALF, :] = top
            grams[at + HALF : at + LANES, :] = low


def split(x):
    high = x.astype(jnp.bfloat16)
    rest = x - high.astype(F32)
    middle = rest.astype(jnp.bfloat16)
    low = (rest - middle.astype(F32)).astype(jnp.bfloat16)
    return jnp.concatenate([high, middle, low], axis=1)


def chosen(one_hot, parts):
    out = jnp.dot(one_hot, parts, preferred_element_type=F32)
    return out[:, :LANES] + out[:, LANES : 2 * LANES] + out[:, 2 * LANES :]


def one_hot(index, at):
    return jnp.where(index == at, 1.0, 0.0).astype(jnp.bfloat16)


def padded(x, rows):
    return jnp.concatenate([x, jnp.zeros((rows - x.shape[0], LANES), F32)], axis=0)


def left_strips(x):
    return jnp.where(lanes(x.shape[0]) < 8, roll(x, 8), 0.0)


def right_strips(x):
    ln = lanes(x.shape[0])
    return jnp.where((ln >= 56) & (ln < 64), roll(x, 56), 0.0)


def lay_out(spots, by_lane, own, sides, field, strips, low, high):
    ln = lanes(LANES)
    own_strip = jnp.where(ln < 32, jnp.where(ln >= 8, roll(own, 8), 0.0), jnp.where(ln < 56, roll(own, 56), 0.0))
    pieces = []
    for i, strip in enumerate((own_strip, sides)):
        upper = (spots[i * LANES : (i + 1) * LANES, :].astype(jnp.int32) & 8) != 0
        pieces.append(split(jnp.where(upper, roll(strip, HALF), strip)))
    own_parts = split(own)
    lane_spots = [by_lane[i * 8 : i * 8 + 1, :].astype(jnp.int32) for i in range(2)]
    p = jnp.broadcast_to(lane_spots[0], (LANES, LANES))
    for start in range(low * LEVELS, high * LEVELS, LANES):
        field[start : start + LANES, :] = chosen(one_hot(places(LANES) + start, p), own_parts)
    folded = [jnp.broadcast_to(((b >> 4) << 3) + (b & 7), (64, LANES)) for b in lane_spots]
    for start in range(low * 8, high * 8, 64):
        at = places(64) + start
        strips[start : start + 64, :] = chosen(one_hot(at, folded[0]), pieces[0]) + chosen(one_hot(at, folded[1]), pieces[1])


def adjoint(rates, source, target, first, last, height):
    before = kept = None
    for r in range(first, last + 1):
        y = source[r * height : (r + 1) * height, :]
        lat, lon = rates(r)
        t = lat * y
        a = jnp.where(lat > 0.0, t, 0.0)
        b = a - t
        s = lon * y
        e = jnp.where(lon > 0.0, s, 0.0)
        f = e - s
        if r > first + 1:
            target[(r - 1) * height : r * height, :] = kept + a
        if r > first:
            kept = y - (a + b) - (e + f) + roll(e, -1) + roll(f, 1) + before
        before = b


def tangent(rates, source, target, first, last, height):
    for r in range(first + 1, last):
        x = source[r * height : (r + 1) * height, :]
        south = source[(r - 1) * height : r * height, :]
        north = source[(r + 1) * height : (r + 2) * height, :]
        lat, lon = rates(r)
        out = x + jnp.abs(lat) * (jnp.where(lat > 0.0, south, north) - x)
        target[r * height : (r + 1) * height, :] = out + jnp.abs(lon) * (jnp.where(lon > 0.0, roll(x, 1), roll(x, -1)) - x)


def merged(field, strips, r):
    ln = lanes(8)
    t = strips[r * 8 : (r + 1) * 8, :]
    low, high = field[r * LEVELS : r * LEVELS + 8, :], field[r * LEVELS + 8 : (r + 1) * LEVELS, :]
    low = jnp.where(ln < 8, roll(t, -8), jnp.where(ln >= 120, roll(t, 72), low))
    high = jnp.where(ln < 8, roll(t, -72), jnp.where(ln >= 120, roll(t, 8), high))
    return low, high


def steps_back(rates, fields, strips, first):
    full, narrow = rates
    for k in range(first, first + STEPS):
        adjoint(full, *fields, k, WIDE - 1 - k, LEVELS)
        adjoint(narrow, *strips, k, WIDE - 1 - k, 8)
        fields, strips = fields[::-1], strips[::-1]
    return fields, strips


def steps_on(rates, fields, strips, first):
    full, narrow = rates
    for k in range(first, first + STEPS):
        tangent(full, *fields, k, WIDE - 1 - k, LEVELS)
        tangent(narrow, *strips, k, WIDE - 1 - k, 8)
        fields, strips = fields[::-1], strips[::-1]
    return fields, strips


def rates_of(wide, mine, beside):
    def full(r):
        at = r * 2 * LEVELS
        return wide[at : at + LEVELS, :], wide[at + LEVELS : at + 2 * LEVELS, :]

    def narrow(r):
        ref, r = (mine, r - HALO) if HALO <= r < HALO + ROWS else (beside, r if r < HALO else r - ROWS)
        return ref[r * 16 : r * 16 + 8, :], ref[r * 16 + 8 : r * 16 + 16, :]

    return full, narrow


def back_and_on(spots, by_lane, own, sides, rates, kept, fields, strips, image):
    lay_out(spots, by_lane, own, sides, fields[0], strips[0], 0, WIDE)
    fields, strips = steps_back(rates, fields, strips, 0)
    lat, last = lax.axis_index(LAT), lax.axis_size(LAT) - 1
    for outside, start in ((lat == 0, STEPS), (lat == last, HALO + ROWS)):
        for ref, height in ((fields[0], LEVELS), (strips[0], 8)):
            block = ref[start * height : (start + STEPS) * height, :]
            ref[start * height : (start + STEPS) * height, :] = jnp.where(outside, 0.0, block)
    square = jnp.zeros((8, LANES), F32)
    for r in range(ROWS):
        low, high = merged(fields[0], strips[0], r + HALO)
        kept[r * LEVELS : r * LEVELS + 8, :] = low
        kept[r * LEVELS + 8 : (r + 1) * LEVELS, :] = high
        square += low * low + high * high
    fields, strips = steps_on(rates, fields, strips, STEPS)
    for r in range(ROWS):
        low, high = merged(fields[0], strips[0], r + HALO)
        image[r * LEVELS : r * LEVELS + 8, :] = low
        image[r * LEVELS + 8 : (r + 1) * LEVELS, :] = high
    mine = spots[OWN : 2 * OWN, :].astype(jnp.int32) - HALO * LEVELS
    hit = jnp.concatenate([one_hot(lanes(OWN), mine), one_hot(lanes(OWN) + LANES, mine)], axis=1)
    return jnp.sum(square, keepdims=True), chosen(hit, split(image[...]))


def weigh(seen, grams):
    column = jnp.transpose(seen)
    out = []
    for t in range(OWN):
        total = jnp.zeros((8, LANES), F32)
        for k in range(LANES // 8):
            at = t * LANES + k * 8
            total += grams[at : at + 8, :] * column[k * 8 : k * 8 + 8, t : t + 1]
        out.append(jnp.sum(total, axis=0, keepdims=True))
    return jnp.concatenate(out, axis=0)


def in_lanes(first, values):
    ln = lanes(8)
    out = jnp.zeros((8, LANES), F32)
    for i, v in enumerate(values):
        out = jnp.where(ln == first + i, v, out)
    return out


def first_half(wide, mine, core, own_message, inter, beside, spots, by_lane, kept, seen, sums, field, other, strip, other_strip, image):
    ln = lanes(8)
    even = lax.axis_index("lat_2") == 0
    beside[:STRIP, :] = jnp.where(even, inter[:STRIP, :], core[:STRIP, :])
    beside[STRIP:, :] = jnp.where(even, core[:STRIP, :], inter[:STRIP, :])
    step = jnp.where(even, float(ROWS * LEVELS), -float(ROWS * LEVELS))
    c, o, i = core[SPOTS:, :] + step, own_message[SPOTS:, :], inter[SPOTS:, :] - step
    tables = (((c, 0), (o, 0), (i, 0)), ((c, 16), (o, 16), (i, 16), (c, 32), (o, 32), (i, 32)))
    for t, table in enumerate(tables):
        spot = jnp.full((8, LANES), NOWHERE, F32)
        for n, (x, at) in enumerate(table):
            spot = jnp.where((ln >= OWN * n) & (ln < OWN * (n + 1)), roll(x, OWN * n - at), spot)
        by_lane[t * 8 : t * 8 + 8, :] = spot
        spots[t * LANES : (t + 1) * LANES, :] = jnp.transpose(jnp.broadcast_to(spot[:1], (LANES, LANES)))
    parts = (core, own_message, inter)
    own = padded(jnp.concatenate([x[STRIP:LEFTS, :] for x in parts], axis=0), LANES)
    sides = padded(jnp.concatenate([x[LEFTS:RIGHTS, :] for x in parts] + [x[RIGHTS:SPOTS, :] for x in parts], axis=0), LANES)
    square, rows = back_and_on(spots, by_lane, own, sides, rates_of(wide, mine, beside), kept, (field, other), (strip, other_strip), image)
    seen[...] = rows
    sums[...] = in_lanes(0, [square])


def stepped(x, unit):
    row = places(OWN)
    for bit in range(4):
        x = jnp.where((row & (1 << bit)) != 0, roll(x, unit << bit), x)
    return x


def herald(rows, message):
    mine = (lanes(OWN) >> 3) == places(OWN)
    message[:OWN, :] = rows
    message[OWN : OWN + 1, :] = jnp.sum(jnp.where(mine, stepped(rows, 8), 0.0), axis=0, keepdims=True)
    message[OWN + 1 : OWN + 2, :] = jnp.sum(jnp.where(mine, stepped(roll(rows, 8), 8), 0.0), axis=0, keepdims=True)
    message[OWN + 2 :, :] = jnp.zeros((HERALD - OWN - 2, LANES), F32)


def first_terms(parcels, seen, before, grams, message, sums):
    unpack(parcels, grams)
    rows = weigh(seen[...], grams)
    herald(rows, message)
    sums[...] = before[...] + in_lanes(1, [jnp.sum(seen[...] * rows, keepdims=True)])


def near(core, step):
    here = lax.axis_index("lat_2")
    return (here if core else 1 - here) * LON + lax.rem(lax.axis_index("lon") + LON + step, LON)


def address(mine, inter, parcels):
    parcels[...] = jnp.zeros(parcels.shape, F32)
    parcels[pl.ds(pl.multiple_of(near(False, 0) * OWN, OWN), OWN), :] = mine[:OWN, :]
    for step, row in ((1, OWN + 1), (-1, OWN)):
        parcels[pl.ds(near(True, step) * OWN, 1), :] = mine[row : row + 1, :]
        parcels[pl.ds(near(True, step) * OWN + 1, 1), :] = inter[row : row + 1, :]
        parcels[pl.ds(near(False, step) * OWN, 1), :] = mine[row : row + 1, :]


def side_strips(lefts, rights):
    ln = lanes(OWN)
    rows = [stepped(jnp.broadcast_to(x, (OWN, LANES)), -8) for x in lefts]
    out = [jnp.where(ln < 8, x, 0.0) for x in rows]
    rows = [stepped(jnp.broadcast_to(x, (OWN, LANES)), -8) for x in rights]
    return padded(jnp.concatenate(out + [right_strips(x) for x in rows], axis=0), LANES)


def second_half(spots, by_lane, mine, inter, parcels, wide, strips, beside, grams, before, kept, message, out, field, other, strip, other_strip, image):
    core = parcels[pl.ds(pl.multiple_of(near(False, 0) * OWN, OWN), OWN), :]
    own = padded(jnp.concatenate([core, mine[:OWN, :], inter[:OWN, :]], axis=0), LANES)
    edges = [
        [parcels[pl.ds(near(here, step) * OWN + row, 1), :] for here, row in ((False, 0), (True, 0), (True, 1))]
        for step in (-1, 1)
    ]
    square, seen = back_and_on(
        spots, by_lane, own, side_strips(*edges), rates_of(wide, strips, beside), kept, (field, other), (strip, other_strip), image
    )
    rows = weigh(seen, grams)
    herald(rows, message)
    sums = before[...] + in_lanes(2, [square, jnp.sum(seen * rows, keepdims=True)])
    out[...] = jnp.concatenate([sums] * (out.shape[0] // 8), axis=0)
    for step, row in ((1, OWN + 1), (-1, OWN)):
        out[pl.ds(in_plane(step) * 2 + 1, 1), :] = message[row : row + 1, :]


def in_plane(step):
    return lax.axis_index("lat_1") * LON + lax.rem(lax.axis_index("lon") + LON + step, LON)


def gathered(parts, mine, sums, message):
    count = parts.shape[0] // 2
    sums[...] = jnp.broadcast_to(jnp.sum(parts[pl.ds(0, count, stride=2), :], axis=0, keepdims=True), sums.shape)
    message[...] = mine[...]
    for i, step in enumerate((-1, 1)):
        message[OWN + i : OWN + i + 1, :] = parts[pl.ds(in_plane(step) * 2 + 1, 1), :]


def finish(spots, by_lane, core, mine, inter, wide, strips, beside, parts, right_side, image, increment, residual, field, other, strip, other_strip):
    lists = (core, mine, inter)
    own = padded(jnp.concatenate([x[:OWN, :] for x in lists], axis=0), LANES)
    sides = side_strips(*([x[OWN + i : OWN + i + 1, :] for x in lists] for i in range(2)))
    lay_out(spots, by_lane, own, sides, field, strip, HALO - STEPS, HALO + ROWS + STEPS)
    fields, narrow = steps_back(rates_of(wide, strips, beside), (field, other), (strip, other_strip), STEPS)
    total = jnp.sum(parts[...], axis=0, keepdims=True)
    m0, m1, m2, m3 = (jnp.sum(jnp.where(lanes(1) == i, total, 0.0), keepdims=True) for i in range(4))
    step_0 = m0 / (m0 + m1)
    rho = m1 / m0
    spread = m2 - rho * m1
    curve = (m3 - rho * m2) - rho * (m2 - rho * m1)
    gamma = step_0 * spread / m0
    step_1 = spread / (spread + curve - gamma * spread)
    on_b = step_0 * (1.0 + step_1 * (gamma + rho))
    on_k = -step_0 * step_1
    rest_b = step_0 * ((1.0 - step_1) * rho - step_1 * gamma)
    rest_k = -step_0 * ((1.0 - step_1) + step_1 * (rho + gamma))
    rest_kk = step_0 * step_1
    on_b, on_k, rest_b, rest_k, rest_kk = (jnp.broadcast_to(v, (8, LANES)) for v in (on_b, on_k, rest_b, rest_k, rest_kk))
    for r in range(ROWS):
        for h, second in enumerate(merged(fields[0], narrow[0], r + HALO)):
            at = r * LEVELS + h * 8
            b, first = right_side[at : at + 8, :], image[at : at + 8, :]
            to = pl.ds(h * 8 * ROWS + r, 8, stride=ROWS)
            increment[to, :] = on_b * b + on_k * first
            residual[to, :] = rest_b * b + rest_k * first + rest_kk * second


def to_core(x):
    return lax.ppermute(x, LAT, [(i, i ^ 1) for i in range(lax.axis_size(LAT))])


def to_inter(x):
    return lax.ppermute(x, LAT, [(i, ((i + 1) ^ 1) - 1) for i in range(1, lax.axis_size(LAT) - 1)])


def spread_out(x, axes):
    return lax.all_to_all(x, axes, split_axis=0, concat_axis=0, tiled=True)


def shards(courant, obs_matrix, obs_weight, innovation, block_owner, block_row, block_count):
    flow = courant.reshape(-1, LANES)
    owner, row, count = block_owner.reshape(-1), block_row.reshape(-1), block_count.reshape(-1)
    wholes = (flow, obs_matrix[0], obs_weight[0], innovation[0])
    parcels, for_core, for_inter = call(
        prepare,
        [(LON * PARCEL, LANES), (EDGE, LANES), (EDGE, LANES)],
        (owner, row, count, *wholes),
        4_000_000,
        [pltpu.SMEM((CAP,), jnp.int32), pltpu.SMEM((CAP,), jnp.int32), pltpu.SMEM((1,), jnp.int32)]
        + [pltpu.VMEM(x.shape, F32) for x in wholes]
        + [pltpu.VMEM((OWN, LANES), F32), pltpu.SemaphoreType.DMA((7,))],
        [pl.BlockSpec(memory_space=pltpu.HBM)] * 7,
        62,
    )
    parcels = spread_out(parcels.reshape(LON, PARCEL, LANES), "lon").reshape(LON * PARCEL, LANES)
    core, inter = to_core(for_core), to_inter(for_inter)
    wide, strips, for_core, for_inter = call(
        arrange,
        [(WIDE * 2 * LEVELS, LANES), (2 * STRIP, LANES), (MESSAGE, LANES), (MESSAGE, LANES)],
        (flow, parcels, core, inter),
        2_000_000,
    )
    core, inter = to_core(for_core), to_inter(for_inter)
    cells, listed = (ROWS * LEVELS, LANES), (OWN, LANES)
    work = [pltpu.VMEM((WIDE * LEVELS, LANES), F32)] * 2 + [pltpu.VMEM((WIDE * 8, LANES), F32)] * 2
    work_too = work + [pltpu.VMEM(cells, F32)]
    beside, spots, by_lane, right_side, seen, sums = call(
        first_half,
        [(2 * STRIP, LANES), (2 * LANES, LANES), (16, LANES), cells, listed, (8, LANES)],
        (wide, strips, core, for_core, inter),
        4_000_000,
        work_too,
    )
    rates = (wide, strips, beside)
    short = (HERALD, LANES)
    grams, mine, sums = call(first_terms, [(OWN * LANES, LANES), short, (8, LANES)], (parcels, seen, sums), 2_000_000)
    inter = to_inter(mine)
    ring = lax.axis_size(("lat_2", "lon"))
    (parcels,) = call(address, [(ring * OWN, LANES)], (mine, inter), 10_000)
    parcels = spread_out(parcels.reshape(ring, OWN, LANES), ("lat_2", "lon")).reshape(ring * OWN, LANES)
    plane, towers = lax.axis_size(("lat_1", "lon")), lax.axis_size(("lat_0", "lat_2"))
    image, mine, parcels = call(
        second_half, [cells, short, (plane * 2, LANES)], (spots, by_lane, mine, inter, parcels, *rates, grams, sums), 4_000_000, work_too
    )
    parcels = spread_out(parcels.reshape(plane, 2, LANES), ("lat_1", "lon")).reshape(plane * 2, LANES)
    sums, mine = call(gathered, [(towers, LANES), short], (parcels, mine), 10_000)
    core, inter = to_core(mine), to_inter(mine)
    parts = spread_out(sums.reshape(towers, 1, LANES), ("lat_0", "lat_2")).reshape(towers, LANES)
    increment, residual = call(
        finish, [cells, cells], (spots, by_lane, core, mine, inter, *rates, parts, right_side, image), 2_000_000, work
    )
    shape = courant.shape[1:]
    return increment.reshape(shape), residual.reshape(shape)


def solution(mesh):
    torus = Mesh(
        mesh.devices.reshape(-1, 4, 2, mesh.shape["lon"]), ("lat_0", "lat_1", "lat_2", "lon")
    )
    placed = (
        P(None, None, LAT, "lon"),
        P(LAT, "lon", None, None),
        P(LAT, "lon", None),
        P(LAT, "lon", None),
        P(LAT, "lon", None),
        P(LAT, "lon"),
        P(LAT, "lon"),
    )
    return jax.shard_map(
        shards,
        mesh=torus,
        in_specs=placed,
        out_specs=(P(None, LAT, "lon"), P(None, LAT, "lon")),
        check_vma=False,
    )
```

```python
import jax
import jax.numpy as jnp
from jax import lax
from jax.experimental import pallas as pl
from jax.experimental.pallas import tpu as pltpu
from jax.sharding import Mesh
from jax.sharding import PartitionSpec as P

LAT = ("lat_0", "lat_1", "lat_2")
LEVELS = 16
ROWS = 16
LANES = 128
CAP = 8
SLOT = 2
STEPS = 4
HALO = 2 * STEPS
WIDE = ROWS + 2 * HALO
LON = 8
HALF = LANES // 2
OWN = LON * SLOT
NEAR = 3 * OWN
BULK = 2 * HALF + 2
LIST = BULK + 6
PARCEL = LIST + 32
EDGE = HALO * 2 * LEVELS
STRIP = HALO * 2 * 8
LEFTS = STRIP + OWN
RIGHTS = LEFTS + OWN
SPOTS = RIGHTS + OWN
MESSAGE = SPOTS + 8
HERALD = OWN + 8
NOWHERE = -4096.0
HIGHEST = lax.Precision.HIGHEST
F32 = jnp.float32
VMEM = pl.BlockSpec(memory_space=pltpu.VMEM)
SMEM = pl.BlockSpec(memory_space=pltpu.SMEM)


def lanes(rows):
    return lax.broadcasted_iota(jnp.int32, (rows, LANES), 1)


def places(rows):
    return lax.broadcasted_iota(jnp.int32, (rows, LANES), 0)


def roll(x, shift):
    shift %= LANES
    return pltpu.roll(x, shift, axis=1) if shift else x


def call(body, outs, args, flops, scratch=(), specs=None, room=24):
    return pl.pallas_call(
        body,
        out_shape=[jax.ShapeDtypeStruct(s, F32) for s in outs],
        in_specs=specs or [SMEM if a.dtype == jnp.int32 else VMEM for a in args],
        out_specs=[VMEM] * len(outs),
        scratch_shapes=list(scratch),
        compiler_params=pltpu.CompilerParams(vmem_limit_bytes=room << 20),
        cost_estimate=pl.CostEstimate(flops=flops, bytes_accessed=0, transcendentals=0),
        name=body.__name__,
    )(*args)


def turns_of(owners):
    return [sum([(o == owners[j]).astype(jnp.int32) for o in owners[:j]], jnp.int32(0)) for j in range(CAP)]


def packed_edges(pick, shift):
    ln = lanes(8)
    out = jnp.zeros((8, LANES), F32)
    for k in range(8):
        low, high = pick(k)
        out = jnp.where((ln >= 16 * k) & (ln < 16 * k + 8), roll(low, 16 * k + shift), out)
        out = jnp.where((ln >= 16 * k + 8) & (ln < 16 * k + 16), roll(high, 16 * k + 8 + shift), out)
    return out


def weigh_blocks(owners, turns, count, matrix, weight, parcels):
    ln, rw = lanes(HALF), places(HALF)
    for j in range(CAP):
        block = matrix[j]
        scaled = jnp.transpose(block) * jnp.where(j < count[0], weight[j : j + 1, :], 0.0)
        gram = jnp.dot(scaled, block, precision=HIGHEST, preferred_element_type=F32)
        top, low = gram[:HALF], gram[HALF:]
        packed = jnp.where((ln >= HALF) & (ln - HALF <= rw), roll(top, HALF), low)
        diagonal = jnp.sum(jnp.where(ln - HALF == rw, low, 0.0), axis=0, keepdims=True)
        at = owners[j] * PARCEL + turns[j] * HALF
        parcels[pl.ds(pl.multiple_of(at, 8), HALF), :] = packed
        parcels[pl.ds(owners[j] * PARCEL + 2 * HALF + turns[j], 1), :] = diagonal


def prepare(owner_at, row_at, count_at, flow_at, matrix_at, weight_at, innovation_at, parcels, to_core, to_inter, owner, row, count, flow, matrix, weight, innovation, lists, sems):
    pairs = ((owner_at, owner), (row_at, row), (count_at, count), (flow_at, flow), (weight_at, weight), (innovation_at, innovation), (matrix_at, matrix))
    copies = [pltpu.make_async_copy(a, b, sems.at[i]) for i, (a, b) in enumerate(pairs)]
    for copy in copies:
        copy.start()
    for d in range(LON):
        parcels[d * PARCEL : d * PARCEL + LIST, :] = jnp.zeros((LIST, LANES), F32)
    lists[...] = jnp.zeros(lists.shape, F32)
    me = lax.axis_index("lon")
    even = lax.axis_index("lat_2") == 0
    to_right = lax.rem(me + 1, LON) * PARCEL + LIST
    to_left = lax.rem(me + LON - 1, LON) * PARCEL + LIST
    copies[3].wait()
    for f in range(2):
        for g in range(2):

            def pick(k, f=f, g=g):
                at = f * LEVELS * ROWS + g * 8 + k
                return flow[pl.ds(at, 8, stride=ROWS), :], flow[pl.ds(at + 8 * ROWS, 8, stride=ROWS), :]

            at = (f * 2 + g) * 8
            parcels[pl.ds(pl.multiple_of(to_right + at, 8), 8), :] = packed_edges(pick, 8)
            parcels[pl.ds(pl.multiple_of(to_left + at, 8), 8), :] = packed_edges(pick, 0)
        for i in range(HALO):
            for h in range(2):
                at = f * LEVELS * ROWS + h * 8 * ROWS + i
                up, down = flow[pl.ds(at + ROWS - HALO, 8, stride=ROWS), :], flow[pl.ds(at, 8, stride=ROWS), :]
                at = (i * 2 + f) * LEVELS + h * 8
                to_core[at : at + 8, :] = jnp.where(even, up, down)
                to_inter[at : at + 8, :] = jnp.where(even, down, up)
    for i in (0, 1, 2, 4, 5, 6):
        copies[i].wait()
    owners = [owner[j] for j in range(CAP)]
    turns = turns_of(owners)
    column = jnp.transpose(weight[...] * innovation[...])
    ln = lanes(8)
    named = jnp.full((8, LANES), NOWHERE, F32)
    for j in range(CAP):
        live = j < count[0]
        total = jnp.zeros((8, LANES), F32)
        for k in range(LANES // 8):
            total += matrix[j, k * 8 : k * 8 + 8, :] * column[k * 8 : k * 8 + 8, j : j + 1]
        slot = owners[j] * SLOT + turns[j]
        lists[pl.ds(slot, 1), :] = jnp.where(live, jnp.sum(total, axis=0, keepdims=True), 0.0)
        place = jnp.where(live, (lax.rem(row[j], ROWS) + HALO) * LEVELS + lax.div(row[j], ROWS), int(NOWHERE)).astype(F32)
        named = jnp.where(ln == slot, place, named)
    weigh_blocks(owners, turns, count, matrix, weight, parcels)
    named = jnp.where(ln < OWN, named, roll(named, OWN))
    line = lanes(1)
    for d in range(LON):
        left, right = 2 * (d - 1) % OWN, 2 * (d + 1) % OWN
        at = d * PARCEL + BULK
        parcels[at : at + 2, :] = lists[2 * d : 2 * d + 2, :]
        edge = jnp.where(line < 8, roll(lists[left : left + 1, :], 8), roll(lists[left + 1 : left + 2, :], 16))
        edge = jnp.where(line < 16, edge, jnp.where(line < 24, roll(lists[right : right + 1, :], 16), roll(lists[right + 1 : right + 2, :], 24)))
        parcels[at + 2 : at + 3, :] = edge
        parcels[at + 3 : at + 4, :] = roll(named, -left)[:1]


def arrange(flow, parcels, core, inter, wide, strips, to_core, to_inter):
    ln = lanes(8)
    me = lax.axis_index("lon")
    even = lax.axis_index("lat_2") == 0
    wide[:EDGE, :] = jnp.where(even, inter[...], core[...])
    wide[EDGE + ROWS * 2 * LEVELS :, :] = jnp.where(even, core[...], inter[...])
    from_left = lax.rem(me + LON - 1, LON) * PARCEL + LIST
    from_right = lax.rem(me + 1, LON) * PARCEL + LIST
    for f in range(2):
        for g in range(2):
            at = (f * 2 + g) * 8
            left = parcels[pl.ds(pl.multiple_of(from_left + at, 8), 8), :]
            right = parcels[pl.ds(pl.multiple_of(from_right + at, 8), 8), :]
            for k in range(8):
                at = f * LEVELS * ROWS + g * 8 + k
                low, high = flow[pl.ds(at, 8, stride=ROWS), :], flow[pl.ds(at + 8 * ROWS, 8, stride=ROWS), :]
                at = EDGE + ((g * 8 + k) * 2 + f) * LEVELS
                wide[at : at + 8, :] = low
                wide[at + 8 : at + 16, :] = high
                a = jnp.where(ln < 8, roll(left, -16 * k), jnp.where(ln < 32, roll(low, 8), jnp.where(ln < 56, roll(low, 56), roll(right, 56 - 16 * k))))
                b = jnp.where(ln < 72, roll(left, 56 - 16 * k), jnp.where(ln < 96, roll(high, 72), jnp.where(ln < 120, roll(high, 120), roll(right, 112 - 16 * k))))
                strip = jnp.where(ln < HALF, a, b)
                at = ((g * 8 + k) * 2 + f) * 8
                strips[at : at + 8, :] = strip
    lower, upper = strips[:STRIP, :], strips[STRIP:, :]
    to_core[:STRIP, :] = jnp.where(even, upper, lower)
    to_inter[:STRIP, :] = jnp.where(even, lower, upper)
    edge = parcels[pl.ds(BULK + 2, LON, stride=PARCEL), :]
    named = parcels[pl.ds(BULK + 3, LON, stride=PARCEL), :]
    turned = jnp.transpose(named)
    spot = jnp.full((1, LANES), NOWHERE, F32)
    line = lanes(1)
    for i, k in enumerate((2, 3, 0, 1, 4, 5)):
        line_k = jnp.concatenate([turned[k : k + 1, :], jnp.zeros((1, LANES - LON), F32)], axis=1)
        spot = jnp.where((line >= 8 * i) & (line < 8 * i + 8), roll(line_k, 8 * i), spot)
    for o in range(SLOT):
        own = parcels[pl.ds(BULK + o, LON, stride=PARCEL), :]
        left = jnp.where(ln < 8, roll(edge, -8 * o), 0.0)
        right = jnp.where((ln >= 56) & (ln < 64), roll(edge, 40 - 8 * o), 0.0)
        for out in (to_core, to_inter):
            out[STRIP + o * LON : STRIP + (o + 1) * LON, :] = own
            out[LEFTS + o * LON : LEFTS + (o + 1) * LON, :] = left
            out[RIGHTS + o * LON : RIGHTS + (o + 1) * LON, :] = right
    for out in (to_core, to_inter):
        out[SPOTS:, :] = jnp.broadcast_to(spot, (8, LANES))


def unpack(parcels, grams):
    ln, rw = lanes(HALF), places(HALF)
    upper, diagonal, first = ln - HALF > rw, ln - HALF == rw, ln < HALF
    for s in range(LON):
        both = parcels[s * PARCEL : s * PARCEL + 2 * HALF, :]
        turned = jnp.transpose(both)
        ct, et = turned[:HALF], turned[HALF:]
        ct_rolled, et_rolled = roll(ct, HALF), roll(et, HALF)
        for o in range(SLOT):
            q = both[o * HALF : (o + 1) * HALF]
            d = parcels[s * PARCEL + 2 * HALF + o : s * PARCEL + 2 * HALF + o + 1, :]
            e_first, e_last = (et, et_rolled) if o == 0 else (et_rolled, et)
            c_last = ct_rolled if o == 0 else ct
            top = jnp.where(first, jnp.where(ln <= rw, roll(q, HALF), e_first), c_last)
            low = jnp.where(first | upper, q, jnp.where(diagonal, d, e_last))
            at = (o * LON + s) * LANES
            grams[at : at + HALF, :] = top
            grams[at + HALF : at + LANES, :] = low


def split(x):
    high = x.astype(jnp.bfloat16)
    rest = x - high.astype(F32)
    middle = rest.astype(jnp.bfloat16)
    low = (rest - middle.astype(F32)).astype(jnp.bfloat16)
    return jnp.concatenate([high, middle, low], axis=1)


def chosen(one_hot, parts):
    out = jnp.dot(one_hot, parts, preferred_element_type=F32)
    return out[:, :LANES] + out[:, LANES : 2 * LANES] + out[:, 2 * LANES :]


def one_hot(index, at):
    return jnp.where(index == at, 1.0, 0.0).astype(jnp.bfloat16)


def padded(x, rows):
    return jnp.concatenate([x, jnp.zeros((rows - x.shape[0], LANES), F32)], axis=0)


def left_strips(x):
    return jnp.where(lanes(x.shape[0]) < 8, roll(x, 8), 0.0)


def right_strips(x):
    ln = lanes(x.shape[0])
    return jnp.where((ln >= 56) & (ln < 64), roll(x, 56), 0.0)


def lay_out(spots, by_lane, own, sides, field, strips, low, high):
    ln = lanes(LANES)
    own_strip = jnp.where(ln < 32, jnp.where(ln >= 8, roll(own, 8), 0.0), jnp.where(ln < 56, roll(own, 56), 0.0))
    pieces = []
    for i, strip in enumerate((own_strip, sides)):
        upper = (spots[i * LANES : (i + 1) * LANES, :].astype(jnp.int32) & 8) != 0
        pieces.append(split(jnp.where(upper, roll(strip, HALF), strip)))
    own_parts = split(own)
    lane_spots = [by_lane[i * 8 : i * 8 + 1, :].astype(jnp.int32) for i in range(2)]
    p = jnp.broadcast_to(lane_spots[0], (LANES, LANES))
    for start in range(low * LEVELS, high * LEVELS, LANES):
        field[start : start + LANES, :] = chosen(one_hot(places(LANES) + start, p), own_parts)
    folded = [jnp.broadcast_to(((b >> 4) << 3) + (b & 7), (64, LANES)) for b in lane_spots]
    for start in range(low * 8, high * 8, 64):
        at = places(64) + start
        strips[start : start + 64, :] = chosen(one_hot(at, folded[0]), pieces[0]) + chosen(one_hot(at, folded[1]), pieces[1])


def adjoint(rates, source, target, first, last, height):
    before = kept = None
    for r in range(first, last + 1):
        y = source[r * height : (r + 1) * height, :]
        lat, lon = rates(r)
        t = lat * y
        a = jnp.where(lat > 0.0, t, 0.0)
        b = a - t
        s = lon * y
        e = jnp.where(lon > 0.0, s, 0.0)
        f = e - s
        if r > first + 1:
            target[(r - 1) * height : r * height, :] = kept + a
        if r > first:
            kept = y - (a + b) - (e + f) + roll(e, -1) + roll(f, 1) + before
        before = b


def tangent(rates, source, target, first, last, height):
    for r in range(first + 1, last):
        x = source[r * height : (r + 1) * height, :]
        south = source[(r - 1) * height : r * height, :]
        north = source[(r + 1) * height : (r + 2) * height, :]
        lat, lon = rates(r)
        out = x + jnp.abs(lat) * (jnp.where(lat > 0.0, south, north) - x)
        target[r * height : (r + 1) * height, :] = out + jnp.abs(lon) * (jnp.where(lon > 0.0, roll(x, 1), roll(x, -1)) - x)


def merged(field, strips, r):
    ln = lanes(8)
    t = strips[r * 8 : (r + 1) * 8, :]
    low, high = field[r * LEVELS : r * LEVELS + 8, :], field[r * LEVELS + 8 : (r + 1) * LEVELS, :]
    low = jnp.where(ln < 8, roll(t, -8), jnp.where(ln >= 120, roll(t, 72), low))
    high = jnp.where(ln < 8, roll(t, -72), jnp.where(ln >= 120, roll(t, 8), high))
    return low, high


def steps_back(rates, fields, strips, first):
    full, narrow = rates
    for k in range(first, first + STEPS):
        adjoint(full, *fields, k, WIDE - 1 - k, LEVELS)
        adjoint(narrow, *strips, k, WIDE - 1 - k, 8)
        fields, strips = fields[::-1], strips[::-1]
    return fields, strips


def steps_on(rates, fields, strips, first):
    full, narrow = rates
    for k in range(first, first + STEPS):
        tangent(full, *fields, k, WIDE - 1 - k, LEVELS)
        tangent(narrow, *strips, k, WIDE - 1 - k, 8)
        fields, strips = fields[::-1], strips[::-1]
    return fields, strips


def rates_of(wide, mine, beside):
    def full(r):
        at = r * 2 * LEVELS
        return wide[at : at + LEVELS, :], wide[at + LEVELS : at + 2 * LEVELS, :]

    def narrow(r):
        ref, r = (mine, r - HALO) if HALO <= r < HALO + ROWS else (beside, r if r < HALO else r - ROWS)
        return ref[r * 16 : r * 16 + 8, :], ref[r * 16 + 8 : r * 16 + 16, :]

    return full, narrow


def back_and_on(spots, by_lane, own, sides, rates, kept, fields, strips, image):
    lay_out(spots, by_lane, own, sides, fields[0], strips[0], 0, WIDE)
    fields, strips = steps_back(rates, fields, strips, 0)
    lat, last = lax.axis_index(LAT), lax.axis_size(LAT) - 1
    for outside, start in ((lat == 0, STEPS), (lat == last, HALO + ROWS)):
        for ref, height in ((fields[0], LEVELS), (strips[0], 8)):
            block = ref[start * height : (start + STEPS) * height, :]
            ref[start * height : (start + STEPS) * height, :] = jnp.where(outside, 0.0, block)
    square = jnp.zeros((8, LANES), F32)
    for r in range(ROWS):
        low, high = merged(fields[0], strips[0], r + HALO)
        kept[r * LEVELS : r * LEVELS + 8, :] = low
        kept[r * LEVELS + 8 : (r + 1) * LEVELS, :] = high
        square += low * low + high * high
    fields, strips = steps_on(rates, fields, strips, STEPS)
    for r in range(ROWS):
        low, high = merged(fields[0], strips[0], r + HALO)
        image[r * LEVELS : r * LEVELS + 8, :] = low
        image[r * LEVELS + 8 : (r + 1) * LEVELS, :] = high
    mine = spots[OWN : 2 * OWN, :].astype(jnp.int32) - HALO * LEVELS
    hit = jnp.concatenate([one_hot(lanes(OWN), mine), one_hot(lanes(OWN) + LANES, mine)], axis=1)
    return jnp.sum(square, keepdims=True), chosen(hit, split(image[...]))


def weigh(seen, grams):
    column = jnp.transpose(seen)
    out = []
    for t in range(OWN):
        total = jnp.zeros((8, LANES), F32)
        for k in range(LANES // 8):
            at = t * LANES + k * 8
            total += grams[at : at + 8, :] * column[k * 8 : k * 8 + 8, t : t + 1]
        out.append(jnp.sum(total, axis=0, keepdims=True))
    return jnp.concatenate(out, axis=0)


def in_lanes(first, values):
    ln = lanes(8)
    out = jnp.zeros((8, LANES), F32)
    for i, v in enumerate(values):
        out = jnp.where(ln == first + i, v, out)
    return out


def first_half(wide, mine, core, own_message, inter, beside, spots, by_lane, kept, seen, sums, field, other, strip, other_strip, image):
    ln = lanes(8)
    even = lax.axis_index("lat_2") == 0
    beside[:STRIP, :] = jnp.where(even, inter[:STRIP, :], core[:STRIP, :])
    beside[STRIP:, :] = jnp.where(even, core[:STRIP, :], inter[:STRIP, :])
    step = jnp.where(even, float(ROWS * LEVELS), -float(ROWS * LEVELS))
    c, o, i = core[SPOTS:, :] + step, own_message[SPOTS:, :], inter[SPOTS:, :] - step
    tables = (((c, 0), (o, 0), (i, 0)), ((c, 16), (o, 16), (i, 16), (c, 32), (o, 32), (i, 32)))
    for t, table in enumerate(tables):
        spot = jnp.full((8, LANES), NOWHERE, F32)
        for n, (x, at) in enumerate(table):
            spot = jnp.where((ln >= OWN * n) & (ln < OWN * (n + 1)), roll(x, OWN * n - at), spot)
        by_lane[t * 8 : t * 8 + 8, :] = spot
        spots[t * LANES : (t + 1) * LANES, :] = jnp.transpose(jnp.broadcast_to(spot[:1], (LANES, LANES)))
    parts = (core, own_message, inter)
    own = padded(jnp.concatenate([x[STRIP:LEFTS, :] for x in parts], axis=0), LANES)
    sides = padded(jnp.concatenate([x[LEFTS:RIGHTS, :] for x in parts] + [x[RIGHTS:SPOTS, :] for x in parts], axis=0), LANES)
    square, rows = back_and_on(spots, by_lane, own, sides, rates_of(wide, mine, beside), kept, (field, other), (strip, other_strip), image)
    seen[...] = rows
    sums[...] = in_lanes(0, [square])


def stepped(x, unit):
    row = places(OWN)
    for bit in range(4):
        x = jnp.where((row & (1 << bit)) != 0, roll(x, unit << bit), x)
    return x


def herald(rows, message):
    mine = (lanes(OWN) >> 3) == places(OWN)
    message[:OWN, :] = rows
    message[OWN : OWN + 1, :] = jnp.sum(jnp.where(mine, stepped(rows, 8), 0.0), axis=0, keepdims=True)
    message[OWN + 1 : OWN + 2, :] = jnp.sum(jnp.where(mine, stepped(roll(rows, 8), 8), 0.0), axis=0, keepdims=True)
    message[OWN + 2 :, :] = jnp.zeros((HERALD - OWN - 2, LANES), F32)


def first_terms(grams, seen, before, message, sums):
    rows = weigh(seen[...], grams)
    herald(rows, message)
    sums[...] = before[...] + in_lanes(1, [jnp.sum(seen[...] * rows, keepdims=True)])


def edges_of(core, mine, inter, out):
    for i, x in enumerate((core, mine, inter)):
        out[i : i + 1, :] = x[OWN : OWN + 1, :]
        out[i + 3 : i + 4, :] = x[OWN + 1 : OWN + 2, :]
    out[6:, :] = jnp.zeros((2, LANES), F32)


def side_strips(lefts, rights):
    ln = lanes(OWN)
    rows = [stepped(jnp.broadcast_to(x, (OWN, LANES)), -8) for x in lefts]
    out = [jnp.where(ln < 8, x, 0.0) for x in rows]
    rows = [stepped(jnp.broadcast_to(x, (OWN, LANES)), -8) for x in rights]
    return padded(jnp.concatenate(out + [right_strips(x) for x in rows], axis=0), LANES)


def second_half(spots, by_lane, core, mine, inter, even, odd, wide, strips, beside, grams, before, kept, message, out, field, other, strip, other_strip, image):
    own = padded(jnp.concatenate([x[:OWN, :] for x in (core, mine, inter)], axis=0), LANES)
    here = lax.rem(lax.axis_index("lon"), 2) == 0
    left, right = jnp.where(here, odd[...], even[...]), jnp.where(here, even[...], odd[...])
    sides = side_strips([left[i : i + 1] for i in (3, 4, 5)], [right[i : i + 1] for i in (0, 1, 2)])
    square, seen = back_and_on(
        spots, by_lane, own, sides, rates_of(wide, strips, beside), kept, (field, other), (strip, other_strip), image
    )
    rows = weigh(seen, grams)
    herald(rows, message)
    sums = before[...] + in_lanes(2, [square, jnp.sum(seen * rows, keepdims=True)])
    out[...] = jnp.concatenate([sums] * (out.shape[0] // 8), axis=0)
    for step, row in ((1, OWN + 1), (-1, OWN)):
        out[pl.ds(in_plane(step) * 2 + 1, 1), :] = message[row : row + 1, :]


def in_plane(step):
    return lax.axis_index("lat_1") * LON + lax.rem(lax.axis_index("lon") + LON + step, LON)


def gathered(parts, mine, sums, message):
    count = parts.shape[0] // 2
    sums[...] = jnp.broadcast_to(jnp.sum(parts[pl.ds(0, count, stride=2), :], axis=0, keepdims=True), sums.shape)
    message[...] = mine[...]
    for i, step in enumerate((-1, 1)):
        message[OWN + i : OWN + i + 1, :] = parts[pl.ds(in_plane(step) * 2 + 1, 1), :]


def last_rows(spots, by_lane, core, mine, inter, wide, strips, beside, kept, field, other, strip, other_strip):
    lists = (core, mine, inter)
    own = padded(jnp.concatenate([x[:OWN, :] for x in lists], axis=0), LANES)
    sides = side_strips(*([x[OWN + i : OWN + i + 1, :] for x in lists] for i in range(2)))
    lay_out(spots, by_lane, own, sides, field, strip, HALO - STEPS, HALO + ROWS + STEPS)
    fields, narrow = steps_back(rates_of(wide, strips, beside), (field, other), (strip, other_strip), STEPS)
    for r in range(ROWS):
        kept[r * LEVELS : r * LEVELS + 8, :], kept[r * LEVELS + 8 : (r + 1) * LEVELS, :] = merged(fields[0], narrow[0], r + HALO)


def finish(parts, right_side, image, second, increment, residual):
    total = jnp.sum(parts[...], axis=0, keepdims=True)
    m0, m1, m2, m3 = (jnp.sum(jnp.where(lanes(1) == i, total, 0.0), keepdims=True) for i in range(4))
    step_0 = m0 / (m0 + m1)
    rho = m1 / m0
    spread = m2 - rho * m1
    curve = (m3 - rho * m2) - rho * (m2 - rho * m1)
    gamma = step_0 * spread / m0
    step_1 = spread / (spread + curve - gamma * spread)
    on_b = step_0 * (1.0 + step_1 * (gamma + rho))
    on_k = -step_0 * step_1
    rest_b = step_0 * ((1.0 - step_1) * rho - step_1 * gamma)
    rest_k = -step_0 * ((1.0 - step_1) + step_1 * (rho + gamma))
    rest_kk = step_0 * step_1
    on_b, on_k, rest_b, rest_k, rest_kk = (jnp.broadcast_to(v, (8, LANES)) for v in (on_b, on_k, rest_b, rest_k, rest_kk))
    for r in range(ROWS):
        for h in range(2):
            at = r * LEVELS + h * 8
            b, k, kk = right_side[at : at + 8, :], image[at : at + 8, :], second[at : at + 8, :]
            to = pl.ds(h * 8 * ROWS + r, 8, stride=ROWS)
            increment[to, :] = on_b * b + on_k * k
            residual[to, :] = rest_b * b + rest_k * k + rest_kk * kk


def to_core(x):
    return lax.ppermute(x, LAT, [(i, i ^ 1) for i in range(lax.axis_size(LAT))])


def to_inter(x):
    return lax.ppermute(x, LAT, [(i, ((i + 1) ^ 1) - 1) for i in range(1, lax.axis_size(LAT) - 1)])


def to_even(x):
    return lax.ppermute(x, "lon", [(i, i ^ 1) for i in range(LON)])


def to_odd(x):
    return lax.ppermute(x, "lon", [(i, (((i + 1) % LON ^ 1) - 1) % LON) for i in range(LON)])


def spread_out(x, axes):
    return lax.all_to_all(x, axes, split_axis=0, concat_axis=0, tiled=True)


def shards(courant, obs_matrix, obs_weight, innovation, block_owner, block_row, block_count):
    flow = courant.reshape(-1, LANES)
    owner, row, count = block_owner.reshape(-1), block_row.reshape(-1), block_count.reshape(-1)
    wholes = (flow, obs_matrix[0], obs_weight[0], innovation[0])
    parcels, for_core, for_inter = call(
        prepare,
        [(LON * PARCEL, LANES), (EDGE, LANES), (EDGE, LANES)],
        (owner, row, count, *wholes),
        4_000_000,
        [pltpu.SMEM((CAP,), jnp.int32), pltpu.SMEM((CAP,), jnp.int32), pltpu.SMEM((1,), jnp.int32)]
        + [pltpu.VMEM(x.shape, F32) for x in wholes]
        + [pltpu.VMEM((OWN, LANES), F32), pltpu.SemaphoreType.DMA((7,))],
        [pl.BlockSpec(memory_space=pltpu.HBM)] * 7,
        62,
    )
    parcels = spread_out(parcels.reshape(LON, PARCEL, LANES), "lon").reshape(LON * PARCEL, LANES)
    core, inter = to_core(for_core), to_inter(for_inter)
    wide, strips, for_core, for_inter = call(
        arrange,
        [(WIDE * 2 * LEVELS, LANES), (2 * STRIP, LANES), (MESSAGE, LANES), (MESSAGE, LANES)],
        (flow, parcels, core, inter),
        2_000_000,
    )
    core, inter = to_core(for_core), to_inter(for_inter)
    (grams,) = call(unpack, [(OWN * LANES, LANES)], (parcels,), 4_000_000)
    cells, listed = (ROWS * LEVELS, LANES), (OWN, LANES)
    work = [pltpu.VMEM((WIDE * LEVELS, LANES), F32)] * 2 + [pltpu.VMEM((WIDE * 8, LANES), F32)] * 2
    work_too = work + [pltpu.VMEM(cells, F32)]
    beside, spots, by_lane, right_side, seen, sums = call(
        first_half,
        [(2 * STRIP, LANES), (2 * LANES, LANES), (16, LANES), cells, listed, (8, LANES)],
        (wide, strips, core, for_core, inter),
        4_000_000,
        work_too,
    )
    rates = (wide, strips, beside)
    short = (HERALD, LANES)
    mine, sums = call(first_terms, [short, (8, LANES)], (grams, seen, sums), 2_000_000)
    core, inter = to_core(mine), to_inter(mine)
    (edges,) = call(edges_of, [(8, LANES)], (core, mine, inter), 10_000)
    lists = (core, mine, inter, to_even(edges), to_odd(edges))
    plane, towers = lax.axis_size(("lat_1", "lon")), lax.axis_size(("lat_0", "lat_2"))
    image, mine, parcels = call(
        second_half, [cells, short, (plane * 2, LANES)], (spots, by_lane, *lists, *rates, grams, sums), 4_000_000, work_too
    )
    parcels = spread_out(parcels.reshape(plane, 2, LANES), ("lat_1", "lon")).reshape(plane * 2, LANES)
    sums, mine = call(gathered, [(towers, LANES), short], (parcels, mine), 10_000)
    core, inter = to_core(mine), to_inter(mine)
    parts = spread_out(sums.reshape(towers, 1, LANES), ("lat_0", "lat_2")).reshape(towers, LANES)
    (second,) = call(last_rows, [cells], (spots, by_lane, core, mine, inter, *rates), 4_000_000, work)
    increment, residual = call(finish, [cells, cells], (parts, right_side, image, second), 100_000)
    shape = courant.shape[1:]
    return increment.reshape(shape), residual.reshape(shape)


def solution(mesh):
    torus = Mesh(
        mesh.devices.reshape(-1, 4, 2, mesh.shape["lon"]), ("lat_0", "lat_1", "lat_2", "lon")
    )
    placed = (
        P(None, None, LAT, "lon"),
        P(LAT, "lon", None, None),
        P(LAT, "lon", None),
        P(LAT, "lon", None),
        P(LAT, "lon", None),
        P(LAT, "lon"),
        P(LAT, "lon"),
    )
    return jax.shard_map(
        shards,
        mesh=torus,
        in_specs=placed,
        out_specs=(P(None, LAT, "lon"), P(None, LAT, "lon")),
        check_vma=False,
    )
```

```python
import jax
import jax.numpy as jnp
from jax import lax
from jax.experimental import pallas as pl
from jax.experimental.pallas import tpu as pltpu
from jax.sharding import Mesh
from jax.sharding import PartitionSpec as P

LAT = ("lat_0", "lat_1", "lat_2")
LEVELS = 16
ROWS = 16
LANES = 128
CAP = 8
SLOT = 2
STEPS = 4
HALO = 2 * STEPS
WIDE = ROWS + 2 * HALO
LON = 8
HALF = LANES // 2
OWN = LON * SLOT
NEAR = 3 * OWN
BULK = 2 * HALF + 2
LIST = BULK + 6
PARCEL = LIST
EDGE = HALO * 2 * LEVELS
STRIP = HALO * 2 * 8
LEFTS = STRIP + OWN
RIGHTS = LEFTS + OWN
SPOTS = RIGHTS + OWN
MESSAGE = SPOTS + 8
HERALD = OWN + 8
NOWHERE = -4096.0
HIGHEST = lax.Precision.HIGHEST
F32 = jnp.float32
VMEM = pl.BlockSpec(memory_space=pltpu.VMEM)
SMEM = pl.BlockSpec(memory_space=pltpu.SMEM)


def lanes(rows):
    return lax.broadcasted_iota(jnp.int32, (rows, LANES), 1)


def places(rows):
    return lax.broadcasted_iota(jnp.int32, (rows, LANES), 0)


def roll(x, shift):
    shift %= LANES
    return pltpu.roll(x, shift, axis=1) if shift else x


def call(body, outs, args, flops, scratch=(), specs=None, room=24):
    return pl.pallas_call(
        body,
        out_shape=[jax.ShapeDtypeStruct(s, F32) for s in outs],
        in_specs=specs or [SMEM if a.dtype == jnp.int32 else VMEM for a in args],
        out_specs=[VMEM] * len(outs),
        scratch_shapes=list(scratch),
        compiler_params=pltpu.CompilerParams(vmem_limit_bytes=room << 20),
        cost_estimate=pl.CostEstimate(flops=flops, bytes_accessed=0, transcendentals=0),
        name=body.__name__,
    )(*args)


def turns_of(owners):
    return [sum([(o == owners[j]).astype(jnp.int32) for o in owners[:j]], jnp.int32(0)) for j in range(CAP)]


def chunk(owner):
    return (owner + LON // 2) % LON if isinstance(owner, int) else lax.rem(owner + LON // 2, LON)


def packed_edges(pick, shift):
    ln = lanes(8)
    out = jnp.zeros((8, LANES), F32)
    for k in range(8):
        low, high = pick(k)
        out = jnp.where((ln >= 16 * k) & (ln < 16 * k + 8), roll(low, 16 * k + shift), out)
        out = jnp.where((ln >= 16 * k + 8) & (ln < 16 * k + 16), roll(high, 16 * k + 8 + shift), out)
    return out


def weigh_blocks(owners, turns, count, matrix, weight, parcels):
    ln, rw = lanes(HALF), places(HALF)
    for j in range(CAP):
        block = matrix[j]
        scaled = jnp.transpose(block) * jnp.where(j < count[0, 0], weight[j : j + 1, :], 0.0)
        gram = jnp.dot(scaled, block, precision=HIGHEST, preferred_element_type=F32)
        top, low = gram[:HALF], gram[HALF:]
        packed = jnp.where((ln >= HALF) & (ln - HALF <= rw), roll(top, HALF), low)
        diagonal = jnp.sum(jnp.where(ln - HALF == rw, low, 0.0), axis=0, keepdims=True)
        at = chunk(owners[j]) * PARCEL + turns[j] * HALF
        parcels[pl.ds(pl.multiple_of(at, 8), HALF), :] = packed
        parcels[pl.ds(chunk(owners[j]) * PARCEL + 2 * HALF + turns[j], 1), :] = diagonal


def prepare(owner_at, row_at, count_at, flow_at, matrix_at, weight_at, innovation_at, parcels, to_core, to_inter, to_even, to_odd, owner, row, count, flow, matrix, weight, innovation, lists, sems):
    pairs = ((owner_at, owner), (row_at, row), (count_at, count), (flow_at, flow), (weight_at, weight), (innovation_at, innovation), (matrix_at, matrix))
    copies = [pltpu.make_async_copy(a, b, sems.at[i]) for i, (a, b) in enumerate(pairs)]
    for copy in copies:
        copy.start()
    for d in range(LON):
        parcels[d * PARCEL : d * PARCEL + LIST, :] = jnp.zeros((LIST, LANES), F32)
    lists[...] = jnp.zeros(lists.shape, F32)
    even = lax.axis_index("lat_2") == 0
    here = lax.rem(lax.axis_index("lon"), 2) == 0
    copies[3].wait()
    for f in range(2):
        for g in range(2):

            def pick(k, f=f, g=g):
                at = f * LEVELS * ROWS + g * 8 + k
                return flow[pl.ds(at, 8, stride=ROWS), :], flow[pl.ds(at + 8 * ROWS, 8, stride=ROWS), :]

            at = (f * 2 + g) * 8
            to_right, to_left = packed_edges(pick, 8), packed_edges(pick, 0)
            to_even[at : at + 8, :] = jnp.where(here, to_right, to_left)
            to_odd[at : at + 8, :] = jnp.where(here, to_left, to_right)
        for i in range(HALO):
            for h in range(2):
                at = f * LEVELS * ROWS + h * 8 * ROWS + i
                up, down = flow[pl.ds(at + ROWS - HALO, 8, stride=ROWS), :], flow[pl.ds(at, 8, stride=ROWS), :]
                at = (i * 2 + f) * LEVELS + h * 8
                to_core[at : at + 8, :] = jnp.where(even, up, down)
                to_inter[at : at + 8, :] = jnp.where(even, down, up)
    for i in (0, 1, 2, 4, 5, 6):
        copies[i].wait()
    owners = [owner[j] for j in range(CAP)]
    turns = turns_of(owners)
    column = jnp.transpose(weight[...] * innovation[...])
    ln = lanes(8)
    named = jnp.full((8, LANES), NOWHERE, F32)
    for j in range(CAP):
        live = j < count[0, 0]
        total = jnp.zeros((8, LANES), F32)
        for k in range(LANES // 8):
            total += matrix[j, k * 8 : k * 8 + 8, :] * column[k * 8 : k * 8 + 8, j : j + 1]
        slot = owners[j] * SLOT + turns[j]
        lists[pl.ds(slot, 1), :] = jnp.where(live, jnp.sum(total, axis=0, keepdims=True), 0.0)
        place = jnp.where(live, (lax.rem(row[j], ROWS) + HALO) * LEVELS + lax.div(row[j], ROWS), int(NOWHERE)).astype(F32)
        named = jnp.where(ln == slot, place, named)
    weigh_blocks(owners, turns, count, matrix, weight, parcels)
    named = jnp.where(ln < OWN, named, roll(named, OWN))
    line = lanes(1)
    for d in range(LON):
        left, right = 2 * (d - 1) % OWN, 2 * (d + 1) % OWN
        at = chunk(d) * PARCEL + BULK
        parcels[at : at + 2, :] = lists[2 * d : 2 * d + 2, :]
        edge = jnp.where(line < 8, roll(lists[left : left + 1, :], 8), roll(lists[left + 1 : left + 2, :], 16))
        edge = jnp.where(line < 16, edge, jnp.where(line < 24, roll(lists[right : right + 1, :], 16), roll(lists[right + 1 : right + 2, :], 24)))
        parcels[at + 2 : at + 3, :] = edge
        parcels[at + 3 : at + 4, :] = roll(named, -left)[:1]


def arrange(flow, parcels, core, inter, even_edges, odd_edges, wide, strips, to_core, to_inter):
    ln = lanes(8)
    here = lax.rem(lax.axis_index("lon"), 2) == 0
    even = lax.axis_index("lat_2") == 0
    wide[:EDGE, :] = jnp.where(even, inter[...], core[...])
    wide[EDGE + ROWS * 2 * LEVELS :, :] = jnp.where(even, core[...], inter[...])
    for f in range(2):
        for g in range(2):
            at = (f * 2 + g) * 8
            first, second = even_edges[at : at + 8, :], odd_edges[at : at + 8, :]
            left, right = jnp.where(here, second, first), jnp.where(here, first, second)
            for k in range(8):
                at = f * LEVELS * ROWS + g * 8 + k
                low, high = flow[pl.ds(at, 8, stride=ROWS), :], flow[pl.ds(at + 8 * ROWS, 8, stride=ROWS), :]
                at = EDGE + ((g * 8 + k) * 2 + f) * LEVELS
                wide[at : at + 8, :] = low
                wide[at + 8 : at + 16, :] = high
                a = jnp.where(ln < 8, roll(left, -16 * k), jnp.where(ln < 32, roll(low, 8), jnp.where(ln < 56, roll(low, 56), roll(right, 56 - 16 * k))))
                b = jnp.where(ln < 72, roll(left, 56 - 16 * k), jnp.where(ln < 96, roll(high, 72), jnp.where(ln < 120, roll(high, 120), roll(right, 112 - 16 * k))))
                strip = jnp.where(ln < HALF, a, b)
                at = ((g * 8 + k) * 2 + f) * 8
                strips[at : at + 8, :] = strip
    lower, upper = strips[:STRIP, :], strips[STRIP:, :]
    to_core[:STRIP, :] = jnp.where(even, upper, lower)
    to_inter[:STRIP, :] = jnp.where(even, lower, upper)
    edge = parcels[pl.ds(BULK + 2, LON, stride=PARCEL), :]
    named = parcels[pl.ds(BULK + 3, LON, stride=PARCEL), :]
    turned = jnp.transpose(named)
    spot = jnp.full((1, LANES), NOWHERE, F32)
    line = lanes(1)
    for i, k in enumerate((2, 3, 0, 1, 4, 5)):
        line_k = jnp.concatenate([turned[k : k + 1, :], jnp.zeros((1, LANES - LON), F32)], axis=1)
        spot = jnp.where((line >= 8 * i) & (line < 8 * i + 8), roll(line_k, 8 * i), spot)
    for o in range(SLOT):
        own = parcels[pl.ds(BULK + o, LON, stride=PARCEL), :]
        left = jnp.where(ln < 8, roll(edge, -8 * o), 0.0)
        right = jnp.where((ln >= 56) & (ln < 64), roll(edge, 40 - 8 * o), 0.0)
        for out in (to_core, to_inter):
            out[STRIP + o * LON : STRIP + (o + 1) * LON, :] = own
            out[LEFTS + o * LON : LEFTS + (o + 1) * LON, :] = left
            out[RIGHTS + o * LON : RIGHTS + (o + 1) * LON, :] = right
    for out in (to_core, to_inter):
        out[SPOTS:, :] = jnp.broadcast_to(spot, (8, LANES))


def unpack(parcels, grams):
    ln, rw = lanes(HALF), places(HALF)
    upper, diagonal, first = ln - HALF > rw, ln - HALF == rw, ln < HALF
    for s in range(LON):
        both = parcels[s * PARCEL : s * PARCEL + 2 * HALF, :]
        turned = jnp.transpose(both)
        ct, et = turned[:HALF], turned[HALF:]
        ct_rolled, et_rolled = roll(ct, HALF), roll(et, HALF)
        for o in range(SLOT):
            q = both[o * HALF : (o + 1) * HALF]
            d = parcels[s * PARCEL + 2 * HALF + o : s * PARCEL + 2 * HALF + o + 1, :]
            e_first, e_last = (et, et_rolled) if o == 0 else (et_rolled, et)
            c_last = ct_rolled if o == 0 else ct
            top = jnp.where(first, jnp.where(ln <= rw, roll(q, HALF), e_first), c_last)
            low = jnp.where(first | upper, q, jnp.where(diagonal, d, e_last))
            at = (o * LON + s) * LANES
            grams[at : at + HALF, :] = top
            grams[at + HALF : at + LANES, :] = low


def split(x):
    high = x.astype(jnp.bfloat16)
    rest = x - high.astype(F32)
    middle = rest.astype(jnp.bfloat16)
    low = (rest - middle.astype(F32)).astype(jnp.bfloat16)
    return jnp.concatenate([high, middle, low], axis=1)


def chosen(one_hot, parts):
    out = jnp.dot(one_hot, parts, preferred_element_type=F32)
    return out[:, :LANES] + out[:, LANES : 2 * LANES] + out[:, 2 * LANES :]


def one_hot(index, at):
    return jnp.where(index == at, 1.0, 0.0).astype(jnp.bfloat16)


def padded(x, rows):
    return jnp.concatenate([x, jnp.zeros((rows - x.shape[0], LANES), F32)], axis=0)


def left_strips(x):
    return jnp.where(lanes(x.shape[0]) < 8, roll(x, 8), 0.0)


def right_strips(x):
    ln = lanes(x.shape[0])
    return jnp.where((ln >= 56) & (ln < 64), roll(x, 56), 0.0)


def lay_out(spots, by_lane, own, sides, field, strips, low, high):
    ln = lanes(LANES)
    own_strip = jnp.where(ln < 32, jnp.where(ln >= 8, roll(own, 8), 0.0), jnp.where(ln < 56, roll(own, 56), 0.0))
    pieces = []
    for i, strip in enumerate((own_strip, sides)):
        upper = (spots[i * LANES : (i + 1) * LANES, :].astype(jnp.int32) & 8) != 0
        pieces.append(split(jnp.where(upper, roll(strip, HALF), strip)))
    own_parts = split(own)
    lane_spots = [by_lane[i * 8 : i * 8 + 1, :].astype(jnp.int32) for i in range(2)]
    p = jnp.broadcast_to(lane_spots[0], (LANES, LANES))
    for start in range(low * LEVELS, high * LEVELS, LANES):
        field[start : start + LANES, :] = chosen(one_hot(places(LANES) + start, p), own_parts)
    folded = [jnp.broadcast_to(((b >> 4) << 3) + (b & 7), (64, LANES)) for b in lane_spots]
    for start in range(low * 8, high * 8, 64):
        at = places(64) + start
        strips[start : start + 64, :] = chosen(one_hot(at, folded[0]), pieces[0]) + chosen(one_hot(at, folded[1]), pieces[1])


def adjoint(rates, source, target, first, last, height):
    before = kept = None
    for r in range(first, last + 1):
        y = source[r * height : (r + 1) * height, :]
        lat, lon = rates(r)
        t = lat * y
        a = jnp.where(lat > 0.0, t, 0.0)
        b = a - t
        s = lon * y
        e = jnp.where(lon > 0.0, s, 0.0)
        f = e - s
        if r > first + 1:
            target[(r - 1) * height : r * height, :] = kept + a
        if r > first:
            kept = y - (a + b) - (e + f) + roll(e, -1) + roll(f, 1) + before
        before = b


def tangent(rates, source, target, first, last, height):
    for r in range(first + 1, last):
        x = source[r * height : (r + 1) * height, :]
        south = source[(r - 1) * height : r * height, :]
        north = source[(r + 1) * height : (r + 2) * height, :]
        lat, lon = rates(r)
        out = x + jnp.abs(lat) * (jnp.where(lat > 0.0, south, north) - x)
        target[r * height : (r + 1) * height, :] = out + jnp.abs(lon) * (jnp.where(lon > 0.0, roll(x, 1), roll(x, -1)) - x)


def merged(field, strips, r):
    ln = lanes(8)
    t = strips[r * 8 : (r + 1) * 8, :]
    low, high = field[r * LEVELS : r * LEVELS + 8, :], field[r * LEVELS + 8 : (r + 1) * LEVELS, :]
    low = jnp.where(ln < 8, roll(t, -8), jnp.where(ln >= 120, roll(t, 72), low))
    high = jnp.where(ln < 8, roll(t, -72), jnp.where(ln >= 120, roll(t, 8), high))
    return low, high


def steps_back(rates, fields, strips, first):
    full, narrow = rates
    for k in range(first, first + STEPS):
        adjoint(full, *fields, k, WIDE - 1 - k, LEVELS)
        adjoint(narrow, *strips, k, WIDE - 1 - k, 8)
        fields, strips = fields[::-1], strips[::-1]
    return fields, strips


def steps_on(rates, fields, strips, first):
    full, narrow = rates
    for k in range(first, first + STEPS):
        tangent(full, *fields, k, WIDE - 1 - k, LEVELS)
        tangent(narrow, *strips, k, WIDE - 1 - k, 8)
        fields, strips = fields[::-1], strips[::-1]
    return fields, strips


def rates_of(wide, mine, beside):
    def full(r):
        at = r * 2 * LEVELS
        return wide[at : at + LEVELS, :], wide[at + LEVELS : at + 2 * LEVELS, :]

    def narrow(r):
        ref, r = (mine, r - HALO) if HALO <= r < HALO + ROWS else (beside, r if r < HALO else r - ROWS)
        return ref[r * 16 : r * 16 + 8, :], ref[r * 16 + 8 : r * 16 + 16, :]

    return full, narrow


def back_and_on(spots, by_lane, own, sides, rates, kept, fields, strips, image):
    lay_out(spots, by_lane, own, sides, fields[0], strips[0], 0, WIDE)
    fields, strips = steps_back(rates, fields, strips, 0)
    lat, last = lax.axis_index(LAT), lax.axis_size(LAT) - 1
    for outside, start in ((lat == 0, STEPS), (lat == last, HALO + ROWS)):
        for ref, height in ((fields[0], LEVELS), (strips[0], 8)):
            block = ref[start * height : (start + STEPS) * height, :]
            ref[start * height : (start + STEPS) * height, :] = jnp.where(outside, 0.0, block)
    square = jnp.zeros((8, LANES), F32)
    for r in range(ROWS):
        low, high = merged(fields[0], strips[0], r + HALO)
        kept[r * LEVELS : r * LEVELS + 8, :] = low
        kept[r * LEVELS + 8 : (r + 1) * LEVELS, :] = high
        square += low * low + high * high
    fields, strips = steps_on(rates, fields, strips, STEPS)
    for r in range(ROWS):
        low, high = merged(fields[0], strips[0], r + HALO)
        image[r * LEVELS : r * LEVELS + 8, :] = low
        image[r * LEVELS + 8 : (r + 1) * LEVELS, :] = high
    mine = spots[OWN : 2 * OWN, :].astype(jnp.int32) - HALO * LEVELS
    hit = jnp.concatenate([one_hot(lanes(OWN), mine), one_hot(lanes(OWN) + LANES, mine)], axis=1)
    return jnp.sum(square, keepdims=True), chosen(hit, split(image[...]))


def weigh(seen, grams):
    column = jnp.transpose(seen)
    out = []
    for t in range(OWN):
        total = jnp.zeros((8, LANES), F32)
        for k in range(LANES // 8):
            at = t * LANES + k * 8
            total += grams[at : at + 8, :] * column[k * 8 : k * 8 + 8, t : t + 1]
        out.append(jnp.sum(total, axis=0, keepdims=True))
    return jnp.concatenate(out, axis=0)


def in_lanes(first, values):
    ln = lanes(8)
    out = jnp.zeros((8, LANES), F32)
    for i, v in enumerate(values):
        out = jnp.where(ln == first + i, v, out)
    return out


def first_half(wide, mine, core, own_message, inter, beside, spots, by_lane, kept, seen, sums, field, other, strip, other_strip, image):
    ln = lanes(8)
    even = lax.axis_index("lat_2") == 0
    beside[:STRIP, :] = jnp.where(even, inter[:STRIP, :], core[:STRIP, :])
    beside[STRIP:, :] = jnp.where(even, core[:STRIP, :], inter[:STRIP, :])
    step = jnp.where(even, float(ROWS * LEVELS), -float(ROWS * LEVELS))
    c, o, i = core[SPOTS:, :] + step, own_message[SPOTS:, :], inter[SPOTS:, :] - step
    tables = (((c, 0), (o, 0), (i, 0)), ((c, 16), (o, 16), (i, 16), (c, 32), (o, 32), (i, 32)))
    for t, table in enumerate(tables):
        spot = jnp.full((8, LANES), NOWHERE, F32)
        for n, (x, at) in enumerate(table):
            spot = jnp.where((ln >= OWN * n) & (ln < OWN * (n + 1)), roll(x, OWN * n - at), spot)
        by_lane[t * 8 : t * 8 + 8, :] = spot
        spots[t * LANES : (t + 1) * LANES, :] = jnp.transpose(jnp.broadcast_to(spot[:1], (LANES, LANES)))
    parts = (core, own_message, inter)
    own = padded(jnp.concatenate([x[STRIP:LEFTS, :] for x in parts], axis=0), LANES)
    sides = padded(jnp.concatenate([x[LEFTS:RIGHTS, :] for x in parts] + [x[RIGHTS:SPOTS, :] for x in parts], axis=0), LANES)
    square, rows = back_and_on(spots, by_lane, own, sides, rates_of(wide, mine, beside), kept, (field, other), (strip, other_strip), image)
    seen[...] = rows
    sums[...] = in_lanes(0, [square])


def stepped(x, unit):
    row = places(OWN)
    for bit in range(4):
        x = jnp.where((row & (1 << bit)) != 0, roll(x, unit << bit), x)
    return x


def herald(rows, message):
    mine = (lanes(OWN) >> 3) == places(OWN)
    message[:OWN, :] = rows
    message[OWN : OWN + 1, :] = jnp.sum(jnp.where(mine, stepped(rows, 8), 0.0), axis=0, keepdims=True)
    message[OWN + 1 : OWN + 2, :] = jnp.sum(jnp.where(mine, stepped(roll(rows, 8), 8), 0.0), axis=0, keepdims=True)
    message[OWN + 2 :, :] = jnp.zeros((HERALD - OWN - 2, LANES), F32)


def first_terms(grams, seen, before, message, sums):
    rows = weigh(seen[...], grams)
    herald(rows, message)
    sums[...] = before[...] + in_lanes(1, [jnp.sum(seen[...] * rows, keepdims=True)])


def edges_of(core, mine, inter, out):
    for i, x in enumerate((core, mine, inter)):
        out[i : i + 1, :] = x[OWN : OWN + 1, :]
        out[i + 3 : i + 4, :] = x[OWN + 1 : OWN + 2, :]
    out[6:, :] = jnp.zeros((2, LANES), F32)


def side_strips(lefts, rights):
    ln = lanes(OWN)
    rows = [stepped(jnp.broadcast_to(x, (OWN, LANES)), -8) for x in lefts]
    out = [jnp.where(ln < 8, x, 0.0) for x in rows]
    rows = [stepped(jnp.broadcast_to(x, (OWN, LANES)), -8) for x in rights]
    return padded(jnp.concatenate(out + [right_strips(x) for x in rows], axis=0), LANES)


def second_half(spots, by_lane, core, mine, inter, even, odd, wide, strips, beside, grams, before, kept, message, out, field, other, strip, other_strip, image):
    own = padded(jnp.concatenate([x[:OWN, :] for x in (core, mine, inter)], axis=0), LANES)
    here = lax.rem(lax.axis_index("lon"), 2) == 0
    left, right = jnp.where(here, odd[...], even[...]), jnp.where(here, even[...], odd[...])
    sides = side_strips([left[i : i + 1] for i in (3, 4, 5)], [right[i : i + 1] for i in (0, 1, 2)])
    square, seen = back_and_on(
        spots, by_lane, own, sides, rates_of(wide, strips, beside), kept, (field, other), (strip, other_strip), image
    )
    rows = weigh(seen, grams)
    herald(rows, message)
    sums = before[...] + in_lanes(2, [square, jnp.sum(seen * rows, keepdims=True)])
    out[...] = jnp.concatenate([sums] * (out.shape[0] // 8), axis=0)
    for step, row in ((1, OWN + 1), (-1, OWN)):
        out[pl.ds(in_plane(step) * 2 + 1, 1), :] = message[row : row + 1, :]


def in_plane(step):
    size = lax.axis_size(("lat_1", "lon"))
    at = lax.axis_index("lat_1") * LON + lax.rem(lax.axis_index("lon") + LON + step, LON)
    return lax.rem(at + size - middle_of_plane(), size)


def middle_of_plane():
    return lax.axis_size("lat_1") // 2 * LON + LON // 2


def gathered(parts, mine, sums, message):
    count = parts.shape[0] // 2
    sums[...] = jnp.broadcast_to(jnp.sum(parts[pl.ds(0, count, stride=2), :], axis=0, keepdims=True), sums.shape)
    message[...] = mine[...]
    for i, step in enumerate((-1, 1)):
        message[OWN + i : OWN + i + 1, :] = parts[pl.ds(in_plane(step) * 2 + 1, 1), :]


def last_rows(spots, by_lane, core, mine, inter, wide, strips, beside, kept, field, other, strip, other_strip):
    lists = (core, mine, inter)
    own = padded(jnp.concatenate([x[:OWN, :] for x in lists], axis=0), LANES)
    sides = side_strips(*([x[OWN + i : OWN + i + 1, :] for x in lists] for i in range(2)))
    lay_out(spots, by_lane, own, sides, field, strip, HALO - STEPS, HALO + ROWS + STEPS)
    fields, narrow = steps_back(rates_of(wide, strips, beside), (field, other), (strip, other_strip), STEPS)
    for r in range(ROWS):
        kept[r * LEVELS : r * LEVELS + 8, :], kept[r * LEVELS + 8 : (r + 1) * LEVELS, :] = merged(fields[0], narrow[0], r + HALO)


def finish(parts, right_side, image, second, increment, residual):
    total = jnp.sum(parts[...], axis=0, keepdims=True)
    m0, m1, m2, m3 = (jnp.sum(jnp.where(lanes(1) == i, total, 0.0), keepdims=True) for i in range(4))
    step_0 = m0 / (m0 + m1)
    rho = m1 / m0
    spread = m2 - rho * m1
    curve = (m3 - rho * m2) - rho * (m2 - rho * m1)
    gamma = step_0 * spread / m0
    step_1 = spread / (spread + curve - gamma * spread)
    on_b = step_0 * (1.0 + step_1 * (gamma + rho))
    on_k = -step_0 * step_1
    rest_b = step_0 * ((1.0 - step_1) * rho - step_1 * gamma)
    rest_k = -step_0 * ((1.0 - step_1) + step_1 * (rho + gamma))
    rest_kk = step_0 * step_1
    on_b, on_k, rest_b, rest_k, rest_kk = (jnp.broadcast_to(v, (8, LANES)) for v in (on_b, on_k, rest_b, rest_k, rest_kk))
    for r in range(ROWS):
        for h in range(2):
            at = r * LEVELS + h * 8
            b, k, kk = right_side[at : at + 8, :], image[at : at + 8, :], second[at : at + 8, :]
            to = pl.ds(h * 8 * ROWS + r, 8, stride=ROWS)
            increment[to, :] = on_b * b + on_k * k
            residual[to, :] = rest_b * b + rest_k * k + rest_kk * kk


def to_core(x):
    return lax.ppermute(x, LAT, [(i, i ^ 1) for i in range(lax.axis_size(LAT))])


def to_inter(x):
    return lax.ppermute(x, LAT, [(i, ((i + 1) ^ 1) - 1) for i in range(1, lax.axis_size(LAT) - 1)])


def to_even(x):
    return lax.ppermute(x, "lon", [(i, i ^ 1) for i in range(LON)])


def to_odd(x):
    return lax.ppermute(x, "lon", [(i, (((i + 1) % LON ^ 1) - 1) % LON) for i in range(LON)])


def spread_out(x, axes, first):
    count = lax.axis_size(axes)
    group = [(i + first) % count for i in range(count)]
    return lax.all_to_all(x, axes, split_axis=0, concat_axis=0, tiled=True, axis_index_groups=[group])


def shards(courant, obs_matrix, obs_weight, innovation, block_owner, block_row, block_count):
    flow = courant.reshape(-1, LANES)
    owner, row, count = block_owner.reshape(-1), block_row.reshape(-1), block_count
    wholes = (flow, obs_matrix[0], obs_weight[0], innovation[0])
    parcels, for_core, for_inter, for_even, for_odd = call(
        prepare,
        [(LON * PARCEL, LANES), (EDGE, LANES), (EDGE, LANES), (2 * OWN, LANES), (2 * OWN, LANES)],
        (owner, row, count, *wholes),
        4_000_000,
        [pltpu.SMEM((CAP,), jnp.int32), pltpu.SMEM((CAP,), jnp.int32), pltpu.SMEM((1, 1), jnp.int32)]
        + [pltpu.VMEM(x.shape, F32) for x in wholes]
        + [pltpu.VMEM((OWN, LANES), F32), pltpu.SemaphoreType.DMA((7,))],
        [pl.BlockSpec(memory_space=pltpu.HBM)] * 7,
        62,
    )
    parcels = spread_out(parcels.reshape(LON, PARCEL, LANES), "lon", LON // 2).reshape(LON * PARCEL, LANES)
    core, inter = to_core(for_core), to_inter(for_inter)
    wide, strips, for_core, for_inter = call(
        arrange,
        [(WIDE * 2 * LEVELS, LANES), (2 * STRIP, LANES), (MESSAGE, LANES), (MESSAGE, LANES)],
        (flow, parcels, core, inter, to_even(for_even), to_odd(for_odd)),
        2_000_000,
    )
    core, inter = to_core(for_core), to_inter(for_inter)
    (grams,) = call(unpack, [(OWN * LANES, LANES)], (parcels,), 4_000_000)
    cells, listed = (ROWS * LEVELS, LANES), (OWN, LANES)
    work = [pltpu.VMEM((WIDE * LEVELS, LANES), F32)] * 2 + [pltpu.VMEM((WIDE * 8, LANES), F32)] * 2
    work_too = work + [pltpu.VMEM(cells, F32)]
    beside, spots, by_lane, right_side, seen, sums = call(
        first_half,
        [(2 * STRIP, LANES), (2 * LANES, LANES), (16, LANES), cells, listed, (8, LANES)],
        (wide, strips, core, for_core, inter),
        4_000_000,
        work_too,
    )
    rates = (wide, strips, beside)
    short = (HERALD, LANES)
    mine, sums = call(first_terms, [short, (8, LANES)], (grams, seen, sums), 2_000_000)
    core, inter = to_core(mine), to_inter(mine)
    (edges,) = call(edges_of, [(8, LANES)], (core, mine, inter), 10_000)
    lists = (core, mine, inter, to_even(edges), to_odd(edges))
    plane, towers = lax.axis_size(("lat_1", "lon")), lax.axis_size(("lat_0", "lat_2"))
    image, mine, parcels = call(
        second_half, [cells, short, (plane * 2, LANES)], (spots, by_lane, *lists, *rates, grams, sums), 4_000_000, work_too
    )
    parcels = spread_out(parcels.reshape(plane, 2, LANES), ("lat_1", "lon"), middle_of_plane()).reshape(plane * 2, LANES)
    sums, mine = call(gathered, [(towers, LANES), short], (parcels, mine), 10_000)
    core, inter = to_core(mine), to_inter(mine)
    parts = spread_out(sums.reshape(towers, 1, LANES), ("lat_0", "lat_2"), towers * 12 // 16 + 1).reshape(towers, LANES)
    (second,) = call(last_rows, [cells], (spots, by_lane, core, mine, inter, *rates), 4_000_000, work)
    increment, residual = call(finish, [cells, cells], (parts, right_side, image, second), 100_000)
    shape = courant.shape[1:]
    return increment.reshape(shape), residual.reshape(shape)


def solution(mesh):
    torus = Mesh(
        mesh.devices.reshape(-1, 4, 2, mesh.shape["lon"]), ("lat_0", "lat_1", "lat_2", "lon")
    )
    placed = (
        P(None, None, LAT, "lon"),
        P(LAT, "lon", None, None),
        P(LAT, "lon", None),
        P(LAT, "lon", None),
        P(LAT, "lon", None),
        P(LAT, "lon"),
        P(LAT, "lon"),
    )
    return jax.shard_map(
        shards,
        mesh=torus,
        in_specs=placed,
        out_specs=(P(None, LAT, "lon"), P(None, LAT, "lon")),
        check_vma=False,
    )
```

```python
import jax
import jax.numpy as jnp
from jax import lax
from jax.experimental import pallas as pl
from jax.experimental.pallas import tpu as pltpu
from jax.sharding import Mesh
from jax.sharding import PartitionSpec as P


LAT = ("lat_0", "lat_1", "lat_2")
LEVELS = 16
ROWS = 16
LANES = 128
CAP = 8
SLOT = 2
STEPS = 4
HALO = 2 * STEPS
WIDE = ROWS + 2 * HALO
LON = 8
HALF = LANES // 2
OWN = LON * SLOT
BULK = 2 * HALF + 2
LIST = BULK + 6
PARCEL = LIST
EDGE = HALO * 2 * LEVELS
STRIP = HALO * 2 * 8
LEFTS = STRIP + OWN
RIGHTS = LEFTS + OWN
SPOTS = RIGHTS + OWN
MESSAGE = SPOTS + 8
HERALD = OWN + 8
NOWHERE = -4096.0
FIRST = 6
HIGHEST = lax.Precision.HIGHEST
F32 = jnp.float32
VMEM = pl.BlockSpec(memory_space=pltpu.VMEM)
SMEM = pl.BlockSpec(memory_space=pltpu.SMEM)


def lanes(rows):
    return lax.broadcasted_iota(jnp.int32, (rows, LANES), 1)


def places(rows):
    return lax.broadcasted_iota(jnp.int32, (rows, LANES), 0)


def roll(x, shift):
    shift %= LANES
    return pltpu.roll(x, shift, axis=1) if shift else x


def call(body, outs, args, flops, scratch=(), specs=None, room=24):
    return pl.pallas_call(
        body,
        out_shape=[jax.ShapeDtypeStruct(s, F32) for s in outs],
        in_specs=specs or [SMEM if a.dtype == jnp.int32 else VMEM for a in args],
        out_specs=[VMEM] * len(outs),
        scratch_shapes=list(scratch),
        compiler_params=pltpu.CompilerParams(vmem_limit_bytes=room << 20),
        cost_estimate=pl.CostEstimate(flops=flops, bytes_accessed=0, transcendentals=0),
    )(*args)


def turns_of(owners):
    return [sum([(o == owners[j]).astype(jnp.int32) for o in owners[:j]], jnp.int32(0)) for j in range(CAP)]


def chunk(owner):
    return (owner + LON - FIRST) % LON if isinstance(owner, int) else lax.rem(owner + LON - FIRST, LON)


def packed_edges(pick, shift):
    ln = lanes(8)
    out = jnp.zeros((8, LANES), F32)
    for k in range(8):
        low, high = pick(k)
        out = jnp.where((ln >= 16 * k) & (ln < 16 * k + 8), roll(low, 16 * k + shift), out)
        out = jnp.where((ln >= 16 * k + 8) & (ln < 16 * k + 16), roll(high, 16 * k + 8 + shift), out)
    return out


def weigh_blocks(owners, turns, count, matrix, weight, parcels):
    ln, rw = lanes(HALF), places(HALF)
    for j in range(CAP):
        block = matrix[j]
        scaled = jnp.transpose(block) * jnp.where(j < count[0, 0], weight[j : j + 1, :], 0.0)
        gram = jnp.dot(scaled, block, precision=HIGHEST, preferred_element_type=F32)
        top, low = gram[:HALF], gram[HALF:]
        packed = jnp.where((ln >= HALF) & (ln - HALF <= rw), roll(top, HALF), low)
        diagonal = jnp.sum(jnp.where(ln - HALF == rw, low, 0.0), axis=0, keepdims=True)
        at = chunk(owners[j]) * PARCEL + turns[j] * HALF
        parcels[pl.ds(pl.multiple_of(at, 8), HALF), :] = packed
        parcels[pl.ds(chunk(owners[j]) * PARCEL + 2 * HALF + turns[j], 1), :] = diagonal


def prepare(owner_at, row_at, count_at, matrix_at, weight_at, innovation_at, parcels, owner, row, count, matrix, weight, innovation, lists, sems):
    pairs = ((matrix_at, matrix), (owner_at, owner), (row_at, row), (count_at, count), (weight_at, weight), (innovation_at, innovation))
    copies = [pltpu.make_async_copy(a, b, sems.at[i]) for i, (a, b) in enumerate(pairs)]
    for copy in copies:
        copy.start()
    for d in range(LON):
        parcels[d * PARCEL : d * PARCEL + LIST, :] = jnp.zeros((LIST, LANES), F32)
    lists[...] = jnp.zeros(lists.shape, F32)
    for copy in copies:
        copy.wait()
    owners = [owner[j] for j in range(CAP)]
    turns = turns_of(owners)
    column = jnp.transpose(weight[...] * innovation[...])
    ln = lanes(8)
    named = jnp.full((8, LANES), NOWHERE, F32)
    for j in range(CAP):
        live = j < count[0, 0]
        total = jnp.zeros((8, LANES), F32)
        for k in range(LANES // 8):
            total += matrix[j, k * 8 : k * 8 + 8, :] * column[k * 8 : k * 8 + 8, j : j + 1]
        slot = owners[j] * SLOT + turns[j]
        lists[pl.ds(slot, 1), :] = jnp.where(live, jnp.sum(total, axis=0, keepdims=True), 0.0)
        place = jnp.where(live, (lax.rem(row[j], ROWS) + HALO) * LEVELS + lax.div(row[j], ROWS), int(NOWHERE)).astype(F32)
        named = jnp.where(ln == slot, place, named)
    weigh_blocks(owners, turns, count, matrix, weight, parcels)
    named = jnp.where(ln < OWN, named, roll(named, OWN))
    line = lanes(1)
    for d in range(LON):
        left, right = 2 * (d - 1) % OWN, 2 * (d + 1) % OWN
        at = chunk(d) * PARCEL + BULK
        parcels[at : at + 2, :] = lists[2 * d : 2 * d + 2, :]
        edge = jnp.where(line < 8, roll(lists[left : left + 1, :], 8), roll(lists[left + 1 : left + 2, :], 16))
        edge = jnp.where(line < 16, edge, jnp.where(line < 24, roll(lists[right : right + 1, :], 16), roll(lists[right + 1 : right + 2, :], 24)))
        parcels[at + 2 : at + 3, :] = edge
        parcels[at + 3 : at + 4, :] = roll(named, -left)[:1]


def halo(flow, to_core, to_inter, to_even, to_odd):
    even = lax.axis_index("lat_2") == 0
    here = lax.rem(lax.axis_index("lon"), 2) == 0
    for f in range(2):
        for g in range(2):

            def pick(k, f=f, g=g):
                at = f * LEVELS * ROWS + g * 8 + k
                return flow[pl.ds(at, 8, stride=ROWS), :], flow[pl.ds(at + 8 * ROWS, 8, stride=ROWS), :]

            at = (f * 2 + g) * 8
            to_right, to_left = packed_edges(pick, 8), packed_edges(pick, 0)
            to_even[at : at + 8, :] = jnp.where(here, to_right, to_left)
            to_odd[at : at + 8, :] = jnp.where(here, to_left, to_right)
        for i in range(HALO):
            for h in range(2):
                at = f * LEVELS * ROWS + h * 8 * ROWS + i
                up, down = flow[pl.ds(at + ROWS - HALO, 8, stride=ROWS), :], flow[pl.ds(at, 8, stride=ROWS), :]
                at = (i * 2 + f) * LEVELS + h * 8
                to_core[at : at + 8, :] = jnp.where(even, up, down)
                to_inter[at : at + 8, :] = jnp.where(even, down, up)


def arrange(flow, parcels, core, inter, even_edges, odd_edges, wide, strips, to_core, to_inter):
    ln = lanes(8)
    here = lax.rem(lax.axis_index("lon"), 2) == 0
    even = lax.axis_index("lat_2") == 0
    wide[:EDGE, :] = jnp.where(even, inter[...], core[...])
    wide[EDGE + ROWS * 2 * LEVELS :, :] = jnp.where(even, core[...], inter[...])
    for f in range(2):
        for g in range(2):
            at = (f * 2 + g) * 8
            first, second = even_edges[at : at + 8, :], odd_edges[at : at + 8, :]
            left, right = jnp.where(here, second, first), jnp.where(here, first, second)
            for k in range(8):
                at = f * LEVELS * ROWS + g * 8 + k
                low, high = flow[pl.ds(at, 8, stride=ROWS), :], flow[pl.ds(at + 8 * ROWS, 8, stride=ROWS), :]
                at = EDGE + ((g * 8 + k) * 2 + f) * LEVELS
                wide[at : at + 8, :] = low
                wide[at + 8 : at + 16, :] = high
                a = jnp.where(ln < 8, roll(left, -16 * k), jnp.where(ln < 32, roll(low, 8), jnp.where(ln < 56, roll(low, 56), roll(right, 56 - 16 * k))))
                b = jnp.where(ln < 72, roll(left, 56 - 16 * k), jnp.where(ln < 96, roll(high, 72), jnp.where(ln < 120, roll(high, 120), roll(right, 112 - 16 * k))))
                strip = jnp.where(ln < HALF, a, b)
                at = ((g * 8 + k) * 2 + f) * 8
                strips[at : at + 8, :] = strip
    lower, upper = strips[:STRIP, :], strips[STRIP:, :]
    to_core[:STRIP, :] = jnp.where(even, upper, lower)
    to_inter[:STRIP, :] = jnp.where(even, lower, upper)
    edge = parcels[pl.ds(BULK + 2, LON, stride=PARCEL), :]
    named = parcels[pl.ds(BULK + 3, LON, stride=PARCEL), :]
    turned = jnp.transpose(named)
    spot = jnp.full((1, LANES), NOWHERE, F32)
    line = lanes(1)
    for i, k in enumerate((2, 3, 0, 1, 4, 5)):
        line_k = jnp.concatenate([turned[k : k + 1, :], jnp.zeros((1, LANES - LON), F32)], axis=1)
        spot = jnp.where((line >= 8 * i) & (line < 8 * i + 8), roll(line_k, 8 * i), spot)
    for o in range(SLOT):
        own = parcels[pl.ds(BULK + o, LON, stride=PARCEL), :]
        left = jnp.where(ln < 8, roll(edge, -8 * o), 0.0)
        right = jnp.where((ln >= 56) & (ln < 64), roll(edge, 40 - 8 * o), 0.0)
        for out in (to_core, to_inter):
            out[STRIP + o * LON : STRIP + (o + 1) * LON, :] = own
            out[LEFTS + o * LON : LEFTS + (o + 1) * LON, :] = left
            out[RIGHTS + o * LON : RIGHTS + (o + 1) * LON, :] = right
    for out in (to_core, to_inter):
        out[SPOTS:, :] = jnp.broadcast_to(spot, (8, LANES))


def unpack(parcels, grams):
    ln, rw = lanes(HALF), places(HALF)
    upper, diagonal, first = ln - HALF > rw, ln - HALF == rw, ln < HALF
    for s in range(LON):
        both = parcels[s * PARCEL : s * PARCEL + 2 * HALF, :]
        turned = jnp.transpose(both)
        ct, et = turned[:HALF], turned[HALF:]
        ct_rolled, et_rolled = roll(ct, HALF), roll(et, HALF)
        for o in range(SLOT):
            q = both[o * HALF : (o + 1) * HALF]
            d = parcels[s * PARCEL + 2 * HALF + o : s * PARCEL + 2 * HALF + o + 1, :]
            e_first, e_last = (et, et_rolled) if o == 0 else (et_rolled, et)
            c_last = ct_rolled if o == 0 else ct
            top = jnp.where(first, jnp.where(ln <= rw, roll(q, HALF), e_first), c_last)
            low = jnp.where(first | upper, q, jnp.where(diagonal, d, e_last))
            at = (o * LON + s) * LANES
            grams[at : at + HALF, :] = top
            grams[at + HALF : at + LANES, :] = low


def split(x):
    high = x.astype(jnp.bfloat16)
    rest = x - high.astype(F32)
    middle = rest.astype(jnp.bfloat16)
    low = (rest - middle.astype(F32)).astype(jnp.bfloat16)
    return jnp.concatenate([high, middle, low], axis=1)


def chosen(one_hot, parts):
    out = jnp.dot(one_hot, parts, preferred_element_type=F32)
    return out[:, :LANES] + out[:, LANES : 2 * LANES] + out[:, 2 * LANES :]


def one_hot(index, at):
    return jnp.where(index == at, 1.0, 0.0).astype(jnp.bfloat16)


def padded(x, rows):
    return jnp.concatenate([x, jnp.zeros((rows - x.shape[0], LANES), F32)], axis=0)


def right_strips(x):
    ln = lanes(x.shape[0])
    return jnp.where((ln >= 56) & (ln < 64), roll(x, 56), 0.0)


def lay_out(spots, by_lane, own, sides, field, strips, low, high):
    ln = lanes(LANES)
    own_strip = jnp.where(ln < 32, jnp.where(ln >= 8, roll(own, 8), 0.0), jnp.where(ln < 56, roll(own, 56), 0.0))
    pieces = []
    for i, strip in enumerate((own_strip, sides)):
        upper = (spots[i * LANES : (i + 1) * LANES, :].astype(jnp.int32) & 8) != 0
        pieces.append(split(jnp.where(upper, roll(strip, HALF), strip)))
    own_parts = split(own)
    lane_spots = [by_lane[i * 8 : i * 8 + 1, :].astype(jnp.int32) for i in range(2)]
    p = jnp.broadcast_to(lane_spots[0], (LANES, LANES))
    for start in range(low * LEVELS, high * LEVELS, LANES):
        field[start : start + LANES, :] = chosen(one_hot(places(LANES) + start, p), own_parts)
    folded = [jnp.broadcast_to(((b >> 4) << 3) + (b & 7), (64, LANES)) for b in lane_spots]
    for start in range(low * 8, high * 8, 64):
        at = places(64) + start
        strips[start : start + 64, :] = chosen(one_hot(at, folded[0]), pieces[0]) + chosen(one_hot(at, folded[1]), pieces[1])


def adjoint(rates, source, target, first, last, height):
    before = kept = None
    for r in range(first, last + 1):
        y = source[r * height : (r + 1) * height, :]
        lat, lon = rates(r)
        t = lat * y
        a = jnp.where(lat > 0.0, t, 0.0)
        b = a - t
        s = lon * y
        e = jnp.where(lon > 0.0, s, 0.0)
        f = e - s
        if r > first + 1:
            target[(r - 1) * height : r * height, :] = kept + a
        if r > first:
            kept = y - (a + b) - (e + f) + roll(e, -1) + roll(f, 1) + before
        before = b


def tangent(rates, source, target, first, last, height):
    for r in range(first + 1, last):
        x = source[r * height : (r + 1) * height, :]
        south = source[(r - 1) * height : r * height, :]
        north = source[(r + 1) * height : (r + 2) * height, :]
        lat, lon = rates(r)
        out = x + jnp.abs(lat) * (jnp.where(lat > 0.0, south, north) - x)
        target[r * height : (r + 1) * height, :] = out + jnp.abs(lon) * (jnp.where(lon > 0.0, roll(x, 1), roll(x, -1)) - x)


def merged(field, strips, r):
    ln = lanes(8)
    t = strips[r * 8 : (r + 1) * 8, :]
    low, high = field[r * LEVELS : r * LEVELS + 8, :], field[r * LEVELS + 8 : (r + 1) * LEVELS, :]
    low = jnp.where(ln < 8, roll(t, -8), jnp.where(ln >= 120, roll(t, 72), low))
    high = jnp.where(ln < 8, roll(t, -72), jnp.where(ln >= 120, roll(t, 8), high))
    return low, high


def steps_back(rates, fields, strips, first):
    full, narrow = rates
    for k in range(first, first + STEPS):
        adjoint(full, *fields, k, WIDE - 1 - k, LEVELS)
        adjoint(narrow, *strips, k, WIDE - 1 - k, 8)
        fields, strips = fields[::-1], strips[::-1]
    return fields, strips


def steps_on(rates, fields, strips, first):
    full, narrow = rates
    for k in range(first, first + STEPS):
        tangent(full, *fields, k, WIDE - 1 - k, LEVELS)
        tangent(narrow, *strips, k, WIDE - 1 - k, 8)
        fields, strips = fields[::-1], strips[::-1]
    return fields, strips


def rates_of(wide, mine, beside):
    def full(r):
        at = r * 2 * LEVELS
        return wide[at : at + LEVELS, :], wide[at + LEVELS : at + 2 * LEVELS, :]

    def narrow(r):
        ref, r = (mine, r - HALO) if HALO <= r < HALO + ROWS else (beside, r if r < HALO else r - ROWS)
        return ref[r * 16 : r * 16 + 8, :], ref[r * 16 + 8 : r * 16 + 16, :]

    return full, narrow


def back_and_on(spots, by_lane, own, sides, rates, kept, fields, strips, image):
    lay_out(spots, by_lane, own, sides, fields[0], strips[0], 0, WIDE)
    fields, strips = steps_back(rates, fields, strips, 0)
    lat, last = lax.axis_index(LAT), lax.axis_size(LAT) - 1
    for outside, start in ((lat == 0, STEPS), (lat == last, HALO + ROWS)):
        for ref, height in ((fields[0], LEVELS), (strips[0], 8)):
            block = ref[start * height : (start + STEPS) * height, :]
            ref[start * height : (start + STEPS) * height, :] = jnp.where(outside, 0.0, block)
    square = jnp.zeros((8, LANES), F32)
    for r in range(ROWS):
        low, high = merged(fields[0], strips[0], r + HALO)
        kept[r * LEVELS : r * LEVELS + 8, :] = low
        kept[r * LEVELS + 8 : (r + 1) * LEVELS, :] = high
        square += low * low + high * high
    fields, strips = steps_on(rates, fields, strips, STEPS)
    for r in range(ROWS):
        low, high = merged(fields[0], strips[0], r + HALO)
        image[r * LEVELS : r * LEVELS + 8, :] = low
        image[r * LEVELS + 8 : (r + 1) * LEVELS, :] = high
    mine = spots[OWN : 2 * OWN, :].astype(jnp.int32) - HALO * LEVELS
    hit = jnp.concatenate([one_hot(lanes(OWN), mine), one_hot(lanes(OWN) + LANES, mine)], axis=1)
    return jnp.sum(square, keepdims=True), chosen(hit, split(image[...]))


def weigh(seen, grams):
    column = jnp.transpose(seen)
    out = []
    for t in range(OWN):
        total = jnp.zeros((8, LANES), F32)
        for k in range(LANES // 8):
            at = t * LANES + k * 8
            total += grams[at : at + 8, :] * column[k * 8 : k * 8 + 8, t : t + 1]
        out.append(jnp.sum(total, axis=0, keepdims=True))
    return jnp.concatenate(out, axis=0)


def in_lanes(first, values):
    ln = lanes(8)
    out = jnp.zeros((8, LANES), F32)
    for i, v in enumerate(values):
        out = jnp.where(ln == first + i, v, out)
    return out


def first_half(wide, mine, core, own_message, inter, beside, spots, by_lane, kept, seen, sums, field, other, strip, other_strip, image):
    ln = lanes(8)
    even = lax.axis_index("lat_2") == 0
    beside[:STRIP, :] = jnp.where(even, inter[:STRIP, :], core[:STRIP, :])
    beside[STRIP:, :] = jnp.where(even, core[:STRIP, :], inter[:STRIP, :])
    step = jnp.where(even, float(ROWS * LEVELS), -float(ROWS * LEVELS))
    c, o, i = core[SPOTS:, :] + step, own_message[SPOTS:, :], inter[SPOTS:, :] - step
    tables = (((c, 0), (o, 0), (i, 0)), ((c, 16), (o, 16), (i, 16), (c, 32), (o, 32), (i, 32)))
    for t, table in enumerate(tables):
        spot = jnp.full((8, LANES), NOWHERE, F32)
        for n, (x, at) in enumerate(table):
            spot = jnp.where((ln >= OWN * n) & (ln < OWN * (n + 1)), roll(x, OWN * n - at), spot)
        by_lane[t * 8 : t * 8 + 8, :] = spot
        spots[t * LANES : (t + 1) * LANES, :] = jnp.transpose(jnp.broadcast_to(spot[:1], (LANES, LANES)))
    parts = (core, own_message, inter)
    own = padded(jnp.concatenate([x[STRIP:LEFTS, :] for x in parts], axis=0), LANES)
    sides = padded(jnp.concatenate([x[LEFTS:RIGHTS, :] for x in parts] + [x[RIGHTS:SPOTS, :] for x in parts], axis=0), LANES)
    square, rows = back_and_on(spots, by_lane, own, sides, rates_of(wide, mine, beside), kept, (field, other), (strip, other_strip), image)
    seen[...] = rows
    sums[...] = in_lanes(0, [square])


def stepped(x, unit):
    row = places(OWN)
    for bit in range(4):
        x = jnp.where((row & (1 << bit)) != 0, roll(x, unit << bit), x)
    return x


def herald(rows, message):
    mine = (lanes(OWN) >> 3) == places(OWN)
    message[:OWN, :] = rows
    message[OWN : OWN + 1, :] = jnp.sum(jnp.where(mine, stepped(rows, 8), 0.0), axis=0, keepdims=True)
    message[OWN + 1 : OWN + 2, :] = jnp.sum(jnp.where(mine, stepped(roll(rows, 8), 8), 0.0), axis=0, keepdims=True)
    message[OWN + 2 :, :] = jnp.zeros((HERALD - OWN - 2, LANES), F32)


def first_terms(grams, seen, before, message, sums):
    rows = weigh(seen[...], grams)
    herald(rows, message)
    sums[...] = before[...] + in_lanes(1, [jnp.sum(seen[...] * rows, keepdims=True)])


def edges_of(core, mine, inter, out):
    for i, x in enumerate((core, mine, inter)):
        out[i : i + 1, :] = x[OWN : OWN + 1, :]
        out[i + 3 : i + 4, :] = x[OWN + 1 : OWN + 2, :]
    out[6:, :] = jnp.zeros((2, LANES), F32)


def side_strips(lefts, rights):
    ln = lanes(OWN)
    rows = [stepped(jnp.broadcast_to(x, (OWN, LANES)), -8) for x in lefts]
    out = [jnp.where(ln < 8, x, 0.0) for x in rows]
    rows = [stepped(jnp.broadcast_to(x, (OWN, LANES)), -8) for x in rights]
    return padded(jnp.concatenate(out + [right_strips(x) for x in rows], axis=0), LANES)


def second_half(spots, by_lane, core, mine, inter, even, odd, wide, strips, beside, grams, before, kept, message, out, field, other, strip, other_strip, image):
    own = padded(jnp.concatenate([x[:OWN, :] for x in (core, mine, inter)], axis=0), LANES)
    here = lax.rem(lax.axis_index("lon"), 2) == 0
    left, right = jnp.where(here, odd[...], even[...]), jnp.where(here, even[...], odd[...])
    sides = side_strips([left[i : i + 1] for i in (3, 4, 5)], [right[i : i + 1] for i in (0, 1, 2)])
    square, seen = back_and_on(
        spots, by_lane, own, sides, rates_of(wide, strips, beside), kept, (field, other), (strip, other_strip), image
    )
    rows = weigh(seen, grams)
    herald(rows, message)
    sums = before[...] + in_lanes(2, [square, jnp.sum(seen * rows, keepdims=True)])
    out[...] = jnp.concatenate([sums] * (out.shape[0] // 8), axis=0)
    for step, row in ((1, OWN + 1), (-1, OWN)):
        out[pl.ds(in_plane(step) * 2 + 1, 1), :] = message[row : row + 1, :]


def in_plane(step):
    size = lax.axis_size(("lat_1", "lon"))
    at = lax.axis_index("lat_1") * LON + lax.rem(lax.axis_index("lon") + LON + step, LON)
    return lax.rem(at + size - middle_of_plane(), size)


def middle_of_plane():
    return lax.axis_size("lat_1") // 2 * LON + LON // 2


def gathered(parts, mine, sums, message):
    count = parts.shape[0] // 2
    sums[...] = jnp.broadcast_to(jnp.sum(parts[pl.ds(0, count, stride=2), :], axis=0, keepdims=True), sums.shape)
    message[...] = mine[...]
    for i, step in enumerate((-1, 1)):
        message[OWN + i : OWN + i + 1, :] = parts[pl.ds(in_plane(step) * 2 + 1, 1), :]


def finish(spots, by_lane, core, mine, inter, wide, strips, beside, parts, right_side, image, increment, residual, field, other, strip, other_strip):
    lists = (core, mine, inter)
    own = padded(jnp.concatenate([x[:OWN, :] for x in lists], axis=0), LANES)
    sides = side_strips(*([x[OWN + i : OWN + i + 1, :] for x in lists] for i in range(2)))
    lay_out(spots, by_lane, own, sides, field, strip, HALO - STEPS, HALO + ROWS + STEPS)
    fields, narrow = steps_back(rates_of(wide, strips, beside), (field, other), (strip, other_strip), STEPS)
    total = jnp.sum(parts[...], axis=0, keepdims=True)
    m0, m1, m2, m3 = (jnp.sum(jnp.where(lanes(1) == i, total, 0.0), keepdims=True) for i in range(4))
    step_0 = m0 / (m0 + m1)
    rho = m1 / m0
    spread = m2 - rho * m1
    curve = (m3 - rho * m2) - rho * (m2 - rho * m1)
    gamma = step_0 * spread / m0
    step_1 = spread / (spread + curve - gamma * spread)
    on_b = step_0 * (1.0 + step_1 * (gamma + rho))
    on_k = -step_0 * step_1
    rest_b = step_0 * ((1.0 - step_1) * rho - step_1 * gamma)
    rest_k = -step_0 * ((1.0 - step_1) + step_1 * (rho + gamma))
    rest_kk = step_0 * step_1
    on_b, on_k, rest_b, rest_k, rest_kk = (jnp.broadcast_to(v, (8, LANES)) for v in (on_b, on_k, rest_b, rest_k, rest_kk))
    for r in range(ROWS):
        for h, second in enumerate(merged(fields[0], narrow[0], r + HALO)):
            at = r * LEVELS + h * 8
            b, first = right_side[at : at + 8, :], image[at : at + 8, :]
            to = pl.ds(h * 8 * ROWS + r, 8, stride=ROWS)
            increment[to, :] = on_b * b + on_k * first
            residual[to, :] = rest_b * b + rest_k * first + rest_kk * second


def to_core(x):
    return lax.ppermute(x, LAT, [(i, i ^ 1) for i in range(lax.axis_size(LAT))])


def to_inter(x):
    return lax.ppermute(x, LAT, [(i, ((i + 1) ^ 1) - 1) for i in range(1, lax.axis_size(LAT) - 1)])


def to_even(x):
    return lax.ppermute(x, "lon", [(i, i ^ 1) for i in range(LON)])


def to_odd(x):
    return lax.ppermute(x, "lon", [(i, (((i + 1) % LON ^ 1) - 1) % LON) for i in range(LON)])


def spread_out(x, axes, first):
    count = lax.axis_size(axes)
    group = [(i + first) % count for i in range(count)]
    return lax.all_to_all(x, axes, split_axis=0, concat_axis=0, tiled=True, axis_index_groups=[group])


def shards(courant, obs_matrix, obs_weight, innovation, block_owner, block_row, block_count):
    flow = courant.reshape(-1, LANES)
    owner, row, count = block_owner.reshape(-1), block_row.reshape(-1), block_count
    wholes = (obs_matrix[0], obs_weight[0], innovation[0])
    (parcels,) = call(
        prepare,
        [(LON * PARCEL, LANES)],
        (owner, row, count, *wholes),
        4_000_000,
        [pltpu.SMEM((CAP,), jnp.int32), pltpu.SMEM((CAP,), jnp.int32), pltpu.SMEM((1, 1), jnp.int32)]
        + [pltpu.VMEM(x.shape, F32) for x in wholes]
        + [pltpu.VMEM((OWN, LANES), F32), pltpu.SemaphoreType.DMA((6,))],
        [pl.BlockSpec(memory_space=pltpu.HBM)] * 6,
        62,
    )
    parcels = spread_out(parcels.reshape(LON, PARCEL, LANES), "lon", FIRST).reshape(LON * PARCEL, LANES)
    edge = (EDGE, LANES), (2 * OWN, LANES)
    for_core, for_inter, for_even, for_odd = call(halo, [edge[0], edge[0], edge[1], edge[1]], (flow,), 1_000_000)
    core, inter = to_core(for_core), to_inter(for_inter)
    wide, strips, for_core, for_inter = call(
        arrange,
        [(WIDE * 2 * LEVELS, LANES), (2 * STRIP, LANES), (MESSAGE, LANES), (MESSAGE, LANES)],
        (flow, parcels, core, inter, to_even(for_even), to_odd(for_odd)),
        2_000_000,
    )
    core, inter = to_core(for_core), to_inter(for_inter)
    (grams,) = call(unpack, [(OWN * LANES, LANES)], (parcels,), 4_000_000)
    cells, listed = (ROWS * LEVELS, LANES), (OWN, LANES)
    work = [pltpu.VMEM((WIDE * LEVELS, LANES), F32)] * 2 + [pltpu.VMEM((WIDE * 8, LANES), F32)] * 2
    work_too = work + [pltpu.VMEM(cells, F32)]
    beside, spots, by_lane, right_side, seen, sums = call(
        first_half,
        [(2 * STRIP, LANES), (2 * LANES, LANES), (16, LANES), cells, listed, (8, LANES)],
        (wide, strips, core, for_core, inter),
        4_000_000,
        work_too,
    )
    rates = (wide, strips, beside)
    short = (HERALD, LANES)
    mine, sums = call(first_terms, [short, (8, LANES)], (grams, seen, sums), 2_000_000)
    core, inter = to_core(mine), to_inter(mine)
    (edges,) = call(edges_of, [(8, LANES)], (core, mine, inter), 10_000)
    lists = (core, mine, inter, to_even(edges), to_odd(edges))
    plane, towers = lax.axis_size(("lat_1", "lon")), lax.axis_size(("lat_0", "lat_2"))
    image, mine, parcels = call(
        second_half, [cells, short, (plane * 2, LANES)], (spots, by_lane, *lists, *rates, grams, sums), 4_000_000, work_too
    )
    parcels = spread_out(parcels.reshape(plane, 2, LANES), ("lat_1", "lon"), middle_of_plane()).reshape(plane * 2, LANES)
    sums, mine = call(gathered, [(towers, LANES), short], (parcels, mine), 10_000)
    core, inter = to_core(mine), to_inter(mine)
    parts = spread_out(sums.reshape(towers, 1, LANES), ("lat_0", "lat_2"), towers * 12 // 16 + 1).reshape(towers, LANES)
    increment, residual = call(
        finish, [cells, cells], (spots, by_lane, core, mine, inter, *rates, parts, right_side, image), 2_000_000, work
    )
    shape = courant.shape[1:]
    return increment.reshape(shape), residual.reshape(shape)


def solution(mesh):
    torus = Mesh(
        mesh.devices.reshape(-1, 4, 2, mesh.shape["lon"]), ("lat_0", "lat_1", "lat_2", "lon")
    )
    placed = (
        P(None, None, LAT, "lon"),
        P(LAT, "lon", None, None),
        P(LAT, "lon", None),
        P(LAT, "lon", None),
        P(LAT, "lon", None),
        P(LAT, "lon"),
        P(LAT, "lon"),
    )
    return jax.shard_map(
        shards,
        mesh=torus,
        in_specs=placed,
        out_specs=(P(None, LAT, "lon"), P(None, LAT, "lon")),
        check_vma=False,
    )
```

```python
import jax
import jax.numpy as jnp
from jax import lax
from jax.experimental import pallas as pl
from jax.experimental.pallas import tpu as pltpu
from jax.sharding import Mesh
from jax.sharding import PartitionSpec as P


LAT = ("lat_0", "lat_1", "lat_2")
LEVELS = 16
ROWS = 16
LANES = 128
CAP = 8
SLOT = 2
STEPS = 4
HALO = 2 * STEPS
WIDE = ROWS + 2 * HALO
LON = 8
HALF = LANES // 2
OWN = LON * SLOT
BULK = 2 * HALF + 2
LIST = BULK + 6
PARCEL = LIST
EDGE = HALO * 2 * LEVELS
STRIP = HALO * 2 * 8
LEFTS = STRIP + OWN
RIGHTS = LEFTS + OWN
SPOTS = RIGHTS + OWN
MESSAGE = SPOTS + 8
HERALD = OWN + 8
NOWHERE = -4096.0
FIRST = 6
HIGHEST = lax.Precision.HIGHEST
F32 = jnp.float32
VMEM = pl.BlockSpec(memory_space=pltpu.VMEM)
SMEM = pl.BlockSpec(memory_space=pltpu.SMEM)


def lanes(rows):
    return lax.broadcasted_iota(jnp.int32, (rows, LANES), 1)


def places(rows):
    return lax.broadcasted_iota(jnp.int32, (rows, LANES), 0)


def roll(x, shift):
    shift %= LANES
    return pltpu.roll(x, shift, axis=1) if shift else x


def call(body, outs, args, flops, scratch=(), specs=None, room=24):
    return pl.pallas_call(
        body,
        out_shape=[jax.ShapeDtypeStruct(s, F32) for s in outs],
        in_specs=specs or [SMEM if a.dtype == jnp.int32 else VMEM for a in args],
        out_specs=[VMEM] * len(outs),
        scratch_shapes=list(scratch),
        compiler_params=pltpu.CompilerParams(vmem_limit_bytes=room << 20),
        cost_estimate=pl.CostEstimate(flops=flops, bytes_accessed=0, transcendentals=0),
    )(*args)


def turns_of(owners):
    return [sum([(o == owners[j]).astype(jnp.int32) for o in owners[:j]], jnp.int32(0)) for j in range(CAP)]


def chunk(owner):
    return (owner + LON - FIRST) % LON if isinstance(owner, int) else lax.rem(owner + LON - FIRST, LON)


def packed_edges(pick, shift):
    ln = lanes(8)
    out = jnp.zeros((8, LANES), F32)
    for k in range(8):
        low, high = pick(k)
        out = jnp.where((ln >= 16 * k) & (ln < 16 * k + 8), roll(low, 16 * k + shift), out)
        out = jnp.where((ln >= 16 * k + 8) & (ln < 16 * k + 16), roll(high, 16 * k + 8 + shift), out)
    return out


def weigh_blocks(owners, turns, count, matrix, weight, parcels):
    ln, rw = lanes(HALF), places(HALF)
    for j in range(CAP):
        block = matrix[j]
        scaled = jnp.transpose(block) * jnp.where(j < count[0, 0], weight[j : j + 1, :], 0.0)
        gram = jnp.dot(scaled, block, precision=HIGHEST, preferred_element_type=F32)
        top, low = gram[:HALF], gram[HALF:]
        packed = jnp.where((ln >= HALF) & (ln - HALF <= rw), roll(top, HALF), low)
        diagonal = jnp.sum(jnp.where(ln - HALF == rw, low, 0.0), axis=0, keepdims=True)
        at = chunk(owners[j]) * PARCEL + turns[j] * HALF
        parcels[pl.ds(pl.multiple_of(at, 8), HALF), :] = packed
        parcels[pl.ds(chunk(owners[j]) * PARCEL + 2 * HALF + turns[j], 1), :] = diagonal


def prepare(owner_at, row_at, count_at, matrix_at, weight_at, innovation_at, parcels, owner, row, count, matrix, weight, innovation, lists, sems):
    pairs = ((matrix_at, matrix), (owner_at, owner), (row_at, row), (count_at, count), (weight_at, weight), (innovation_at, innovation))
    copies = [pltpu.make_async_copy(a, b, sems.at[i]) for i, (a, b) in enumerate(pairs)]
    for copy in copies:
        copy.start()
    for d in range(LON):
        parcels[d * PARCEL : d * PARCEL + LIST, :] = jnp.zeros((LIST, LANES), F32)
    lists[...] = jnp.zeros(lists.shape, F32)
    for copy in copies:
        copy.wait()
    owners = [owner[j] for j in range(CAP)]
    turns = turns_of(owners)
    column = jnp.transpose(weight[...] * innovation[...])
    ln = lanes(8)
    named = jnp.full((8, LANES), NOWHERE, F32)
    for j in range(CAP):
        live = j < count[0, 0]
        total = jnp.zeros((8, LANES), F32)
        for k in range(LANES // 8):
            total += matrix[j, k * 8 : k * 8 + 8, :] * column[k * 8 : k * 8 + 8, j : j + 1]
        slot = owners[j] * SLOT + turns[j]
        lists[pl.ds(slot, 1), :] = jnp.where(live, jnp.sum(total, axis=0, keepdims=True), 0.0)
        place = jnp.where(live, (lax.rem(row[j], ROWS) + HALO) * LEVELS + lax.div(row[j], ROWS), int(NOWHERE)).astype(F32)
        named = jnp.where(ln == slot, place, named)
    weigh_blocks(owners, turns, count, matrix, weight, parcels)
    named = jnp.where(ln < OWN, named, roll(named, OWN))
    line = lanes(1)
    for d in range(LON):
        left, right = 2 * (d - 1) % OWN, 2 * (d + 1) % OWN
        at = chunk(d) * PARCEL + BULK
        parcels[at : at + 2, :] = lists[2 * d : 2 * d + 2, :]
        edge = jnp.where(line < 8, roll(lists[left : left + 1, :], 8), roll(lists[left + 1 : left + 2, :], 16))
        edge = jnp.where(line < 16, edge, jnp.where(line < 24, roll(lists[right : right + 1, :], 16), roll(lists[right + 1 : right + 2, :], 24)))
        parcels[at + 2 : at + 3, :] = edge
        parcels[at + 3 : at + 4, :] = roll(named, -left)[:1]


def halo(flow, to_core, to_inter, to_even, to_odd):
    even = lax.axis_index("lat_2") == 0
    here = lax.rem(lax.axis_index("lon"), 2) == 0
    for f in range(2):
        for g in range(2):

            def pick(k, f=f, g=g):
                at = f * LEVELS * ROWS + g * 8 + k
                return flow[pl.ds(at, 8, stride=ROWS), :], flow[pl.ds(at + 8 * ROWS, 8, stride=ROWS), :]

            at = (f * 2 + g) * 8
            to_right, to_left = packed_edges(pick, 8), packed_edges(pick, 0)
            to_even[at : at + 8, :] = jnp.where(here, to_right, to_left)
            to_odd[at : at + 8, :] = jnp.where(here, to_left, to_right)
        for i in range(HALO):
            for h in range(2):
                at = f * LEVELS * ROWS + h * 8 * ROWS + i
                up, down = flow[pl.ds(at + ROWS - HALO, 8, stride=ROWS), :], flow[pl.ds(at, 8, stride=ROWS), :]
                at = (i * 2 + f) * LEVELS + h * 8
                to_core[at : at + 8, :] = jnp.where(even, up, down)
                to_inter[at : at + 8, :] = jnp.where(even, down, up)


def arrange(flow, parcels, core, inter, even_edges, odd_edges, wide, strips, to_core, to_inter):
    ln = lanes(8)
    here = lax.rem(lax.axis_index("lon"), 2) == 0
    even = lax.axis_index("lat_2") == 0
    wide[:EDGE, :] = jnp.where(even, inter[...], core[...])
    wide[EDGE + ROWS * 2 * LEVELS :, :] = jnp.where(even, core[...], inter[...])
    for f in range(2):
        for g in range(2):
            at = (f * 2 + g) * 8
            first, second = even_edges[at : at + 8, :], odd_edges[at : at + 8, :]
            left, right = jnp.where(here, second, first), jnp.where(here, first, second)
            for k in range(8):
                at = f * LEVELS * ROWS + g * 8 + k
                low, high = flow[pl.ds(at, 8, stride=ROWS), :], flow[pl.ds(at + 8 * ROWS, 8, stride=ROWS), :]
                at = EDGE + ((g * 8 + k) * 2 + f) * LEVELS
                wide[at : at + 8, :] = low
                wide[at + 8 : at + 16, :] = high
                a = jnp.where(ln < 8, roll(left, -16 * k), jnp.where(ln < 32, roll(low, 8), jnp.where(ln < 56, roll(low, 56), roll(right, 56 - 16 * k))))
                b = jnp.where(ln < 72, roll(left, 56 - 16 * k), jnp.where(ln < 96, roll(high, 72), jnp.where(ln < 120, roll(high, 120), roll(right, 112 - 16 * k))))
                strip = jnp.where(ln < HALF, a, b)
                at = ((g * 8 + k) * 2 + f) * 8
                strips[at : at + 8, :] = strip
    lower, upper = strips[:STRIP, :], strips[STRIP:, :]
    to_core[:STRIP, :] = jnp.where(even, upper, lower)
    to_inter[:STRIP, :] = jnp.where(even, lower, upper)
    edge = parcels[pl.ds(BULK + 2, LON, stride=PARCEL), :]
    named = parcels[pl.ds(BULK + 3, LON, stride=PARCEL), :]
    turned = jnp.transpose(named)
    spot = jnp.full((1, LANES), NOWHERE, F32)
    line = lanes(1)
    for i, k in enumerate((2, 3, 0, 1, 4, 5)):
        line_k = jnp.concatenate([turned[k : k + 1, :], jnp.zeros((1, LANES - LON), F32)], axis=1)
        spot = jnp.where((line >= 8 * i) & (line < 8 * i + 8), roll(line_k, 8 * i), spot)
    for o in range(SLOT):
        own = parcels[pl.ds(BULK + o, LON, stride=PARCEL), :]
        left = jnp.where(ln < 8, roll(edge, -8 * o), 0.0)
        right = jnp.where((ln >= 56) & (ln < 64), roll(edge, 40 - 8 * o), 0.0)
        for out in (to_core, to_inter):
            out[STRIP + o * LON : STRIP + (o + 1) * LON, :] = own
            out[LEFTS + o * LON : LEFTS + (o + 1) * LON, :] = left
            out[RIGHTS + o * LON : RIGHTS + (o + 1) * LON, :] = right
    for out in (to_core, to_inter):
        out[SPOTS:, :] = jnp.broadcast_to(spot, (8, LANES))


def unpack(parcels, grams):
    ln, rw = lanes(HALF), places(HALF)
    upper, diagonal, first = ln - HALF > rw, ln - HALF == rw, ln < HALF
    for s in range(LON):
        both = parcels[s * PARCEL : s * PARCEL + 2 * HALF, :]
        turned = jnp.transpose(both)
        ct, et = turned[:HALF], turned[HALF:]
        ct_rolled, et_rolled = roll(ct, HALF), roll(et, HALF)
        for o in range(SLOT):
            q = both[o * HALF : (o + 1) * HALF]
            d = parcels[s * PARCEL + 2 * HALF + o : s * PARCEL + 2 * HALF + o + 1, :]
            e_first, e_last = (et, et_rolled) if o == 0 else (et_rolled, et)
            c_last = ct_rolled if o == 0 else ct
            top = jnp.where(first, jnp.where(ln <= rw, roll(q, HALF), e_first), c_last)
            low = jnp.where(first | upper, q, jnp.where(diagonal, d, e_last))
            at = (o * LON + s) * LANES
            grams[at : at + HALF, :] = top
            grams[at + HALF : at + LANES, :] = low


def split(x):
    high = x.astype(jnp.bfloat16)
    rest = x - high.astype(F32)
    middle = rest.astype(jnp.bfloat16)
    low = (rest - middle.astype(F32)).astype(jnp.bfloat16)
    return jnp.concatenate([high, middle, low], axis=1)


def chosen(one_hot, parts):
    out = jnp.dot(one_hot, parts, preferred_element_type=F32)
    return out[:, :LANES] + out[:, LANES : 2 * LANES] + out[:, 2 * LANES :]


def one_hot(index, at):
    return jnp.where(index == at, 1.0, 0.0).astype(jnp.bfloat16)


def padded(x, rows):
    return jnp.concatenate([x, jnp.zeros((rows - x.shape[0], LANES), F32)], axis=0)


def right_strips(x):
    ln = lanes(x.shape[0])
    return jnp.where((ln >= 56) & (ln < 64), roll(x, 56), 0.0)


def lay_out(spots, by_lane, own, sides, field, strips, low, high):
    ln = lanes(LANES)
    own_strip = jnp.where(ln < 32, jnp.where(ln >= 8, roll(own, 8), 0.0), jnp.where(ln < 56, roll(own, 56), 0.0))
    pieces = []
    for i, strip in enumerate((own_strip, sides)):
        upper = (spots[i * LANES : (i + 1) * LANES, :].astype(jnp.int32) & 8) != 0
        pieces.append(split(jnp.where(upper, roll(strip, HALF), strip)))
    own_parts = split(own)
    lane_spots = [by_lane[i * 8 : i * 8 + 1, :].astype(jnp.int32) for i in range(2)]
    p = jnp.broadcast_to(lane_spots[0], (LANES, LANES))
    for start in range(low * LEVELS, high * LEVELS, LANES):
        field[start : start + LANES, :] = chosen(one_hot(places(LANES) + start, p), own_parts)
    folded = [jnp.broadcast_to(((b >> 4) << 3) + (b & 7), (64, LANES)) for b in lane_spots]
    for start in range(low * 8, high * 8, 64):
        at = places(64) + start
        strips[start : start + 64, :] = chosen(one_hot(at, folded[0]), pieces[0]) + chosen(one_hot(at, folded[1]), pieces[1])


def adjoint(rates, source, target, first, last, height):
    before = kept = None
    for r in range(first, last + 1):
        y = source[r * height : (r + 1) * height, :]
        lat, lon = rates(r)
        t = lat * y
        a = jnp.where(lat > 0.0, t, 0.0)
        b = a - t
        s = lon * y
        e = jnp.where(lon > 0.0, s, 0.0)
        f = e - s
        if r > first + 1:
            target[(r - 1) * height : r * height, :] = kept + a
        if r > first:
            kept = y - (a + b) - (e + f) + roll(e, -1) + roll(f, 1) + before
        before = b


def tangent(rates, source, target, first, last, height):
    for r in range(first + 1, last):
        x = source[r * height : (r + 1) * height, :]
        south = source[(r - 1) * height : r * height, :]
        north = source[(r + 1) * height : (r + 2) * height, :]
        lat, lon = rates(r)
        out = x + jnp.abs(lat) * (jnp.where(lat > 0.0, south, north) - x)
        target[r * height : (r + 1) * height, :] = out + jnp.abs(lon) * (jnp.where(lon > 0.0, roll(x, 1), roll(x, -1)) - x)


def merged(field, strips, r):
    ln = lanes(8)
    t = strips[r * 8 : (r + 1) * 8, :]
    low, high = field[r * LEVELS : r * LEVELS + 8, :], field[r * LEVELS + 8 : (r + 1) * LEVELS, :]
    low = jnp.where(ln < 8, roll(t, -8), jnp.where(ln >= 120, roll(t, 72), low))
    high = jnp.where(ln < 8, roll(t, -72), jnp.where(ln >= 120, roll(t, 8), high))
    return low, high


def steps_back(rates, fields, strips, first):
    full, narrow = rates
    for k in range(first, first + STEPS):
        adjoint(full, *fields, k, WIDE - 1 - k, LEVELS)
        adjoint(narrow, *strips, k, WIDE - 1 - k, 8)
        fields, strips = fields[::-1], strips[::-1]
    return fields, strips


def steps_on(rates, fields, strips, first):
    full, narrow = rates
    for k in range(first, first + STEPS):
        tangent(full, *fields, k, WIDE - 1 - k, LEVELS)
        tangent(narrow, *strips, k, WIDE - 1 - k, 8)
        fields, strips = fields[::-1], strips[::-1]
    return fields, strips


def rates_of(wide, mine, beside):
    def full(r):
        at = r * 2 * LEVELS
        return wide[at : at + LEVELS, :], wide[at + LEVELS : at + 2 * LEVELS, :]

    def narrow(r):
        ref, r = (mine, r - HALO) if HALO <= r < HALO + ROWS else (beside, r if r < HALO else r - ROWS)
        return ref[r * 16 : r * 16 + 8, :], ref[r * 16 + 8 : r * 16 + 16, :]

    return full, narrow


def back_and_on(spots, by_lane, own, sides, rates, kept, fields, strips, image):
    lay_out(spots, by_lane, own, sides, fields[0], strips[0], 0, WIDE)
    fields, strips = steps_back(rates, fields, strips, 0)
    lat, last = lax.axis_index(LAT), lax.axis_size(LAT) - 1
    for outside, start in ((lat == 0, STEPS), (lat == last, HALO + ROWS)):
        for ref, height in ((fields[0], LEVELS), (strips[0], 8)):
            block = ref[start * height : (start + STEPS) * height, :]
            ref[start * height : (start + STEPS) * height, :] = jnp.where(outside, 0.0, block)
    square = jnp.zeros((8, LANES), F32)
    for r in range(ROWS):
        low, high = merged(fields[0], strips[0], r + HALO)
        kept[r * LEVELS : r * LEVELS + 8, :] = low
        kept[r * LEVELS + 8 : (r + 1) * LEVELS, :] = high
        square += low * low + high * high
    fields, strips = steps_on(rates, fields, strips, STEPS)
    for r in range(ROWS):
        low, high = merged(fields[0], strips[0], r + HALO)
        image[r * LEVELS : r * LEVELS + 8, :] = low
        image[r * LEVELS + 8 : (r + 1) * LEVELS, :] = high
    mine = spots[OWN : 2 * OWN, :].astype(jnp.int32) - HALO * LEVELS
    hit = jnp.concatenate([one_hot(lanes(OWN), mine), one_hot(lanes(OWN) + LANES, mine)], axis=1)
    return jnp.sum(square, keepdims=True), chosen(hit, split(image[...]))


def weigh(seen, grams):
    column = jnp.transpose(seen)
    out = []
    for t in range(OWN):
        total = jnp.zeros((8, LANES), F32)
        for k in range(LANES // 8):
            at = t * LANES + k * 8
            total += grams[at : at + 8, :] * column[k * 8 : k * 8 + 8, t : t + 1]
        out.append(jnp.sum(total, axis=0, keepdims=True))
    return jnp.concatenate(out, axis=0)


def in_lanes(first, values):
    ln = lanes(8)
    out = jnp.zeros((8, LANES), F32)
    for i, v in enumerate(values):
        out = jnp.where(ln == first + i, v, out)
    return out


def first_half(wide, mine, core, own_message, inter, beside, spots, by_lane, kept, seen, sums, field, other, strip, other_strip, image):
    ln = lanes(8)
    even = lax.axis_index("lat_2") == 0
    beside[:STRIP, :] = jnp.where(even, inter[:STRIP, :], core[:STRIP, :])
    beside[STRIP:, :] = jnp.where(even, core[:STRIP, :], inter[:STRIP, :])
    step = jnp.where(even, float(ROWS * LEVELS), -float(ROWS * LEVELS))
    c, o, i = core[SPOTS:, :] + step, own_message[SPOTS:, :], inter[SPOTS:, :] - step
    tables = (((c, 0), (o, 0), (i, 0)), ((c, 16), (o, 16), (i, 16), (c, 32), (o, 32), (i, 32)))
    for t, table in enumerate(tables):
        spot = jnp.full((8, LANES), NOWHERE, F32)
        for n, (x, at) in enumerate(table):
            spot = jnp.where((ln >= OWN * n) & (ln < OWN * (n + 1)), roll(x, OWN * n - at), spot)
        by_lane[t * 8 : t * 8 + 8, :] = spot
        spots[t * LANES : (t + 1) * LANES, :] = jnp.transpose(jnp.broadcast_to(spot[:1], (LANES, LANES)))
    parts = (core, own_message, inter)
    own = padded(jnp.concatenate([x[STRIP:LEFTS, :] for x in parts], axis=0), LANES)
    sides = padded(jnp.concatenate([x[LEFTS:RIGHTS, :] for x in parts] + [x[RIGHTS:SPOTS, :] for x in parts], axis=0), LANES)
    square, rows = back_and_on(spots, by_lane, own, sides, rates_of(wide, mine, beside), kept, (field, other), (strip, other_strip), image)
    seen[...] = rows
    sums[...] = in_lanes(0, [square])


def stepped(x, unit):
    row = places(OWN)
    for bit in range(4):
        x = jnp.where((row & (1 << bit)) != 0, roll(x, unit << bit), x)
    return x


def herald(rows, message):
    mine = (lanes(OWN) >> 3) == places(OWN)
    message[:OWN, :] = rows
    message[OWN : OWN + 1, :] = jnp.sum(jnp.where(mine, stepped(rows, 8), 0.0), axis=0, keepdims=True)
    message[OWN + 1 : OWN + 2, :] = jnp.sum(jnp.where(mine, stepped(roll(rows, 8), 8), 0.0), axis=0, keepdims=True)
    message[OWN + 2 :, :] = jnp.zeros((HERALD - OWN - 2, LANES), F32)


def first_terms(grams, seen, before, message, sums):
    rows = weigh(seen[...], grams)
    herald(rows, message)
    sums[...] = before[...] + in_lanes(1, [jnp.sum(seen[...] * rows, keepdims=True)])


def edges_of(core, mine, inter, out):
    for i, x in enumerate((core, mine, inter)):
        out[i : i + 1, :] = x[OWN : OWN + 1, :]
        out[i + 3 : i + 4, :] = x[OWN + 1 : OWN + 2, :]
    out[6:, :] = jnp.zeros((2, LANES), F32)


def side_strips(lefts, rights):
    ln = lanes(OWN)
    rows = [stepped(jnp.broadcast_to(x, (OWN, LANES)), -8) for x in lefts]
    out = [jnp.where(ln < 8, x, 0.0) for x in rows]
    rows = [stepped(jnp.broadcast_to(x, (OWN, LANES)), -8) for x in rights]
    return padded(jnp.concatenate(out + [right_strips(x) for x in rows], axis=0), LANES)


def second_half(spots, by_lane, core, mine, inter, even, odd, wide, strips, beside, grams, before, kept, message, out, field, other, strip, other_strip, image):
    own = padded(jnp.concatenate([x[:OWN, :] for x in (core, mine, inter)], axis=0), LANES)
    here = lax.rem(lax.axis_index("lon"), 2) == 0
    left, right = jnp.where(here, odd[...], even[...]), jnp.where(here, even[...], odd[...])
    sides = side_strips([left[i : i + 1] for i in (3, 4, 5)], [right[i : i + 1] for i in (0, 1, 2)])
    square, seen = back_and_on(
        spots, by_lane, own, sides, rates_of(wide, strips, beside), kept, (field, other), (strip, other_strip), image
    )
    rows = weigh(seen, grams)
    herald(rows, message)
    sums = before[...] + in_lanes(2, [square, jnp.sum(seen * rows, keepdims=True)])
    out[...] = jnp.concatenate([sums] * (out.shape[0] // 8), axis=0)
    for step, row in ((1, OWN + 1), (-1, OWN)):
        out[pl.ds(in_plane(step) * 2 + 1, 1), :] = message[row : row + 1, :]


def in_plane(step):
    size = lax.axis_size(("lat_1", "lon"))
    at = lax.axis_index("lat_1") * LON + lax.rem(lax.axis_index("lon") + LON + step, LON)
    return lax.rem(at + size - middle_of_plane(), size)


def middle_of_plane():
    return lax.axis_size("lat_1") // 2 * LON + LON // 2


def gathered(parts, mine, sums, message):
    count = parts.shape[0] // 2
    sums[...] = jnp.broadcast_to(jnp.sum(parts[pl.ds(0, count, stride=2), :], axis=0, keepdims=True), sums.shape)
    message[...] = mine[...]
    for i, step in enumerate((-1, 1)):
        message[OWN + i : OWN + i + 1, :] = parts[pl.ds(in_plane(step) * 2 + 1, 1), :]


def finish(spots, by_lane, core, mine, inter, wide, strips, beside, parts, right_side, image, increment, residual, field, other, strip, other_strip):
    lists = (core, mine, inter)
    own = padded(jnp.concatenate([x[:OWN, :] for x in lists], axis=0), LANES)
    sides = side_strips(*([x[OWN + i : OWN + i + 1, :] for x in lists] for i in range(2)))
    lay_out(spots, by_lane, own, sides, field, strip, HALO - STEPS, HALO + ROWS + STEPS)
    fields, narrow = steps_back(rates_of(wide, strips, beside), (field, other), (strip, other_strip), STEPS)
    total = jnp.sum(parts[...], axis=0, keepdims=True)
    m0, m1, m2, m3 = (jnp.sum(jnp.where(lanes(1) == i, total, 0.0), keepdims=True) for i in range(4))
    step_0 = m0 / (m0 + m1)
    rho = m1 / m0
    spread = m2 - rho * m1
    curve = (m3 - rho * m2) - rho * (m2 - rho * m1)
    gamma = step_0 * spread / m0
    step_1 = spread / (spread + curve - gamma * spread)
    on_b = step_0 * (1.0 + step_1 * (gamma + rho))
    on_k = -step_0 * step_1
    rest_b = step_0 * ((1.0 - step_1) * rho - step_1 * gamma)
    rest_k = -step_0 * ((1.0 - step_1) + step_1 * (rho + gamma))
    rest_kk = step_0 * step_1
    on_b, on_k, rest_b, rest_k, rest_kk = (jnp.broadcast_to(v, (8, LANES)) for v in (on_b, on_k, rest_b, rest_k, rest_kk))
    for r in range(ROWS):
        for h, second in enumerate(merged(fields[0], narrow[0], r + HALO)):
            at = r * LEVELS + h * 8
            b, first = right_side[at : at + 8, :], image[at : at + 8, :]
            to = pl.ds(h * 8 * ROWS + r, 8, stride=ROWS)
            increment[to, :] = on_b * b + on_k * first
            residual[to, :] = rest_b * b + rest_k * first + rest_kk * second


def to_core(x):
    return lax.ppermute(x, LAT, [(i, i ^ 1) for i in range(lax.axis_size(LAT))])


def to_inter(x):
    return lax.ppermute(x, LAT, [(i, ((i + 1) ^ 1) - 1) for i in range(1, lax.axis_size(LAT) - 1)])


def to_even(x):
    return lax.ppermute(x, "lon", [(i, i ^ 1) for i in range(LON)])


def to_odd(x):
    return lax.ppermute(x, "lon", [(i, (((i + 1) % LON ^ 1) - 1) % LON) for i in range(LON)])


def spread_out(x, axes, first):
    count = lax.axis_size(axes)
    group = [(i + first) % count for i in range(count)]
    return lax.all_to_all(x, axes, split_axis=0, concat_axis=0, tiled=True, axis_index_groups=[group])


def shards(courant, obs_matrix, obs_weight, innovation, block_owner, block_row, block_count):
    flow = courant.reshape(-1, LANES)
    owner, row, count = block_owner.reshape(-1), block_row.reshape(-1), block_count
    wholes = (obs_matrix[0], obs_weight[0], innovation[0])
    (parcels,) = call(
        prepare,
        [(LON * PARCEL, LANES)],
        (owner, row, count, *wholes),
        4_000_000,
        [pltpu.SMEM((CAP,), jnp.int32), pltpu.SMEM((CAP,), jnp.int32), pltpu.SMEM((1, 1), jnp.int32)]
        + [pltpu.VMEM(x.shape, F32) for x in wholes]
        + [pltpu.VMEM((OWN, LANES), F32), pltpu.SemaphoreType.DMA((6,))],
        [pl.BlockSpec(memory_space=pltpu.HBM)] * 6,
        62,
    )
    parcels = spread_out(parcels.reshape(LON, PARCEL, LANES), "lon", FIRST).reshape(LON * PARCEL, LANES)
    edge = (EDGE, LANES), (2 * OWN, LANES)
    for_core, for_inter, for_even, for_odd = call(halo, [edge[0], edge[0], edge[1], edge[1]], (flow,), 1_000_000)
    odd = to_odd(for_odd)
    even = to_even(for_even)
    inter = to_inter(for_inter)
    core = to_core(for_core)
    wide, strips, for_core, for_inter = call(
        arrange,
        [(WIDE * 2 * LEVELS, LANES), (2 * STRIP, LANES), (MESSAGE, LANES), (MESSAGE, LANES)],
        (flow, parcels, core, inter, even, odd),
        2_000_000,
    )
    core, inter = to_core(for_core), to_inter(for_inter)
    (grams,) = call(unpack, [(OWN * LANES, LANES)], (parcels,), 4_000_000)
    cells, listed = (ROWS * LEVELS, LANES), (OWN, LANES)
    work = [pltpu.VMEM((WIDE * LEVELS, LANES), F32)] * 2 + [pltpu.VMEM((WIDE * 8, LANES), F32)] * 2
    work_too = work + [pltpu.VMEM(cells, F32)]
    beside, spots, by_lane, right_side, seen, sums = call(
        first_half,
        [(2 * STRIP, LANES), (2 * LANES, LANES), (16, LANES), cells, listed, (8, LANES)],
        (wide, strips, core, for_core, inter),
        4_000_000,
        work_too,
    )
    rates = (wide, strips, beside)
    short = (HERALD, LANES)
    mine, sums = call(first_terms, [short, (8, LANES)], (grams, seen, sums), 2_000_000)
    core, inter = to_core(mine), to_inter(mine)
    (edges,) = call(edges_of, [(8, LANES)], (core, mine, inter), 10_000)
    lists = (core, mine, inter, to_even(edges), to_odd(edges))
    plane, towers = lax.axis_size(("lat_1", "lon")), lax.axis_size(("lat_0", "lat_2"))
    image, mine, parcels = call(
        second_half, [cells, short, (plane * 2, LANES)], (spots, by_lane, *lists, *rates, grams, sums), 4_000_000, work_too
    )
    parcels = spread_out(parcels.reshape(plane, 2, LANES), ("lat_1", "lon"), middle_of_plane()).reshape(plane * 2, LANES)
    sums, mine = call(gathered, [(towers, LANES), short], (parcels, mine), 10_000)
    core, inter = to_core(mine), to_inter(mine)
    parts = spread_out(sums.reshape(towers, 1, LANES), ("lat_0", "lat_2"), towers * 12 // 16 + 1).reshape(towers, LANES)
    increment, residual = call(
        finish, [cells, cells], (spots, by_lane, core, mine, inter, *rates, parts, right_side, image), 2_000_000, work
    )
    shape = courant.shape[1:]
    return increment.reshape(shape), residual.reshape(shape)


def solution(mesh):
    torus = Mesh(
        mesh.devices.reshape(-1, 4, 2, mesh.shape["lon"]), ("lat_0", "lat_1", "lat_2", "lon")
    )
    placed = (
        P(None, None, LAT, "lon"),
        P(LAT, "lon", None, None),
        P(LAT, "lon", None),
        P(LAT, "lon", None),
        P(LAT, "lon", None),
        P(LAT, "lon"),
        P(LAT, "lon"),
    )
    return jax.shard_map(
        shards,
        mesh=torus,
        in_specs=placed,
        out_specs=(P(None, LAT, "lon"), P(None, LAT, "lon")),
        check_vma=False,
    )
```

```python
import jax
import jax.numpy as jnp
from jax import lax
from jax.experimental import pallas as pl
from jax.experimental.pallas import tpu as pltpu
from jax.sharding import Mesh
from jax.sharding import PartitionSpec as P


LAT = ("lat_0", "lat_1", "lat_2")
LEVELS = 16
ROWS = 16
LANES = 128
CAP = 8
SLOT = 2
STEPS = 4
HALO = 2 * STEPS
WIDE = ROWS + 2 * HALO
LON = 8
HALF = LANES // 2
OWN = LON * SLOT
BULK = 2 * HALF + 2
LIST = BULK + 6
PARCEL = LIST
EDGE = HALO * 2 * LEVELS
STRIP = HALO * 2 * 8
LEFTS = STRIP + OWN
RIGHTS = LEFTS + OWN
SPOTS = RIGHTS + OWN
MESSAGE = SPOTS + 8
HERALD = OWN + 8
NOWHERE = -4096.0
FIRST = 6
HIGHEST = lax.Precision.HIGHEST
F32 = jnp.float32
VMEM = pl.BlockSpec(memory_space=pltpu.VMEM)
SMEM = pl.BlockSpec(memory_space=pltpu.SMEM)


def lanes(rows):
    return lax.broadcasted_iota(jnp.int32, (rows, LANES), 1)


def places(rows):
    return lax.broadcasted_iota(jnp.int32, (rows, LANES), 0)


def roll(x, shift):
    shift %= LANES
    return pltpu.roll(x, shift, axis=1) if shift else x


def call(body, outs, args, flops, scratch=(), specs=None, room=24):
    return pl.pallas_call(
        body,
        out_shape=[jax.ShapeDtypeStruct(s, F32) for s in outs],
        in_specs=specs or [SMEM if a.dtype == jnp.int32 else VMEM for a in args],
        out_specs=[VMEM] * len(outs),
        scratch_shapes=list(scratch),
        compiler_params=pltpu.CompilerParams(vmem_limit_bytes=room << 20),
        cost_estimate=pl.CostEstimate(flops=flops, bytes_accessed=0, transcendentals=0),
    )(*args)


def turns_of(owners):
    return [sum([(o == owners[j]).astype(jnp.int32) for o in owners[:j]], jnp.int32(0)) for j in range(CAP)]


def chunk(owner):
    return (owner + LON - FIRST) % LON if isinstance(owner, int) else lax.rem(owner + LON - FIRST, LON)


def packed_edges(pick, shift):
    ln = lanes(8)
    out = jnp.zeros((8, LANES), F32)
    for k in range(8):
        low, high = pick(k)
        out = jnp.where((ln >= 16 * k) & (ln < 16 * k + 8), roll(low, 16 * k + shift), out)
        out = jnp.where((ln >= 16 * k + 8) & (ln < 16 * k + 16), roll(high, 16 * k + 8 + shift), out)
    return out


def weigh_blocks(owners, turns, count, matrix, weight, parcels):
    ln, rw = lanes(HALF), places(HALF)
    for j in range(CAP):
        block = matrix[j]
        scaled = jnp.transpose(block) * jnp.where(j < count[0, 0], weight[j : j + 1, :], 0.0)
        gram = jnp.dot(scaled, block, precision=HIGHEST, preferred_element_type=F32)
        top, low = gram[:HALF], gram[HALF:]
        packed = jnp.where((ln >= HALF) & (ln - HALF <= rw), roll(top, HALF), low)
        diagonal = jnp.sum(jnp.where(ln - HALF == rw, low, 0.0), axis=0, keepdims=True)
        at = chunk(owners[j]) * PARCEL + turns[j] * HALF
        parcels[pl.ds(pl.multiple_of(at, 8), HALF), :] = packed
        parcels[pl.ds(chunk(owners[j]) * PARCEL + 2 * HALF + turns[j], 1), :] = diagonal


def prepare(owner_at, row_at, count_at, matrix_at, weight_at, innovation_at, parcels, owner, row, count, matrix, weight, innovation, lists, sems):
    pairs = ((matrix_at, matrix), (owner_at, owner), (row_at, row), (count_at, count), (weight_at, weight), (innovation_at, innovation))
    copies = [pltpu.make_async_copy(a, b, sems.at[i]) for i, (a, b) in enumerate(pairs)]
    for copy in copies:
        copy.start()
    for d in range(LON):
        parcels[d * PARCEL : d * PARCEL + LIST, :] = jnp.zeros((LIST, LANES), F32)
    lists[...] = jnp.zeros(lists.shape, F32)
    for copy in copies:
        copy.wait()
    owners = [owner[j] for j in range(CAP)]
    turns = turns_of(owners)
    column = jnp.transpose(weight[...] * innovation[...])
    ln = lanes(8)
    named = jnp.full((8, LANES), NOWHERE, F32)
    for j in range(CAP):
        live = j < count[0, 0]
        total = jnp.zeros((8, LANES), F32)
        for k in range(LANES // 8):
            total += matrix[j, k * 8 : k * 8 + 8, :] * column[k * 8 : k * 8 + 8, j : j + 1]
        slot = owners[j] * SLOT + turns[j]
        lists[pl.ds(slot, 1), :] = jnp.where(live, jnp.sum(total, axis=0, keepdims=True), 0.0)
        place = jnp.where(live, (lax.rem(row[j], ROWS) + HALO) * LEVELS + lax.div(row[j], ROWS), int(NOWHERE)).astype(F32)
        named = jnp.where(ln == slot, place, named)
    weigh_blocks(owners, turns, count, matrix, weight, parcels)
    named = jnp.where(ln < OWN, named, roll(named, OWN))
    line = lanes(1)
    for d in range(LON):
        left, right = 2 * (d - 1) % OWN, 2 * (d + 1) % OWN
        at = chunk(d) * PARCEL + BULK
        parcels[at : at + 2, :] = lists[2 * d : 2 * d + 2, :]
        edge = jnp.where(line < 8, roll(lists[left : left + 1, :], 8), roll(lists[left + 1 : left + 2, :], 16))
        edge = jnp.where(line < 16, edge, jnp.where(line < 24, roll(lists[right : right + 1, :], 16), roll(lists[right + 1 : right + 2, :], 24)))
        parcels[at + 2 : at + 3, :] = edge
        parcels[at + 3 : at + 4, :] = roll(named, -left)[:1]


def halo(flow, to_core, to_inter, to_even, to_odd):
    even = lax.axis_index("lat_2") == 0
    here = lax.rem(lax.axis_index("lon"), 2) == 0
    for f in range(2):
        for g in range(2):

            def pick(k, f=f, g=g):
                at = f * LEVELS * ROWS + g * 8 + k
                return flow[pl.ds(at, 8, stride=ROWS), :], flow[pl.ds(at + 8 * ROWS, 8, stride=ROWS), :]

            at = (f * 2 + g) * 8
            to_right, to_left = packed_edges(pick, 8), packed_edges(pick, 0)
            to_even[at : at + 8, :] = jnp.where(here, to_right, to_left)
            to_odd[at : at + 8, :] = jnp.where(here, to_left, to_right)
        for i in range(HALO):
            for h in range(2):
                at = f * LEVELS * ROWS + h * 8 * ROWS + i
                up, down = flow[pl.ds(at + ROWS - HALO, 8, stride=ROWS), :], flow[pl.ds(at, 8, stride=ROWS), :]
                at = (i * 2 + f) * LEVELS + h * 8
                to_core[at : at + 8, :] = jnp.where(even, up, down)
                to_inter[at : at + 8, :] = jnp.where(even, down, up)


def backwards(x):
    return jnp.concatenate([x[i : i + 1] for i in reversed(range(x.shape[0]))], axis=0)


def arrange(flow, parcels, core, inter, even_edges, odd_edges, wide, strips, to_core, to_inter):
    ln = lanes(8)
    here = lax.rem(lax.axis_index("lon"), 2) == 0
    even = lax.axis_index("lat_2") == 0
    wide[:EDGE, :] = jnp.where(even, inter[...], core[...])
    wide[EDGE + ROWS * 2 * LEVELS :, :] = jnp.where(even, core[...], inter[...])
    for f in range(2):
        for g in range(2):
            at = (f * 2 + g) * 8
            first, second = even_edges[at : at + 8, :], odd_edges[at : at + 8, :]
            left, right = jnp.where(here, second, first), jnp.where(here, first, second)
            for k in range(8):
                at = f * LEVELS * ROWS + g * 8 + k
                low, high = flow[pl.ds(at, 8, stride=ROWS), :], flow[pl.ds(at + 8 * ROWS, 8, stride=ROWS), :]
                at = EDGE + ((g * 8 + k) * 2 + f) * LEVELS
                wide[at : at + 8, :] = low
                wide[at + 8 : at + 16, :] = high
                a = jnp.where(ln < 8, roll(left, -16 * k), jnp.where(ln < 32, roll(low, 8), jnp.where(ln < 56, roll(low, 56), roll(right, 56 - 16 * k))))
                b = jnp.where(ln < 72, roll(left, 56 - 16 * k), jnp.where(ln < 96, roll(high, 72), jnp.where(ln < 120, roll(high, 120), roll(right, 112 - 16 * k))))
                strip = jnp.where(ln < HALF, a, b)
                at = ((g * 8 + k) * 2 + f) * 8
                strips[at : at + 8, :] = strip
    lower, upper = strips[:STRIP, :], strips[STRIP:, :]
    to_core[:STRIP, :] = jnp.where(even, upper, lower)
    to_inter[:STRIP, :] = jnp.where(even, lower, upper)
    edge = backwards(parcels[pl.ds(BULK + 2, LON, stride=PARCEL), :])
    named = parcels[pl.ds(BULK + 3, LON, stride=PARCEL), :]
    turned, turned_back = jnp.transpose(named), jnp.transpose(backwards(named))
    spot = jnp.full((1, LANES), NOWHERE, F32)
    line = lanes(1)
    for i, k in enumerate((2, 3, 0, 1, 4, 5)):
        rows = turned if k in (2, 3) else turned_back
        line_k = jnp.concatenate([rows[k : k + 1, :], jnp.zeros((1, LANES - LON), F32)], axis=1)
        spot = jnp.where((line >= 8 * i) & (line < 8 * i + 8), roll(line_k, 8 * i), spot)
    for o in range(SLOT):
        own = parcels[pl.ds(BULK + o, LON, stride=PARCEL), :]
        left = jnp.where(ln < 8, roll(edge, -8 * o), 0.0)
        right = jnp.where((ln >= 56) & (ln < 64), roll(edge, 40 - 8 * o), 0.0)
        for out in (to_core, to_inter):
            out[STRIP + o * LON : STRIP + (o + 1) * LON, :] = own
            out[LEFTS + o * LON : LEFTS + (o + 1) * LON, :] = left
            out[RIGHTS + o * LON : RIGHTS + (o + 1) * LON, :] = right
    for out in (to_core, to_inter):
        out[SPOTS:, :] = jnp.broadcast_to(spot, (8, LANES))


def unpack(parcels, grams):
    ln, rw = lanes(HALF), places(HALF)
    upper, diagonal, first = ln - HALF > rw, ln - HALF == rw, ln < HALF
    for s in range(LON):
        both = parcels[s * PARCEL : s * PARCEL + 2 * HALF, :]
        turned = jnp.transpose(both)
        ct, et = turned[:HALF], turned[HALF:]
        ct_rolled, et_rolled = roll(ct, HALF), roll(et, HALF)
        for o in range(SLOT):
            q = both[o * HALF : (o + 1) * HALF]
            d = parcels[s * PARCEL + 2 * HALF + o : s * PARCEL + 2 * HALF + o + 1, :]
            e_first, e_last = (et, et_rolled) if o == 0 else (et_rolled, et)
            c_last = ct_rolled if o == 0 else ct
            top = jnp.where(first, jnp.where(ln <= rw, roll(q, HALF), e_first), c_last)
            low = jnp.where(first | upper, q, jnp.where(diagonal, d, e_last))
            at = (o * LON + s) * LANES
            grams[at : at + HALF, :] = top
            grams[at + HALF : at + LANES, :] = low


def split(x):
    high = x.astype(jnp.bfloat16)
    rest = x - high.astype(F32)
    middle = rest.astype(jnp.bfloat16)
    low = (rest - middle.astype(F32)).astype(jnp.bfloat16)
    return jnp.concatenate([high, middle, low], axis=1)


def chosen(one_hot, parts):
    out = jnp.dot(one_hot, parts, preferred_element_type=F32)
    return out[:, :LANES] + out[:, LANES : 2 * LANES] + out[:, 2 * LANES :]


def one_hot(index, at):
    return jnp.where(index == at, 1.0, 0.0).astype(jnp.bfloat16)


def padded(x, rows):
    return jnp.concatenate([x, jnp.zeros((rows - x.shape[0], LANES), F32)], axis=0)


def lay_out(spots, by_lane, own, sides, field, strips, low, high):
    ln = lanes(LANES)
    own_strip = jnp.where(ln < 32, jnp.where(ln >= 8, roll(own, 8), 0.0), jnp.where(ln < 56, roll(own, 56), 0.0))
    pieces = []
    for i, strip in enumerate((own_strip, sides)):
        upper = (spots[i * LANES : (i + 1) * LANES, :].astype(jnp.int32) & 8) != 0
        pieces.append(split(jnp.where(upper, roll(strip, HALF), strip)))
    own_parts = split(own)
    lane_spots = [by_lane[i * 8 : i * 8 + 1, :].astype(jnp.int32) for i in range(2)]
    p = jnp.broadcast_to(lane_spots[0], (LANES, LANES))
    for start in range(low * LEVELS, high * LEVELS, LANES):
        field[start : start + LANES, :] = chosen(one_hot(places(LANES) + start, p), own_parts)
    folded = [jnp.broadcast_to(((b >> 4) << 3) + (b & 7), (64, LANES)) for b in lane_spots]
    for start in range(low * 8, high * 8, 64):
        at = places(64) + start
        strips[start : start + 64, :] = chosen(one_hot(at, folded[0]), pieces[0]) + chosen(one_hot(at, folded[1]), pieces[1])


def adjoint(rates, source, target, first, last, height):
    before = kept = None
    for r in range(first, last + 1):
        y = source[r * height : (r + 1) * height, :]
        lat, lon = rates(r)
        t = lat * y
        a = jnp.where(lat > 0.0, t, 0.0)
        b = a - t
        s = lon * y
        e = jnp.where(lon > 0.0, s, 0.0)
        f = e - s
        if r > first + 1:
            target[(r - 1) * height : r * height, :] = kept + a
        if r > first:
            kept = y - (a + b) - (e + f) + roll(e, -1) + roll(f, 1) + before
        before = b


def tangent(rates, source, target, first, last, height):
    for r in range(first + 1, last):
        x = source[r * height : (r + 1) * height, :]
        south = source[(r - 1) * height : r * height, :]
        north = source[(r + 1) * height : (r + 2) * height, :]
        lat, lon = rates(r)
        out = x + jnp.abs(lat) * (jnp.where(lat > 0.0, south, north) - x)
        target[r * height : (r + 1) * height, :] = out + jnp.abs(lon) * (jnp.where(lon > 0.0, roll(x, 1), roll(x, -1)) - x)


def merged(field, strips, r):
    ln = lanes(8)
    t = strips[r * 8 : (r + 1) * 8, :]
    low, high = field[r * LEVELS : r * LEVELS + 8, :], field[r * LEVELS + 8 : (r + 1) * LEVELS, :]
    low = jnp.where(ln < 8, roll(t, -8), jnp.where(ln >= 120, roll(t, 72), low))
    high = jnp.where(ln < 8, roll(t, -72), jnp.where(ln >= 120, roll(t, 8), high))
    return low, high


def steps_back(rates, fields, strips, first):
    full, narrow = rates
    for k in range(first, first + STEPS):
        adjoint(full, *fields, k, WIDE - 1 - k, LEVELS)
        adjoint(narrow, *strips, k, WIDE - 1 - k, 8)
        fields, strips = fields[::-1], strips[::-1]
    return fields, strips


def steps_on(rates, fields, strips, first):
    full, narrow = rates
    for k in range(first, first + STEPS):
        tangent(full, *fields, k, WIDE - 1 - k, LEVELS)
        tangent(narrow, *strips, k, WIDE - 1 - k, 8)
        fields, strips = fields[::-1], strips[::-1]
    return fields, strips


def rates_of(wide, mine, beside):
    def full(r):
        at = r * 2 * LEVELS
        return wide[at : at + LEVELS, :], wide[at + LEVELS : at + 2 * LEVELS, :]

    def narrow(r):
        ref, r = (mine, r - HALO) if HALO <= r < HALO + ROWS else (beside, r if r < HALO else r - ROWS)
        return ref[r * 16 : r * 16 + 8, :], ref[r * 16 + 8 : r * 16 + 16, :]

    return full, narrow


def back_and_on(spots, by_lane, own, sides, rates, kept, fields, strips, image):
    lay_out(spots, by_lane, own, sides, fields[0], strips[0], 0, WIDE)
    fields, strips = steps_back(rates, fields, strips, 0)
    lat, last = lax.axis_index(LAT), lax.axis_size(LAT) - 1
    for outside, start in ((lat == 0, STEPS), (lat == last, HALO + ROWS)):
        for ref, height in ((fields[0], LEVELS), (strips[0], 8)):
            block = ref[start * height : (start + STEPS) * height, :]
            ref[start * height : (start + STEPS) * height, :] = jnp.where(outside, 0.0, block)
    square = jnp.zeros((8, LANES), F32)
    for r in range(ROWS):
        low, high = merged(fields[0], strips[0], r + HALO)
        kept[r * LEVELS : r * LEVELS + 8, :] = low
        kept[r * LEVELS + 8 : (r + 1) * LEVELS, :] = high
        square += low * low + high * high
    fields, strips = steps_on(rates, fields, strips, STEPS)
    for r in range(ROWS):
        low, high = merged(fields[0], strips[0], r + HALO)
        image[r * LEVELS : r * LEVELS + 8, :] = low
        image[r * LEVELS + 8 : (r + 1) * LEVELS, :] = high
    mine = spots[OWN : 2 * OWN, :].astype(jnp.int32) - HALO * LEVELS
    hit = jnp.concatenate([one_hot(lanes(OWN), mine), one_hot(lanes(OWN) + LANES, mine)], axis=1)
    return jnp.sum(square, keepdims=True), chosen(hit, split(image[...]))


def weigh(seen, grams):
    column = jnp.transpose(seen)
    out = []
    for t in range(OWN):
        total = jnp.zeros((8, LANES), F32)
        for k in range(LANES // 8):
            at = t * LANES + k * 8
            total += grams[at : at + 8, :] * column[k * 8 : k * 8 + 8, t : t + 1]
        out.append(jnp.sum(total, axis=0, keepdims=True))
    return jnp.concatenate(out, axis=0)


def in_lanes(first, values):
    ln = lanes(8)
    out = jnp.zeros((8, LANES), F32)
    for i, v in enumerate(values):
        out = jnp.where(ln == first + i, v, out)
    return out


def first_half(wide, mine, core, own_message, inter, beside, spots, by_lane, kept, seen, sums, field, other, strip, other_strip, image):
    ln = lanes(8)
    even = lax.axis_index("lat_2") == 0
    beside[:STRIP, :] = jnp.where(even, inter[:STRIP, :], core[:STRIP, :])
    beside[STRIP:, :] = jnp.where(even, core[:STRIP, :], inter[:STRIP, :])
    step = jnp.where(even, float(ROWS * LEVELS), -float(ROWS * LEVELS))
    c, o, i = core[SPOTS:, :] + step, own_message[SPOTS:, :], inter[SPOTS:, :] - step
    tables = (((c, 0), (o, 0), (i, 0)), ((c, 16), (o, 16), (i, 16), (c, 32), (o, 32), (i, 32)))
    for t, table in enumerate(tables):
        spot = jnp.full((8, LANES), NOWHERE, F32)
        for n, (x, at) in enumerate(table):
            spot = jnp.where((ln >= OWN * n) & (ln < OWN * (n + 1)), roll(x, OWN * n - at), spot)
        by_lane[t * 8 : t * 8 + 8, :] = spot
        spots[t * LANES : (t + 1) * LANES, :] = jnp.transpose(jnp.broadcast_to(spot[:1], (LANES, LANES)))
    parts = (core, own_message, inter)
    own = padded(jnp.concatenate([x[STRIP:LEFTS, :] for x in parts], axis=0), LANES)
    sides = padded(jnp.concatenate([x[LEFTS:RIGHTS, :] for x in parts] + [x[RIGHTS:SPOTS, :] for x in parts], axis=0), LANES)
    square, rows = back_and_on(spots, by_lane, own, sides, rates_of(wide, mine, beside), kept, (field, other), (strip, other_strip), image)
    seen[...] = rows
    sums[...] = in_lanes(0, [square])


def fanned(x, shift):
    return pltpu.roll(x, shift % LANES, axis=1, stride=8, stride_axis=0)


def herald(rows, message):
    mine = (lanes(OWN) >> 3) == places(OWN)
    message[:OWN, :] = rows
    for at, shift in ((OWN, 0), (OWN + 1, 8)):
        spread = jnp.concatenate([fanned(rows[:8], shift), fanned(rows[8:], shift + HALF)], axis=0)
        message[at : at + 1, :] = jnp.sum(jnp.where(mine, spread, 0.0), axis=0, keepdims=True)
    message[OWN + 2 :, :] = jnp.zeros((HERALD - OWN - 2, LANES), F32)


def first_terms(grams, seen, before, message, sums):
    rows = weigh(seen[...], grams)
    herald(rows, message)
    sums[...] = before[...] + in_lanes(1, [jnp.sum(seen[...] * rows, keepdims=True)])


def edges_of(core, mine, inter, out):
    for i, x in enumerate((core, mine, inter)):
        out[i : i + 1, :] = x[OWN : OWN + 1, :]
        out[i + 3 : i + 4, :] = x[OWN + 1 : OWN + 2, :]
    out[6:, :] = jnp.zeros((2, LANES), F32)


def side_strips(lefts, rights):
    ln = lanes(OWN)

    def rows(x, shift):
        x = jnp.broadcast_to(x, (8, LANES))
        return jnp.concatenate([fanned(x, shift - 56), fanned(x, shift - 120)], axis=0)

    out = [jnp.where(ln < 8, rows(x, 0), 0.0) for x in lefts]
    out += [jnp.where((ln >= 56) & (ln < 64), rows(x, 56), 0.0) for x in rights]
    return padded(jnp.concatenate(out, axis=0), LANES)


def second_half(spots, by_lane, core, mine, inter, even, odd, wide, strips, beside, grams, before, kept, message, out, field, other, strip, other_strip, image):
    own = padded(jnp.concatenate([x[:OWN, :] for x in (core, mine, inter)], axis=0), LANES)
    here = lax.rem(lax.axis_index("lon"), 2) == 0
    left, right = jnp.where(here, odd[...], even[...]), jnp.where(here, even[...], odd[...])
    sides = side_strips([left[i : i + 1] for i in (3, 4, 5)], [right[i : i + 1] for i in (0, 1, 2)])
    square, seen = back_and_on(
        spots, by_lane, own, sides, rates_of(wide, strips, beside), kept, (field, other), (strip, other_strip), image
    )
    rows = weigh(seen, grams)
    herald(rows, message)
    sums = before[...] + in_lanes(2, [square, jnp.sum(seen * rows, keepdims=True)])
    out[...] = jnp.concatenate([sums] * (out.shape[0] // 8), axis=0)
    for step, row in ((1, OWN + 1), (-1, OWN)):
        out[pl.ds(in_plane(step) * 2 + 1, 1), :] = message[row : row + 1, :]


def in_plane(step):
    size = lax.axis_size(("lat_1", "lon"))
    at = lax.axis_index("lat_1") * LON + lax.rem(lax.axis_index("lon") + LON + step, LON)
    return lax.rem(at + size - middle_of_plane(), size)


def middle_of_plane():
    return lax.axis_size("lat_1") // 2 * LON + LON // 2


def gathered(parts, mine, sums, message):
    count = parts.shape[0] // 2
    sums[...] = jnp.broadcast_to(jnp.sum(parts[pl.ds(0, count, stride=2), :], axis=0, keepdims=True), sums.shape)
    message[...] = mine[...]
    for i, step in enumerate((-1, 1)):
        message[OWN + i : OWN + i + 1, :] = parts[pl.ds(in_plane(step) * 2 + 1, 1), :]


def finish(spots, by_lane, core, mine, inter, wide, strips, beside, parts, right_side, image, increment, residual, field, other, strip, other_strip):
    lists = (core, mine, inter)
    own = padded(jnp.concatenate([x[:OWN, :] for x in lists], axis=0), LANES)
    sides = side_strips(*([x[OWN + i : OWN + i + 1, :] for x in lists] for i in range(2)))
    lay_out(spots, by_lane, own, sides, field, strip, HALO - STEPS, HALO + ROWS + STEPS)
    fields, narrow = steps_back(rates_of(wide, strips, beside), (field, other), (strip, other_strip), STEPS)
    total = jnp.sum(parts[...], axis=0, keepdims=True)
    m0, m1, m2, m3 = (jnp.sum(jnp.where(lanes(1) == i, total, 0.0), keepdims=True) for i in range(4))
    step_0 = m0 / (m0 + m1)
    rho = m1 / m0
    spread = m2 - rho * m1
    curve = (m3 - rho * m2) - rho * (m2 - rho * m1)
    gamma = step_0 * spread / m0
    step_1 = spread / (spread + curve - gamma * spread)
    on_b = step_0 * (1.0 + step_1 * (gamma + rho))
    on_k = -step_0 * step_1
    rest_b = step_0 * ((1.0 - step_1) * rho - step_1 * gamma)
    rest_k = -step_0 * ((1.0 - step_1) + step_1 * (rho + gamma))
    rest_kk = step_0 * step_1
    on_b, on_k, rest_b, rest_k, rest_kk = (jnp.broadcast_to(v, (8, LANES)) for v in (on_b, on_k, rest_b, rest_k, rest_kk))
    for r in range(ROWS):
        for h, second in enumerate(merged(fields[0], narrow[0], r + HALO)):
            at = r * LEVELS + h * 8
            b, first = right_side[at : at + 8, :], image[at : at + 8, :]
            to = pl.ds(h * 8 * ROWS + r, 8, stride=ROWS)
            increment[to, :] = on_b * b + on_k * first
            residual[to, :] = rest_b * b + rest_k * first + rest_kk * second


def to_core(x):
    return lax.ppermute(x, LAT, [(i, i ^ 1) for i in range(lax.axis_size(LAT))])


def to_inter(x):
    return lax.ppermute(x, LAT, [(i, ((i + 1) ^ 1) - 1) for i in range(1, lax.axis_size(LAT) - 1)])


def to_even(x):
    return lax.ppermute(x, "lon", [(i, i ^ 1) for i in range(LON)])


def to_odd(x):
    return lax.ppermute(x, "lon", [(i, (((i + 1) % LON ^ 1) - 1) % LON) for i in range(LON)])


def spread_out(x, axes, first):
    count = lax.axis_size(axes)
    group = [(i + first) % count for i in range(count)]
    return lax.all_to_all(x, axes, split_axis=0, concat_axis=0, tiled=True, axis_index_groups=[group])


def shards(courant, obs_matrix, obs_weight, innovation, block_owner, block_row, block_count):
    flow = courant.reshape(-1, LANES)
    owner, row, count = block_owner.reshape(-1), block_row.reshape(-1), block_count
    wholes = (obs_matrix[0], obs_weight[0], innovation[0])
    (parcels,) = call(
        prepare,
        [(LON * PARCEL, LANES)],
        (owner, row, count, *wholes),
        4_000_000,
        [pltpu.SMEM((CAP,), jnp.int32), pltpu.SMEM((CAP,), jnp.int32), pltpu.SMEM((1, 1), jnp.int32)]
        + [pltpu.VMEM(x.shape, F32) for x in wholes]
        + [pltpu.VMEM((OWN, LANES), F32), pltpu.SemaphoreType.DMA((6,))],
        [pl.BlockSpec(memory_space=pltpu.HBM)] * 6,
        62,
    )
    parcels = spread_out(parcels.reshape(LON, PARCEL, LANES), "lon", FIRST).reshape(LON * PARCEL, LANES)
    edge = (EDGE, LANES), (2 * OWN, LANES)
    for_core, for_inter, for_even, for_odd = call(halo, [edge[0], edge[0], edge[1], edge[1]], (flow,), 1_000_000)
    odd = to_odd(for_odd)
    even = to_even(for_even)
    inter = to_inter(for_inter)
    core = to_core(for_core)
    wide, strips, for_core, for_inter = call(
        arrange,
        [(WIDE * 2 * LEVELS, LANES), (2 * STRIP, LANES), (MESSAGE, LANES), (MESSAGE, LANES)],
        (flow, parcels, core, inter, even, odd),
        2_000_000,
    )
    core, inter = to_core(for_core), to_inter(for_inter)
    (grams,) = call(unpack, [(OWN * LANES, LANES)], (parcels,), 4_000_000)
    cells, listed = (ROWS * LEVELS, LANES), (OWN, LANES)
    work = [pltpu.VMEM((WIDE * LEVELS, LANES), F32)] * 2 + [pltpu.VMEM((WIDE * 8, LANES), F32)] * 2
    work_too = work + [pltpu.VMEM(cells, F32)]
    beside, spots, by_lane, right_side, seen, sums = call(
        first_half,
        [(2 * STRIP, LANES), (2 * LANES, LANES), (16, LANES), cells, listed, (8, LANES)],
        (wide, strips, core, for_core, inter),
        4_000_000,
        work_too,
    )
    rates = (wide, strips, beside)
    short = (HERALD, LANES)
    mine, sums = call(first_terms, [short, (8, LANES)], (grams, seen, sums), 2_000_000)
    core, inter = to_core(mine), to_inter(mine)
    (edges,) = call(edges_of, [(8, LANES)], (core, mine, inter), 10_000)
    lists = (core, mine, inter, to_even(edges), to_odd(edges))
    plane, towers = lax.axis_size(("lat_1", "lon")), lax.axis_size(("lat_0", "lat_2"))
    image, mine, parcels = call(
        second_half, [cells, short, (plane * 2, LANES)], (spots, by_lane, *lists, *rates, grams, sums), 4_000_000, work_too
    )
    parcels = spread_out(parcels.reshape(plane, 2, LANES), ("lat_1", "lon"), middle_of_plane()).reshape(plane * 2, LANES)
    sums, mine = call(gathered, [(towers, LANES), short], (parcels, mine), 10_000)
    core, inter = to_core(mine), to_inter(mine)
    parts = spread_out(sums.reshape(towers, 1, LANES), ("lat_0", "lat_2"), towers * 12 // 16 + 1).reshape(towers, LANES)
    increment, residual = call(
        finish, [cells, cells], (spots, by_lane, core, mine, inter, *rates, parts, right_side, image), 2_000_000, work
    )
    shape = courant.shape[1:]
    return increment.reshape(shape), residual.reshape(shape)


def solution(mesh):
    torus = Mesh(
        mesh.devices.reshape(-1, 4, 2, mesh.shape["lon"]), ("lat_0", "lat_1", "lat_2", "lon")
    )
    placed = (
        P(None, None, LAT, "lon"),
        P(LAT, "lon", None, None),
        P(LAT, "lon", None),
        P(LAT, "lon", None),
        P(LAT, "lon", None),
        P(LAT, "lon"),
        P(LAT, "lon"),
    )
    return jax.shard_map(
        shards,
        mesh=torus,
        in_specs=placed,
        out_specs=(P(None, LAT, "lon"), P(None, LAT, "lon")),
        check_vma=False,
    )
```

```python
import jax
import jax.numpy as jnp
from jax import lax
from jax.experimental import pallas as pl
from jax.experimental.pallas import tpu as pltpu
from jax.sharding import Mesh
from jax.sharding import PartitionSpec as P


LAT = ("lat_0", "lat_1", "lat_2")
LEVELS = 16
ROWS = 16
LANES = 128
CAP = 8
SLOT = 2
STEPS = 4
HALO = 2 * STEPS
WIDE = ROWS + 2 * HALO
LON = 8
HALF = LANES // 2
OWN = LON * SLOT
BULK = 2 * HALF + 2
LIST = BULK + 6
PARCEL = LIST
EDGE = HALO * 2 * LEVELS
STRIP = HALO * 2 * 8
RAW = 2 * 2 * 8
LEFTS = RAW + OWN
RIGHTS = LEFTS + OWN
SPOTS = RIGHTS + OWN
MESSAGE = SPOTS + 8
HERALD = OWN + 8
NOWHERE = -4096.0
FIRST = 6
HIGHEST = lax.Precision.HIGHEST
F32 = jnp.float32
VMEM = pl.BlockSpec(memory_space=pltpu.VMEM)
SMEM = pl.BlockSpec(memory_space=pltpu.SMEM)


def lanes(rows):
    return lax.broadcasted_iota(jnp.int32, (rows, LANES), 1)


def places(rows):
    return lax.broadcasted_iota(jnp.int32, (rows, LANES), 0)


def roll(x, shift):
    shift %= LANES
    return pltpu.roll(x, shift, axis=1) if shift else x


def call(body, outs, args, flops, scratch=(), specs=None, room=24):
    return pl.pallas_call(
        body,
        out_shape=[jax.ShapeDtypeStruct(s, F32) for s in outs],
        in_specs=specs or [SMEM if a.dtype == jnp.int32 else VMEM for a in args],
        out_specs=[VMEM] * len(outs),
        scratch_shapes=list(scratch),
        compiler_params=pltpu.CompilerParams(vmem_limit_bytes=room << 20),
        cost_estimate=pl.CostEstimate(flops=flops, bytes_accessed=0, transcendentals=0),
    )(*args)


def turns_of(owners):
    return [sum([(o == owners[j]).astype(jnp.int32) for o in owners[:j]], jnp.int32(0)) for j in range(CAP)]


def chunk(owner):
    return (owner + LON - FIRST) % LON if isinstance(owner, int) else lax.rem(owner + LON - FIRST, LON)


def packed_edges(pick, shift):
    ln = lanes(8)
    out = jnp.zeros((8, LANES), F32)
    for k in range(8):
        low, high = pick(k)
        out = jnp.where((ln >= 16 * k) & (ln < 16 * k + 8), roll(low, 16 * k + shift), out)
        out = jnp.where((ln >= 16 * k + 8) & (ln < 16 * k + 16), roll(high, 16 * k + 8 + shift), out)
    return out


def weigh_blocks(owners, turns, count, matrix, weight, parcels):
    ln, rw = lanes(HALF), places(HALF)
    for j in range(CAP):
        block = matrix[j]
        scaled = jnp.transpose(block) * jnp.where(j < count[0, 0], weight[j : j + 1, :], 0.0)
        gram = jnp.dot(scaled, block, precision=HIGHEST, preferred_element_type=F32)
        top, low = gram[:HALF], gram[HALF:]
        packed = jnp.where((ln >= HALF) & (ln - HALF <= rw), roll(top, HALF), low)
        diagonal = jnp.sum(jnp.where(ln - HALF == rw, low, 0.0), axis=0, keepdims=True)
        at = chunk(owners[j]) * PARCEL + turns[j] * HALF
        parcels[pl.ds(pl.multiple_of(at, 8), HALF), :] = packed
        parcels[pl.ds(chunk(owners[j]) * PARCEL + 2 * HALF + turns[j], 1), :] = diagonal


def prepare(owner_at, row_at, count_at, matrix_at, weight_at, innovation_at, parcels, owner, row, count, matrix, weight, innovation, lists, sems):
    pairs = ((matrix_at, matrix), (owner_at, owner), (row_at, row), (count_at, count), (weight_at, weight), (innovation_at, innovation))
    copies = [pltpu.make_async_copy(a, b, sems.at[i]) for i, (a, b) in enumerate(pairs)]
    for copy in copies:
        copy.start()
    for d in range(LON):
        parcels[d * PARCEL : d * PARCEL + LIST, :] = jnp.zeros((LIST, LANES), F32)
    lists[...] = jnp.zeros(lists.shape, F32)
    for copy in copies:
        copy.wait()
    owners = [owner[j] for j in range(CAP)]
    turns = turns_of(owners)
    column = jnp.transpose(weight[...] * innovation[...])
    ln = lanes(8)
    named = jnp.full((8, LANES), NOWHERE, F32)
    for j in range(CAP):
        live = j < count[0, 0]
        total = jnp.zeros((8, LANES), F32)
        for k in range(LANES // 8):
            total += matrix[j, k * 8 : k * 8 + 8, :] * column[k * 8 : k * 8 + 8, j : j + 1]
        slot = owners[j] * SLOT + turns[j]
        lists[pl.ds(slot, 1), :] = jnp.where(live, jnp.sum(total, axis=0, keepdims=True), 0.0)
        place = jnp.where(live, (lax.rem(row[j], ROWS) + HALO) * LEVELS + lax.div(row[j], ROWS), int(NOWHERE)).astype(F32)
        named = jnp.where(ln == slot, place, named)
    weigh_blocks(owners, turns, count, matrix, weight, parcels)
    named = jnp.where(ln < OWN, named, roll(named, OWN))
    line = lanes(1)
    for d in range(LON):
        left, right = 2 * (d - 1) % OWN, 2 * (d + 1) % OWN
        at = chunk(d) * PARCEL + BULK
        parcels[at : at + 2, :] = lists[2 * d : 2 * d + 2, :]
        edge = jnp.where(line < 8, roll(lists[left : left + 1, :], 8), roll(lists[left + 1 : left + 2, :], 16))
        edge = jnp.where(line < 16, edge, jnp.where(line < 24, roll(lists[right : right + 1, :], 16), roll(lists[right + 1 : right + 2, :], 24)))
        parcels[at + 2 : at + 3, :] = edge
        parcels[at + 3 : at + 4, :] = roll(named, -left)[:1]


def halo(flow, to_core, to_inter, to_even, to_odd):
    even = lax.axis_index("lat_2") == 0
    here = lax.rem(lax.axis_index("lon"), 2) == 0
    for f in range(2):
        for g in range(2):

            def pick(k, f=f, g=g):
                at = f * LEVELS * ROWS + g * 8 + k
                return flow[pl.ds(at, 8, stride=ROWS), :], flow[pl.ds(at + 8 * ROWS, 8, stride=ROWS), :]

            at = (f * 2 + g) * 8
            to_right, to_left = packed_edges(pick, 8), packed_edges(pick, 0)
            to_even[at : at + 8, :] = jnp.where(here, to_right, to_left)
            to_odd[at : at + 8, :] = jnp.where(here, to_left, to_right)
        for i in range(HALO):
            for h in range(2):
                at = f * LEVELS * ROWS + h * 8 * ROWS + i
                up, down = flow[pl.ds(at + ROWS - HALO, 8, stride=ROWS), :], flow[pl.ds(at, 8, stride=ROWS), :]
                at = (i * 2 + f) * LEVELS + h * 8
                to_core[at : at + 8, :] = jnp.where(even, up, down)
                to_inter[at : at + 8, :] = jnp.where(even, down, up)


def backwards(x):
    return jnp.concatenate([x[i : i + 1] for i in reversed(range(x.shape[0]))], axis=0)


def strip_of(low, high, left, right, k):
    ln = lanes(8)
    a = jnp.where(ln < 8, roll(left, -16 * k), jnp.where(ln < 32, roll(low, 8), jnp.where(ln < 56, roll(low, 56), roll(right, 56 - 16 * k))))
    b = jnp.where(ln < 72, roll(left, 56 - 16 * k), jnp.where(ln < 96, roll(high, 72), jnp.where(ln < 120, roll(high, 120), roll(right, 112 - 16 * k))))
    return jnp.where(ln < HALF, a, b)


def widen(flow, core, inter, even_edges, odd_edges, wide, strips):
    even = lax.axis_index("lat_2") == 0
    wide[:EDGE, :] = jnp.where(even, inter[...], core[...])
    wide[EDGE + ROWS * 2 * LEVELS :, :] = jnp.where(even, core[...], inter[...])
    for f in range(2):
        for g in range(2):
            left, right = left_and_right(even_edges, odd_edges, f, g)
            for k in range(8):
                at = f * LEVELS * ROWS + g * 8 + k
                low, high = flow[pl.ds(at, 8, stride=ROWS), :], flow[pl.ds(at + 8 * ROWS, 8, stride=ROWS), :]
                at = EDGE + ((g * 8 + k) * 2 + f) * LEVELS
                wide[at : at + 8, :] = low
                wide[at + 8 : at + 16, :] = high
                at = ((g * 8 + k) * 2 + f) * 8
                strips[at : at + 8, :] = strip_of(low, high, left, right, k)


def left_and_right(even_edges, odd_edges, f, g):
    here = lax.rem(lax.axis_index("lon"), 2) == 0
    at = (f * 2 + g) * 8
    first, second = even_edges[at : at + 8, :], odd_edges[at : at + 8, :]
    return jnp.where(here, second, first), jnp.where(here, first, second)


def arrange(parcels, even_edges, odd_edges, to_core, to_inter):
    ln = lanes(8)
    even = lax.axis_index("lat_2") == 0
    for f in range(2):
        lower, upper = (left_and_right(even_edges, odd_edges, f, g) for g in range(2))
        for side in range(2):
            at = (f * 2 + side) * 8
            to_core[at : at + 8, :] = jnp.where(even, upper[side], lower[side])
            to_inter[at : at + 8, :] = jnp.where(even, lower[side], upper[side])
    edge = backwards(parcels[pl.ds(BULK + 2, LON, stride=PARCEL), :])
    named = parcels[pl.ds(BULK + 3, LON, stride=PARCEL), :]
    turned, turned_back = jnp.transpose(named), jnp.transpose(backwards(named))
    spot = jnp.full((1, LANES), NOWHERE, F32)
    line = lanes(1)
    for i, k in enumerate((2, 3, 0, 1, 4, 5)):
        rows = turned if k in (2, 3) else turned_back
        line_k = jnp.concatenate([rows[k : k + 1, :], jnp.zeros((1, LANES - LON), F32)], axis=1)
        spot = jnp.where((line >= 8 * i) & (line < 8 * i + 8), roll(line_k, 8 * i), spot)
    for o in range(SLOT):
        own = parcels[pl.ds(BULK + o, LON, stride=PARCEL), :]
        left = jnp.where(ln < 8, roll(edge, -8 * o), 0.0)
        right = jnp.where((ln >= 56) & (ln < 64), roll(edge, 40 - 8 * o), 0.0)
        for out in (to_core, to_inter):
            out[RAW + o * LON : RAW + (o + 1) * LON, :] = own
            out[LEFTS + o * LON : LEFTS + (o + 1) * LON, :] = left
            out[RIGHTS + o * LON : RIGHTS + (o + 1) * LON, :] = right
    for out in (to_core, to_inter):
        out[SPOTS:, :] = jnp.broadcast_to(spot, (8, LANES))


def unpack(parcels, grams):
    ln, rw = lanes(HALF), places(HALF)
    upper, diagonal, first = ln - HALF > rw, ln - HALF == rw, ln < HALF
    for s in range(LON):
        both = parcels[s * PARCEL : s * PARCEL + 2 * HALF, :]
        turned = jnp.transpose(both)
        ct, et = turned[:HALF], turned[HALF:]
        ct_rolled, et_rolled = roll(ct, HALF), roll(et, HALF)
        for o in range(SLOT):
            q = both[o * HALF : (o + 1) * HALF]
            d = parcels[s * PARCEL + 2 * HALF + o : s * PARCEL + 2 * HALF + o + 1, :]
            e_first, e_last = (et, et_rolled) if o == 0 else (et_rolled, et)
            c_last = ct_rolled if o == 0 else ct
            top = jnp.where(first, jnp.where(ln <= rw, roll(q, HALF), e_first), c_last)
            low = jnp.where(first | upper, q, jnp.where(diagonal, d, e_last))
            at = (o * LON + s) * LANES
            grams[at : at + HALF, :] = top
            grams[at + HALF : at + LANES, :] = low


def split(x):
    high = x.astype(jnp.bfloat16)
    rest = x - high.astype(F32)
    middle = rest.astype(jnp.bfloat16)
    low = (rest - middle.astype(F32)).astype(jnp.bfloat16)
    return jnp.concatenate([high, middle, low], axis=1)


def chosen(one_hot, parts):
    out = jnp.dot(one_hot, parts, preferred_element_type=F32)
    return out[:, :LANES] + out[:, LANES : 2 * LANES] + out[:, 2 * LANES :]


def one_hot(index, at):
    return jnp.where(index == at, 1.0, 0.0).astype(jnp.bfloat16)


def padded(x, rows):
    return jnp.concatenate([x, jnp.zeros((rows - x.shape[0], LANES), F32)], axis=0)


def lay_out(spots, by_lane, own, sides, field, strips, low, high):
    ln = lanes(LANES)
    own_strip = jnp.where(ln < 32, jnp.where(ln >= 8, roll(own, 8), 0.0), jnp.where(ln < 56, roll(own, 56), 0.0))
    pieces = []
    for i, strip in enumerate((own_strip, sides)):
        upper = (spots[i * LANES : (i + 1) * LANES, :].astype(jnp.int32) & 8) != 0
        pieces.append(split(jnp.where(upper, roll(strip, HALF), strip)))
    own_parts = split(own)
    lane_spots = [by_lane[i * 8 : i * 8 + 1, :].astype(jnp.int32) for i in range(2)]
    p = jnp.broadcast_to(lane_spots[0], (LANES, LANES))
    for start in range(low * LEVELS, high * LEVELS, LANES):
        field[start : start + LANES, :] = chosen(one_hot(places(LANES) + start, p), own_parts)
    folded = [jnp.broadcast_to(((b >> 4) << 3) + (b & 7), (64, LANES)) for b in lane_spots]
    for start in range(low * 8, high * 8, 64):
        at = places(64) + start
        strips[start : start + 64, :] = chosen(one_hot(at, folded[0]), pieces[0]) + chosen(one_hot(at, folded[1]), pieces[1])


def adjoint(rates, source, target, first, last, height):
    before = kept = None
    for r in range(first, last + 1):
        y = source[r * height : (r + 1) * height, :]
        lat, lon = rates(r)
        t = lat * y
        a = jnp.where(lat > 0.0, t, 0.0)
        b = a - t
        s = lon * y
        e = jnp.where(lon > 0.0, s, 0.0)
        f = e - s
        if r > first + 1:
            target[(r - 1) * height : r * height, :] = kept + a
        if r > first:
            kept = y - (a + b) - (e + f) + roll(e, -1) + roll(f, 1) + before
        before = b


def tangent(rates, source, target, first, last, height):
    for r in range(first + 1, last):
        x = source[r * height : (r + 1) * height, :]
        south = source[(r - 1) * height : r * height, :]
        north = source[(r + 1) * height : (r + 2) * height, :]
        lat, lon = rates(r)
        out = x + jnp.abs(lat) * (jnp.where(lat > 0.0, south, north) - x)
        target[r * height : (r + 1) * height, :] = out + jnp.abs(lon) * (jnp.where(lon > 0.0, roll(x, 1), roll(x, -1)) - x)


def merged(field, strips, r):
    ln = lanes(8)
    t = strips[r * 8 : (r + 1) * 8, :]
    low, high = field[r * LEVELS : r * LEVELS + 8, :], field[r * LEVELS + 8 : (r + 1) * LEVELS, :]
    low = jnp.where(ln < 8, roll(t, -8), jnp.where(ln >= 120, roll(t, 72), low))
    high = jnp.where(ln < 8, roll(t, -72), jnp.where(ln >= 120, roll(t, 8), high))
    return low, high


def steps_back(rates, fields, strips, first):
    full, narrow = rates
    for k in range(first, first + STEPS):
        adjoint(full, *fields, k, WIDE - 1 - k, LEVELS)
        adjoint(narrow, *strips, k, WIDE - 1 - k, 8)
        fields, strips = fields[::-1], strips[::-1]
    return fields, strips


def steps_on(rates, fields, strips, first):
    full, narrow = rates
    for k in range(first, first + STEPS):
        tangent(full, *fields, k, WIDE - 1 - k, LEVELS)
        tangent(narrow, *strips, k, WIDE - 1 - k, 8)
        fields, strips = fields[::-1], strips[::-1]
    return fields, strips


def rates_of(wide, mine, beside):
    def full(r):
        at = r * 2 * LEVELS
        return wide[at : at + LEVELS, :], wide[at + LEVELS : at + 2 * LEVELS, :]

    def narrow(r):
        ref, r = (mine, r - HALO) if HALO <= r < HALO + ROWS else (beside, r if r < HALO else r - ROWS)
        return ref[r * 16 : r * 16 + 8, :], ref[r * 16 + 8 : r * 16 + 16, :]

    return full, narrow


def back_and_on(spots, by_lane, own, sides, rates, kept, fields, strips, image):
    lay_out(spots, by_lane, own, sides, fields[0], strips[0], 0, WIDE)
    fields, strips = steps_back(rates, fields, strips, 0)
    lat, last = lax.axis_index(LAT), lax.axis_size(LAT) - 1
    for outside, start in ((lat == 0, STEPS), (lat == last, HALO + ROWS)):
        for ref, height in ((fields[0], LEVELS), (strips[0], 8)):
            block = ref[start * height : (start + STEPS) * height, :]
            ref[start * height : (start + STEPS) * height, :] = jnp.where(outside, 0.0, block)
    square = jnp.zeros((8, LANES), F32)
    for r in range(ROWS):
        low, high = merged(fields[0], strips[0], r + HALO)
        kept[r * LEVELS : r * LEVELS + 8, :] = low
        kept[r * LEVELS + 8 : (r + 1) * LEVELS, :] = high
        square += low * low + high * high
    fields, strips = steps_on(rates, fields, strips, STEPS)
    for r in range(ROWS):
        low, high = merged(fields[0], strips[0], r + HALO)
        image[r * LEVELS : r * LEVELS + 8, :] = low
        image[r * LEVELS + 8 : (r + 1) * LEVELS, :] = high
    mine = spots[OWN : 2 * OWN, :].astype(jnp.int32) - HALO * LEVELS
    hit = jnp.concatenate([one_hot(lanes(OWN), mine), one_hot(lanes(OWN) + LANES, mine)], axis=1)
    return jnp.sum(square, keepdims=True), chosen(hit, split(image[...]))


def weigh(seen, grams):
    column = jnp.transpose(seen)
    out = []
    for t in range(OWN):
        total = jnp.zeros((8, LANES), F32)
        for k in range(LANES // 8):
            at = t * LANES + k * 8
            total += grams[at : at + 8, :] * column[k * 8 : k * 8 + 8, t : t + 1]
        out.append(jnp.sum(total, axis=0, keepdims=True))
    return jnp.concatenate(out, axis=0)


def in_lanes(first, values):
    ln = lanes(8)
    out = jnp.zeros((8, LANES), F32)
    for i, v in enumerate(values):
        out = jnp.where(ln == first + i, v, out)
    return out


def first_half(wide, mine, core, own_message, inter, beside, spots, by_lane, kept, seen, sums, field, other, strip, other_strip, image):
    ln = lanes(8)
    even = lax.axis_index("lat_2") == 0
    for n in range(2):
        edges = jnp.where(even == (n == 0), inter[:RAW, :], core[:RAW, :])
        for f in range(2):
            left, right = edges[f * 16 : f * 16 + 8], edges[f * 16 + 8 : f * 16 + 16]
            for k in range(HALO):
                at = ((n * (HALO + ROWS) + k) * 2 + f) * LEVELS
                low, high = wide[at : at + 8, :], wide[at + 8 : at + 16, :]
                at = n * STRIP + (k * 2 + f) * 8
                beside[at : at + 8, :] = strip_of(low, high, left, right, k)
    step = jnp.where(even, float(ROWS * LEVELS), -float(ROWS * LEVELS))
    c, o, i = core[SPOTS:, :] + step, own_message[SPOTS:, :], inter[SPOTS:, :] - step
    tables = (((c, 0), (o, 0), (i, 0)), ((c, 16), (o, 16), (i, 16), (c, 32), (o, 32), (i, 32)))
    for t, table in enumerate(tables):
        spot = jnp.full((8, LANES), NOWHERE, F32)
        for n, (x, at) in enumerate(table):
            spot = jnp.where((ln >= OWN * n) & (ln < OWN * (n + 1)), roll(x, OWN * n - at), spot)
        by_lane[t * 8 : t * 8 + 8, :] = spot
        spots[t * LANES : (t + 1) * LANES, :] = jnp.transpose(jnp.broadcast_to(spot[:1], (LANES, LANES)))
    parts = (core, own_message, inter)
    own = padded(jnp.concatenate([x[RAW:LEFTS, :] for x in parts], axis=0), LANES)
    sides = padded(jnp.concatenate([x[LEFTS:RIGHTS, :] for x in parts] + [x[RIGHTS:SPOTS, :] for x in parts], axis=0), LANES)
    square, rows = back_and_on(spots, by_lane, own, sides, rates_of(wide, mine, beside), kept, (field, other), (strip, other_strip), image)
    seen[...] = rows
    sums[...] = in_lanes(0, [square])


def fanned(x, shift):
    return pltpu.roll(x, shift % LANES, axis=1, stride=8, stride_axis=0)


def herald(rows, message):
    mine = (lanes(OWN) >> 3) == places(OWN)
    message[:OWN, :] = rows
    for at, shift in ((OWN, 0), (OWN + 1, 8)):
        spread = jnp.concatenate([fanned(rows[:8], shift), fanned(rows[8:], shift + HALF)], axis=0)
        message[at : at + 1, :] = jnp.sum(jnp.where(mine, spread, 0.0), axis=0, keepdims=True)
    message[OWN + 2 :, :] = jnp.zeros((HERALD - OWN - 2, LANES), F32)


def first_terms(grams, seen, before, message, sums):
    rows = weigh(seen[...], grams)
    herald(rows, message)
    sums[...] = before[...] + in_lanes(1, [jnp.sum(seen[...] * rows, keepdims=True)])


def edges_of(core, mine, inter, out):
    for i, x in enumerate((core, mine, inter)):
        out[i : i + 1, :] = x[OWN : OWN + 1, :]
        out[i + 3 : i + 4, :] = x[OWN + 1 : OWN + 2, :]
    out[6:, :] = jnp.zeros((2, LANES), F32)


def side_strips(lefts, rights):
    ln = lanes(OWN)

    def rows(x, shift):
        x = jnp.broadcast_to(x, (8, LANES))
        return jnp.concatenate([fanned(x, shift - 56), fanned(x, shift - 120)], axis=0)

    out = [jnp.where(ln < 8, rows(x, 0), 0.0) for x in lefts]
    out += [jnp.where((ln >= 56) & (ln < 64), rows(x, 56), 0.0) for x in rights]
    return padded(jnp.concatenate(out, axis=0), LANES)


def second_half(spots, by_lane, core, mine, inter, even, odd, wide, strips, beside, grams, before, kept, message, out, field, other, strip, other_strip, image):
    own = padded(jnp.concatenate([x[:OWN, :] for x in (core, mine, inter)], axis=0), LANES)
    here = lax.rem(lax.axis_index("lon"), 2) == 0
    left, right = jnp.where(here, odd[...], even[...]), jnp.where(here, even[...], odd[...])
    sides = side_strips([left[i : i + 1] for i in (3, 4, 5)], [right[i : i + 1] for i in (0, 1, 2)])
    square, seen = back_and_on(
        spots, by_lane, own, sides, rates_of(wide, strips, beside), kept, (field, other), (strip, other_strip), image
    )
    rows = weigh(seen, grams)
    herald(rows, message)
    sums = before[...] + in_lanes(2, [square, jnp.sum(seen * rows, keepdims=True)])
    out[...] = jnp.concatenate([sums] * (out.shape[0] // 8), axis=0)
    for step, row in ((1, OWN + 1), (-1, OWN)):
        out[pl.ds(in_plane(step) * 2 + 1, 1), :] = message[row : row + 1, :]


def in_plane(step):
    size = lax.axis_size(("lat_1", "lon"))
    at = lax.axis_index("lat_1") * LON + lax.rem(lax.axis_index("lon") + LON + step, LON)
    return lax.rem(at + size - middle_of_plane(), size)


def middle_of_plane():
    return lax.axis_size("lat_1") // 2 * LON + LON // 2


def gathered(parts, mine, sums, message):
    count = parts.shape[0] // 2
    sums[...] = jnp.broadcast_to(jnp.sum(parts[pl.ds(0, count, stride=2), :], axis=0, keepdims=True), sums.shape)
    message[...] = mine[...]
    for i, step in enumerate((-1, 1)):
        message[OWN + i : OWN + i + 1, :] = parts[pl.ds(in_plane(step) * 2 + 1, 1), :]


def finish(spots, by_lane, core, mine, inter, wide, strips, beside, parts, right_side, image, increment, residual, field, other, strip, other_strip):
    lists = (core, mine, inter)
    own = padded(jnp.concatenate([x[:OWN, :] for x in lists], axis=0), LANES)
    sides = side_strips(*([x[OWN + i : OWN + i + 1, :] for x in lists] for i in range(2)))
    lay_out(spots, by_lane, own, sides, field, strip, HALO - STEPS, HALO + ROWS + STEPS)
    fields, narrow = steps_back(rates_of(wide, strips, beside), (field, other), (strip, other_strip), STEPS)
    total = jnp.sum(parts[...], axis=0, keepdims=True)
    m0, m1, m2, m3 = (jnp.sum(jnp.where(lanes(1) == i, total, 0.0), keepdims=True) for i in range(4))
    step_0 = m0 / (m0 + m1)
    rho = m1 / m0
    spread = m2 - rho * m1
    curve = (m3 - rho * m2) - rho * (m2 - rho * m1)
    gamma = step_0 * spread / m0
    step_1 = spread / (spread + curve - gamma * spread)
    on_b = step_0 * (1.0 + step_1 * (gamma + rho))
    on_k = -step_0 * step_1
    rest_b = step_0 * ((1.0 - step_1) * rho - step_1 * gamma)
    rest_k = -step_0 * ((1.0 - step_1) + step_1 * (rho + gamma))
    rest_kk = step_0 * step_1
    on_b, on_k, rest_b, rest_k, rest_kk = (jnp.broadcast_to(v, (8, LANES)) for v in (on_b, on_k, rest_b, rest_k, rest_kk))
    for r in range(ROWS):
        for h, second in enumerate(merged(fields[0], narrow[0], r + HALO)):
            at = r * LEVELS + h * 8
            b, first = right_side[at : at + 8, :], image[at : at + 8, :]
            to = pl.ds(h * 8 * ROWS + r, 8, stride=ROWS)
            increment[to, :] = on_b * b + on_k * first
            residual[to, :] = rest_b * b + rest_k * first + rest_kk * second


def to_core(x):
    return lax.ppermute(x, LAT, [(i, i ^ 1) for i in range(lax.axis_size(LAT))])


def to_inter(x):
    return lax.ppermute(x, LAT, [(i, ((i + 1) ^ 1) - 1) for i in range(1, lax.axis_size(LAT) - 1)])


def to_even(x):
    return lax.ppermute(x, "lon", [(i, i ^ 1) for i in range(LON)])


def to_odd(x):
    return lax.ppermute(x, "lon", [(i, (((i + 1) % LON ^ 1) - 1) % LON) for i in range(LON)])


def spread_out(x, axes, first):
    count = lax.axis_size(axes)
    group = [(i + first) % count for i in range(count)]
    return lax.all_to_all(x, axes, split_axis=0, concat_axis=0, tiled=True, axis_index_groups=[group])


def shards(courant, obs_matrix, obs_weight, innovation, block_owner, block_row, block_count):
    flow = courant.reshape(-1, LANES)
    owner, row, count = block_owner.reshape(-1), block_row.reshape(-1), block_count
    wholes = (obs_matrix[0], obs_weight[0], innovation[0])
    (parcels,) = call(
        prepare,
        [(LON * PARCEL, LANES)],
        (owner, row, count, *wholes),
        4_000_000,
        [pltpu.SMEM((CAP,), jnp.int32), pltpu.SMEM((CAP,), jnp.int32), pltpu.SMEM((1, 1), jnp.int32)]
        + [pltpu.VMEM(x.shape, F32) for x in wholes]
        + [pltpu.VMEM((OWN, LANES), F32), pltpu.SemaphoreType.DMA((6,))],
        [pl.BlockSpec(memory_space=pltpu.HBM)] * 6,
        62,
    )
    parcels = spread_out(parcels.reshape(LON, PARCEL, LANES), "lon", FIRST).reshape(LON * PARCEL, LANES)
    edge = (EDGE, LANES), (2 * OWN, LANES)
    for_core, for_inter, for_even, for_odd = call(halo, [edge[0], edge[0], edge[1], edge[1]], (flow,), 1_000_000)
    odd = to_odd(for_odd)
    even = to_even(for_even)
    inter = to_inter(for_inter)
    core = to_core(for_core)
    wide, strips = call(
        widen, [(WIDE * 2 * LEVELS, LANES), (2 * STRIP, LANES)], (flow, core, inter, even, odd), 4_000_000
    )
    for_core, for_inter = call(arrange, [(MESSAGE, LANES)] * 2, (parcels, even, odd), 1_000_000)
    core, inter = to_core(for_core), to_inter(for_inter)
    (grams,) = call(unpack, [(OWN * LANES, LANES)], (parcels,), 4_000_000)
    cells, listed = (ROWS * LEVELS, LANES), (OWN, LANES)
    work = [pltpu.VMEM((WIDE * LEVELS, LANES), F32)] * 2 + [pltpu.VMEM((WIDE * 8, LANES), F32)] * 2
    work_too = work + [pltpu.VMEM(cells, F32)]
    beside, spots, by_lane, right_side, seen, sums = call(
        first_half,
        [(2 * STRIP, LANES), (2 * LANES, LANES), (16, LANES), cells, listed, (8, LANES)],
        (wide, strips, core, for_core, inter),
        4_000_000,
        work_too,
    )
    rates = (wide, strips, beside)
    short = (HERALD, LANES)
    mine, sums = call(first_terms, [short, (8, LANES)], (grams, seen, sums), 2_000_000)
    core, inter = to_core(mine), to_inter(mine)
    (edges,) = call(edges_of, [(8, LANES)], (core, mine, inter), 10_000)
    lists = (core, mine, inter, to_even(edges), to_odd(edges))
    plane, towers = lax.axis_size(("lat_1", "lon")), lax.axis_size(("lat_0", "lat_2"))
    image, mine, parcels = call(
        second_half, [cells, short, (plane * 2, LANES)], (spots, by_lane, *lists, *rates, grams, sums), 4_000_000, work_too
    )
    parcels = spread_out(parcels.reshape(plane, 2, LANES), ("lat_1", "lon"), middle_of_plane()).reshape(plane * 2, LANES)
    sums, mine = call(gathered, [(towers, LANES), short], (parcels, mine), 10_000)
    core, inter = to_core(mine), to_inter(mine)
    parts = spread_out(sums.reshape(towers, 1, LANES), ("lat_0", "lat_2"), towers * 12 // 16 + 1).reshape(towers, LANES)
    increment, residual = call(
        finish, [cells, cells], (spots, by_lane, core, mine, inter, *rates, parts, right_side, image), 2_000_000, work
    )
    shape = courant.shape[1:]
    return increment.reshape(shape), residual.reshape(shape)


def solution(mesh):
    torus = Mesh(
        mesh.devices.reshape(-1, 4, 2, mesh.shape["lon"]), ("lat_0", "lat_1", "lat_2", "lon")
    )
    placed = (
        P(None, None, LAT, "lon"),
        P(LAT, "lon", None, None),
        P(LAT, "lon", None),
        P(LAT, "lon", None),
        P(LAT, "lon", None),
        P(LAT, "lon"),
        P(LAT, "lon"),
    )
    return jax.shard_map(
        shards,
        mesh=torus,
        in_specs=placed,
        out_specs=(P(None, LAT, "lon"), P(None, LAT, "lon")),
        check_vma=False,
    )
```

```python
import jax
import jax.numpy as jnp
from jax import lax
from jax.experimental import pallas as pl
from jax.experimental.pallas import tpu as pltpu
from jax.sharding import Mesh
from jax.sharding import PartitionSpec as P


LAT = ("lat_0", "lat_1", "lat_2")
LEVELS = 16
ROWS = 16
LANES = 128
CAP = 8
SLOT = 2
STEPS = 4
HALO = 2 * STEPS
WIDE = ROWS + 2 * HALO
LON = 8
HALF = LANES // 2
OWN = LON * SLOT
NEAR = 3 * OWN
BULK = 2 * HALF + 2
LIST = BULK + 6
PARCEL = LIST
EDGE = HALO * 2 * LEVELS
STRIP = HALO * 2 * 8
RAW = 2 * 2 * 8
LEFTS = RAW + OWN
RIGHTS = LEFTS + OWN
SPOTS = RIGHTS + OWN
MESSAGE = SPOTS + 8
HERALD = OWN + 8
NOWHERE = -4096.0
FIRST = 5
HIGHEST = lax.Precision.HIGHEST
F32 = jnp.float32
VMEM = pl.BlockSpec(memory_space=pltpu.VMEM)
SMEM = pl.BlockSpec(memory_space=pltpu.SMEM)


def lanes(rows):
    return lax.broadcasted_iota(jnp.int32, (rows, LANES), 1)


def places(rows):
    return lax.broadcasted_iota(jnp.int32, (rows, LANES), 0)


def roll(x, shift):
    shift %= LANES
    return pltpu.roll(x, shift, axis=1) if shift else x


def call(body, outs, args, flops, scratch=(), specs=None, room=24):
    return pl.pallas_call(
        body,
        out_shape=[jax.ShapeDtypeStruct(s, F32) for s in outs],
        in_specs=specs or [SMEM if a.dtype == jnp.int32 else VMEM for a in args],
        out_specs=[VMEM] * len(outs),
        scratch_shapes=list(scratch),
        compiler_params=pltpu.CompilerParams(vmem_limit_bytes=room << 20),
        cost_estimate=pl.CostEstimate(flops=flops, bytes_accessed=0, transcendentals=0),
    )(*args)


def turns_of(owners):
    return [sum([(o == owners[j]).astype(jnp.int32) for o in owners[:j]], jnp.int32(0)) for j in range(CAP)]


def chunk(owner):
    return (owner + LON - FIRST) % LON if isinstance(owner, int) else lax.rem(owner + LON - FIRST, LON)


def packed_edges(pick, shift):
    ln = lanes(8)
    out = jnp.zeros((8, LANES), F32)
    for k in range(8):
        low, high = pick(k)
        out = jnp.where((ln >= 16 * k) & (ln < 16 * k + 8), roll(low, 16 * k + shift), out)
        out = jnp.where((ln >= 16 * k + 8) & (ln < 16 * k + 16), roll(high, 16 * k + 8 + shift), out)
    return out


def weigh_blocks(owners, turns, count, matrix, weight, parcels):
    ln, rw = lanes(HALF), places(HALF)
    for j in range(CAP):
        block = matrix[j]
        scaled = jnp.transpose(block) * jnp.where(j < count[0, 0], weight[j : j + 1, :], 0.0)
        gram = jnp.dot(scaled, block, precision=HIGHEST, preferred_element_type=F32)
        top, low = gram[:HALF], gram[HALF:]
        packed = jnp.where((ln >= HALF) & (ln - HALF <= rw), roll(top, HALF), low)
        diagonal = jnp.sum(jnp.where(ln - HALF == rw, low, 0.0), axis=0, keepdims=True)
        at = chunk(owners[j]) * PARCEL + turns[j] * HALF
        parcels[pl.ds(pl.multiple_of(at, 8), HALF), :] = packed
        parcels[pl.ds(chunk(owners[j]) * PARCEL + 2 * HALF + turns[j], 1), :] = diagonal


def prepare(owner_at, row_at, count_at, matrix_at, weight_at, innovation_at, parcels, owner, row, count, matrix, weight, innovation, lists, sems):
    pairs = ((matrix_at, matrix), (owner_at, owner), (row_at, row), (count_at, count), (weight_at, weight), (innovation_at, innovation))
    copies = [pltpu.make_async_copy(a, b, sems.at[i]) for i, (a, b) in enumerate(pairs)]
    for copy in copies:
        copy.start()
    for d in range(LON):
        parcels[d * PARCEL : d * PARCEL + LIST, :] = jnp.zeros((LIST, LANES), F32)
    lists[...] = jnp.zeros(lists.shape, F32)
    for copy in copies:
        copy.wait()
    owners = [owner[j] for j in range(CAP)]
    turns = turns_of(owners)
    column = jnp.transpose(weight[...] * innovation[...])
    ln = lanes(8)
    named = jnp.full((8, LANES), NOWHERE, F32)
    for j in range(CAP):
        live = j < count[0, 0]
        total = jnp.zeros((8, LANES), F32)
        for k in range(LANES // 8):
            total += matrix[j, k * 8 : k * 8 + 8, :] * column[k * 8 : k * 8 + 8, j : j + 1]
        slot = owners[j] * SLOT + turns[j]
        lists[pl.ds(slot, 1), :] = jnp.where(live, jnp.sum(total, axis=0, keepdims=True), 0.0)
        place = jnp.where(live, (lax.rem(row[j], ROWS) + HALO) * LEVELS + lax.div(row[j], ROWS), int(NOWHERE)).astype(F32)
        named = jnp.where(ln == slot, place, named)
    weigh_blocks(owners, turns, count, matrix, weight, parcels)
    named = jnp.where(ln < OWN, named, roll(named, OWN))
    line = lanes(1)
    for d in range(LON):
        left, right = 2 * (d - 1) % OWN, 2 * (d + 1) % OWN
        at = chunk(d) * PARCEL + BULK
        parcels[at : at + 2, :] = lists[2 * d : 2 * d + 2, :]
        edge = jnp.where(line < 8, roll(lists[left : left + 1, :], 8), roll(lists[left + 1 : left + 2, :], 16))
        edge = jnp.where(line < 16, edge, jnp.where(line < 24, roll(lists[right : right + 1, :], 16), roll(lists[right + 1 : right + 2, :], 24)))
        parcels[at + 2 : at + 3, :] = edge
        parcels[at + 3 : at + 4, :] = roll(named, -left)[:1]


def halo(flow, to_core, to_inter, to_even, to_odd):
    even = lax.axis_index("lat_2") == 0
    here = lax.rem(lax.axis_index("lon"), 2) == 0
    for f in range(2):
        for g in range(2):

            def pick(k, f=f, g=g):
                at = f * LEVELS * ROWS + g * 8 + k
                return flow[pl.ds(at, 8, stride=ROWS), :], flow[pl.ds(at + 8 * ROWS, 8, stride=ROWS), :]

            at = (f * 2 + g) * 8
            to_right, to_left = packed_edges(pick, 8), packed_edges(pick, 0)
            to_even[at : at + 8, :] = jnp.where(here, to_right, to_left)
            to_odd[at : at + 8, :] = jnp.where(here, to_left, to_right)
        for i in range(HALO):
            for h in range(2):
                at = f * LEVELS * ROWS + h * 8 * ROWS + i
                up, down = flow[pl.ds(at + ROWS - HALO, 8, stride=ROWS), :], flow[pl.ds(at, 8, stride=ROWS), :]
                at = (i * 2 + f) * LEVELS + h * 8
                to_core[at : at + 8, :] = jnp.where(even, up, down)
                to_inter[at : at + 8, :] = jnp.where(even, down, up)


def backwards(x):
    return jnp.concatenate([x[i : i + 1] for i in reversed(range(x.shape[0]))], axis=0)


def strip_of(low, high, left, right, k):
    ln = lanes(8)
    a = jnp.where(ln < 8, roll(left, -16 * k), jnp.where(ln < 32, roll(low, 8), jnp.where(ln < 56, roll(low, 56), roll(right, 56 - 16 * k))))
    b = jnp.where(ln < 72, roll(left, 56 - 16 * k), jnp.where(ln < 96, roll(high, 72), jnp.where(ln < 120, roll(high, 120), roll(right, 112 - 16 * k))))
    return jnp.where(ln < HALF, a, b)


def widen(flow, core, inter, even_edges, odd_edges, wide, strips):
    even = lax.axis_index("lat_2") == 0
    wide[:EDGE, :] = jnp.where(even, inter[...], core[...])
    wide[EDGE + ROWS * 2 * LEVELS :, :] = jnp.where(even, core[...], inter[...])
    for f in range(2):
        for g in range(2):
            left, right = left_and_right(even_edges, odd_edges, f, g)
            for k in range(8):
                at = f * LEVELS * ROWS + g * 8 + k
                low, high = flow[pl.ds(at, 8, stride=ROWS), :], flow[pl.ds(at + 8 * ROWS, 8, stride=ROWS), :]
                at = EDGE + ((g * 8 + k) * 2 + f) * LEVELS
                wide[at : at + 8, :] = low
                wide[at + 8 : at + 16, :] = high
                at = ((g * 8 + k) * 2 + f) * 8
                strips[at : at + 8, :] = strip_of(low, high, left, right, k)


def left_and_right(even_edges, odd_edges, f, g):
    here = lax.rem(lax.axis_index("lon"), 2) == 0
    at = (f * 2 + g) * 8
    first, second = even_edges[at : at + 8, :], odd_edges[at : at + 8, :]
    return jnp.where(here, second, first), jnp.where(here, first, second)


def arrange(parcels, even_edges, odd_edges, to_core, to_inter):
    ln = lanes(8)
    even = lax.axis_index("lat_2") == 0
    for f in range(2):
        lower, upper = (left_and_right(even_edges, odd_edges, f, g) for g in range(2))
        for side in range(2):
            at = (f * 2 + side) * 8
            to_core[at : at + 8, :] = jnp.where(even, upper[side], lower[side])
            to_inter[at : at + 8, :] = jnp.where(even, lower[side], upper[side])
    edge = backwards(parcels[pl.ds(BULK + 2, LON, stride=PARCEL), :])
    named = parcels[pl.ds(BULK + 3, LON, stride=PARCEL), :]
    turned, turned_back = jnp.transpose(named), jnp.transpose(backwards(named))
    spot = jnp.full((1, LANES), NOWHERE, F32)
    line = lanes(1)
    for i, k in enumerate((2, 3, 0, 1, 4, 5)):
        rows = turned if k in (2, 3) else turned_back
        line_k = jnp.concatenate([rows[k : k + 1, :], jnp.zeros((1, LANES - LON), F32)], axis=1)
        spot = jnp.where((line >= 8 * i) & (line < 8 * i + 8), roll(line_k, 8 * i), spot)
    for o in range(SLOT):
        own = parcels[pl.ds(BULK + o, LON, stride=PARCEL), :]
        left = jnp.where(ln < 8, roll(edge, -8 * o), 0.0)
        right = jnp.where((ln >= 56) & (ln < 64), roll(edge, 40 - 8 * o), 0.0)
        for out in (to_core, to_inter):
            out[RAW + o * LON : RAW + (o + 1) * LON, :] = own
            out[LEFTS + o * LON : LEFTS + (o + 1) * LON, :] = left
            out[RIGHTS + o * LON : RIGHTS + (o + 1) * LON, :] = right
    for out in (to_core, to_inter):
        out[SPOTS:, :] = jnp.broadcast_to(spot, (8, LANES))


def unpack(parcels, grams):
    ln, rw = lanes(HALF), places(HALF)
    upper, diagonal, first = ln - HALF > rw, ln - HALF == rw, ln < HALF
    for s in range(LON):
        both = parcels[s * PARCEL : s * PARCEL + 2 * HALF, :]
        turned = jnp.transpose(both)
        ct, et = turned[:HALF], turned[HALF:]
        ct_rolled, et_rolled = roll(ct, HALF), roll(et, HALF)
        for o in range(SLOT):
            q = both[o * HALF : (o + 1) * HALF]
            d = parcels[s * PARCEL + 2 * HALF + o : s * PARCEL + 2 * HALF + o + 1, :]
            e_first, e_last = (et, et_rolled) if o == 0 else (et_rolled, et)
            c_last = ct_rolled if o == 0 else ct
            top = jnp.where(first, jnp.where(ln <= rw, roll(q, HALF), e_first), c_last)
            low = jnp.where(first | upper, q, jnp.where(diagonal, d, e_last))
            at = (o * LON + s) * LANES
            grams[at : at + HALF, :] = top
            grams[at + HALF : at + LANES, :] = low


def split(x):
    high = x.astype(jnp.bfloat16)
    rest = x - high.astype(F32)
    middle = rest.astype(jnp.bfloat16)
    low = (rest - middle.astype(F32)).astype(jnp.bfloat16)
    return jnp.concatenate([high, middle, low], axis=1)


def chosen(one_hot, parts):
    out = jnp.dot(one_hot, parts, preferred_element_type=F32)
    return out[:, :LANES] + out[:, LANES : 2 * LANES] + out[:, 2 * LANES :]


def one_hot(index, at):
    return jnp.where(index == at, 1.0, 0.0).astype(jnp.bfloat16)


def padded(x, rows):
    return jnp.concatenate([x, jnp.zeros((rows - x.shape[0], LANES), F32)], axis=0)


def lay_out(spots, by_lane, own, sides, field, strips, low, high):
    ln = lanes(NEAR)
    first, last = (ln & (HALF - 1)) < 32, (ln & (HALF - 1)) < 56
    inner = (ln & (HALF - 1)) >= 8
    rows = own[:NEAR]
    own_upper = (spots[:NEAR, :].astype(jnp.int32) & 8) != 0
    near_left = jnp.where(own_upper, roll(rows, 72), roll(rows, 8))
    near_right = jnp.where(own_upper, roll(rows, 120), roll(rows, 56))
    own_strip = jnp.where((ln >= HALF) == own_upper, jnp.where(first, jnp.where(inner, near_left, 0.0), jnp.where(last, near_right, 0.0)), 0.0)
    edge = sides[: 2 * NEAR]
    side_upper = (spots[LANES : LANES + 2 * NEAR, :].astype(jnp.int32) & 8) != 0
    side_strip = jnp.where(side_upper, roll(edge, HALF), edge)
    pieces = [split(padded(own_strip, LANES)), split(padded(side_strip, LANES))]
    own_parts = split(own)
    lane_spots = [by_lane[i * 8 : i * 8 + 1, :].astype(jnp.int32) for i in range(2)]
    p = jnp.broadcast_to(lane_spots[0], (LANES, LANES))
    for start in range(low * LEVELS, high * LEVELS, LANES):
        field[start : start + LANES, :] = chosen(one_hot(places(LANES) + start, p), own_parts)
    folded = [jnp.broadcast_to(((b >> 4) << 3) + (b & 7), (64, LANES)) for b in lane_spots]
    for start in range(low * 8, high * 8, 64):
        at = places(64) + start
        strips[start : start + 64, :] = chosen(one_hot(at, folded[0]), pieces[0]) + chosen(one_hot(at, folded[1]), pieces[1])


def adjoint(rates, source, target, first, last, height):
    before = kept = None
    for r in range(first, last + 1):
        y = source[r * height : (r + 1) * height, :]
        lat, lon = rates(r)
        t = lat * y
        a = jnp.where(lat > 0.0, t, 0.0)
        b = a - t
        s = lon * y
        e = jnp.where(lon > 0.0, s, 0.0)
        f = e - s
        if r > first + 1:
            target[(r - 1) * height : r * height, :] = kept + a
        if r > first:
            kept = y - (a + b) - (e + f) + roll(e, -1) + roll(f, 1) + before
        before = b


def tangent(rates, source, target, first, last, height):
    for r in range(first + 1, last):
        x = source[r * height : (r + 1) * height, :]
        south = source[(r - 1) * height : r * height, :]
        north = source[(r + 1) * height : (r + 2) * height, :]
        lat, lon = rates(r)
        out = x + jnp.abs(lat) * (jnp.where(lat > 0.0, south, north) - x)
        target[r * height : (r + 1) * height, :] = out + jnp.abs(lon) * (jnp.where(lon > 0.0, roll(x, 1), roll(x, -1)) - x)


def merged(field, strips, r):
    ln = lanes(8)
    t = strips[r * 8 : (r + 1) * 8, :]
    low, high = field[r * LEVELS : r * LEVELS + 8, :], field[r * LEVELS + 8 : (r + 1) * LEVELS, :]
    low = jnp.where(ln < 8, roll(t, -8), jnp.where(ln >= 120, roll(t, 72), low))
    high = jnp.where(ln < 8, roll(t, -72), jnp.where(ln >= 120, roll(t, 8), high))
    return low, high


def steps_back(rates, fields, strips, first):
    full, narrow = rates
    for k in range(first, first + STEPS):
        adjoint(full, *fields, k, WIDE - 1 - k, LEVELS)
        adjoint(narrow, *strips, k, WIDE - 1 - k, 8)
        fields, strips = fields[::-1], strips[::-1]
    return fields, strips


def steps_on(rates, fields, strips, first):
    full, narrow = rates
    for k in range(first, first + STEPS):
        tangent(full, *fields, k, WIDE - 1 - k, LEVELS)
        tangent(narrow, *strips, k, WIDE - 1 - k, 8)
        fields, strips = fields[::-1], strips[::-1]
    return fields, strips


def rates_of(wide, mine, beside):
    def full(r):
        at = r * 2 * LEVELS
        return wide[at : at + LEVELS, :], wide[at + LEVELS : at + 2 * LEVELS, :]

    def narrow(r):
        ref, r = (mine, r - HALO) if HALO <= r < HALO + ROWS else (beside, r if r < HALO else r - ROWS)
        return ref[r * 16 : r * 16 + 8, :], ref[r * 16 + 8 : r * 16 + 16, :]

    return full, narrow


def back_and_on(spots, by_lane, own, sides, rates, kept, fields, strips, image):
    lay_out(spots, by_lane, own, sides, fields[0], strips[0], 0, WIDE)
    fields, strips = steps_back(rates, fields, strips, 0)
    lat, last = lax.axis_index(LAT), lax.axis_size(LAT) - 1
    for outside, start in ((lat == 0, STEPS), (lat == last, HALO + ROWS)):
        for ref, height in ((fields[0], LEVELS), (strips[0], 8)):
            block = ref[start * height : (start + STEPS) * height, :]
            ref[start * height : (start + STEPS) * height, :] = jnp.where(outside, 0.0, block)
    square = jnp.zeros((8, LANES), F32)
    for r in range(ROWS):
        low, high = merged(fields[0], strips[0], r + HALO)
        kept[r * LEVELS : r * LEVELS + 8, :] = low
        kept[r * LEVELS + 8 : (r + 1) * LEVELS, :] = high
        square += low * low + high * high
    fields, strips = steps_on(rates, fields, strips, STEPS)
    for r in range(ROWS):
        low, high = merged(fields[0], strips[0], r + HALO)
        image[r * LEVELS : r * LEVELS + 8, :] = low
        image[r * LEVELS + 8 : (r + 1) * LEVELS, :] = high
    mine = spots[OWN : 2 * OWN, :].astype(jnp.int32) - HALO * LEVELS
    hit = jnp.concatenate([one_hot(lanes(OWN), mine), one_hot(lanes(OWN) + LANES, mine)], axis=1)
    return jnp.sum(square, keepdims=True), chosen(hit, split(image[...]))


def weigh(seen, grams):
    column = jnp.transpose(seen)
    out = []
    for t in range(OWN):
        total = jnp.zeros((8, LANES), F32)
        for k in range(LANES // 8):
            at = t * LANES + k * 8
            total += grams[at : at + 8, :] * column[k * 8 : k * 8 + 8, t : t + 1]
        out.append(jnp.sum(total, axis=0, keepdims=True))
    return jnp.concatenate(out, axis=0)


def in_lanes(first, values):
    ln = lanes(8)
    out = jnp.zeros((8, LANES), F32)
    for i, v in enumerate(values):
        out = jnp.where(ln == first + i, v, out)
    return out


def first_half(wide, mine, core, own_message, inter, beside, spots, by_lane, kept, seen, sums, field, other, strip, other_strip, image):
    ln = lanes(8)
    even = lax.axis_index("lat_2") == 0
    for n in range(2):
        edges = jnp.where(even == (n == 0), inter[:RAW, :], core[:RAW, :])
        for f in range(2):
            left, right = edges[f * 16 : f * 16 + 8], edges[f * 16 + 8 : f * 16 + 16]
            for k in range(HALO):
                at = ((n * (HALO + ROWS) + k) * 2 + f) * LEVELS
                low, high = wide[at : at + 8, :], wide[at + 8 : at + 16, :]
                at = n * STRIP + (k * 2 + f) * 8
                beside[at : at + 8, :] = strip_of(low, high, left, right, k)
    step = jnp.where(even, float(ROWS * LEVELS), -float(ROWS * LEVELS))
    c, o, i = core[SPOTS:, :] + step, own_message[SPOTS:, :], inter[SPOTS:, :] - step
    tables = (((c, 0), (o, 0), (i, 0)), ((c, 16), (o, 16), (i, 16), (c, 32), (o, 32), (i, 32)))
    for t, table in enumerate(tables):
        spot = jnp.full((8, LANES), NOWHERE, F32)
        for n, (x, at) in enumerate(table):
            spot = jnp.where((ln >= OWN * n) & (ln < OWN * (n + 1)), roll(x, OWN * n - at), spot)
        by_lane[t * 8 : t * 8 + 8, :] = spot
        spots[t * LANES : (t + 1) * LANES, :] = jnp.transpose(jnp.broadcast_to(spot[:1], (LANES, LANES)))
    parts = (core, own_message, inter)
    own = padded(jnp.concatenate([x[RAW:LEFTS, :] for x in parts], axis=0), LANES)
    sides = padded(jnp.concatenate([x[LEFTS:RIGHTS, :] for x in parts] + [x[RIGHTS:SPOTS, :] for x in parts], axis=0), LANES)
    square, rows = back_and_on(spots, by_lane, own, sides, rates_of(wide, mine, beside), kept, (field, other), (strip, other_strip), image)
    seen[...] = rows
    sums[...] = in_lanes(0, [square])


def fanned(x, shift):
    return pltpu.roll(x, shift % LANES, axis=1, stride=8, stride_axis=0)


def herald(rows, message):
    mine = (lanes(OWN) >> 3) == places(OWN)
    message[:OWN, :] = rows
    for at, shift in ((OWN, 0), (OWN + 1, 8)):
        spread = jnp.concatenate([fanned(rows[:8], shift), fanned(rows[8:], shift + HALF)], axis=0)
        message[at : at + 1, :] = jnp.sum(jnp.where(mine, spread, 0.0), axis=0, keepdims=True)
    message[OWN + 2 :, :] = jnp.zeros((HERALD - OWN - 2, LANES), F32)


def first_terms(grams, seen, before, message, sums):
    rows = weigh(seen[...], grams)
    herald(rows, message)
    sums[...] = before[...] + in_lanes(1, [jnp.sum(seen[...] * rows, keepdims=True)])


def edges_of(core, mine, inter, out):
    for i, x in enumerate((core, mine, inter)):
        out[i : i + 1, :] = x[OWN : OWN + 1, :]
        out[i + 3 : i + 4, :] = x[OWN + 1 : OWN + 2, :]
    out[6:, :] = jnp.zeros((2, LANES), F32)


def side_strips(lefts, rights):
    ln = lanes(OWN)

    def rows(x, shift):
        x = jnp.broadcast_to(x, (8, LANES))
        return jnp.concatenate([fanned(x, shift - 56), fanned(x, shift - 120)], axis=0)

    out = [jnp.where(ln < 8, rows(x, 0), 0.0) for x in lefts]
    out += [jnp.where((ln >= 56) & (ln < 64), rows(x, 56), 0.0) for x in rights]
    return padded(jnp.concatenate(out, axis=0), LANES)


def second_half(spots, by_lane, core, mine, inter, even, odd, wide, strips, beside, grams, before, kept, message, out, field, other, strip, other_strip, image):
    own = padded(jnp.concatenate([x[:OWN, :] for x in (core, mine, inter)], axis=0), LANES)
    here = lax.rem(lax.axis_index("lon"), 2) == 0
    left, right = jnp.where(here, odd[...], even[...]), jnp.where(here, even[...], odd[...])
    sides = side_strips([left[i : i + 1] for i in (3, 4, 5)], [right[i : i + 1] for i in (0, 1, 2)])
    square, seen = back_and_on(
        spots, by_lane, own, sides, rates_of(wide, strips, beside), kept, (field, other), (strip, other_strip), image
    )
    rows = weigh(seen, grams)
    herald(rows, message)
    sums = before[...] + in_lanes(2, [square, jnp.sum(seen * rows, keepdims=True)])
    out[...] = jnp.concatenate([sums] * (out.shape[0] // 8), axis=0)
    for step, row in ((1, OWN + 1), (-1, OWN)):
        out[pl.ds(in_plane(step) * 2 + 1, 1), :] = message[row : row + 1, :]


def in_plane(step):
    size = lax.axis_size(("lat_1", "lon"))
    at = lax.axis_index("lat_1") * LON + lax.rem(lax.axis_index("lon") + LON + step, LON)
    return lax.rem(at + size - middle_of_plane(), size)


def middle_of_plane():
    return lax.axis_size("lat_1") // 2 * LON + LON // 2


def gathered(parts, mine, sums, message):
    count = parts.shape[0] // 2
    sums[...] = jnp.broadcast_to(jnp.sum(parts[pl.ds(0, count, stride=2), :], axis=0, keepdims=True), sums.shape)
    message[...] = mine[...]
    for i, step in enumerate((-1, 1)):
        message[OWN + i : OWN + i + 1, :] = parts[pl.ds(in_plane(step) * 2 + 1, 1), :]


def finish(spots, by_lane, core, mine, inter, wide, strips, beside, parts, right_side, image, increment, residual, field, other, strip, other_strip):
    lists = (core, mine, inter)
    own = padded(jnp.concatenate([x[:OWN, :] for x in lists], axis=0), LANES)
    sides = side_strips(*([x[OWN + i : OWN + i + 1, :] for x in lists] for i in range(2)))
    lay_out(spots, by_lane, own, sides, field, strip, HALO - STEPS, HALO + ROWS + STEPS)
    fields, narrow = steps_back(rates_of(wide, strips, beside), (field, other), (strip, other_strip), STEPS)
    total = jnp.sum(parts[...], axis=0, keepdims=True)
    m0, m1, m2, m3 = (jnp.sum(jnp.where(lanes(1) == i, total, 0.0), keepdims=True) for i in range(4))
    step_0 = m0 / (m0 + m1)
    rho = m1 / m0
    spread = m2 - rho * m1
    curve = (m3 - rho * m2) - rho * (m2 - rho * m1)
    gamma = step_0 * spread / m0
    step_1 = spread / (spread + curve - gamma * spread)
    on_b = step_0 * (1.0 + step_1 * (gamma + rho))
    on_k = -step_0 * step_1
    rest_b = step_0 * ((1.0 - step_1) * rho - step_1 * gamma)
    rest_k = -step_0 * ((1.0 - step_1) + step_1 * (rho + gamma))
    rest_kk = step_0 * step_1
    on_b, on_k, rest_b, rest_k, rest_kk = (jnp.broadcast_to(v, (8, LANES)) for v in (on_b, on_k, rest_b, rest_k, rest_kk))
    for r in range(ROWS):
        for h, second in enumerate(merged(fields[0], narrow[0], r + HALO)):
            at = r * LEVELS + h * 8
            b, first = right_side[at : at + 8, :], image[at : at + 8, :]
            to = pl.ds(h * 8 * ROWS + r, 8, stride=ROWS)
            increment[to, :] = on_b * b + on_k * first
            residual[to, :] = rest_b * b + rest_k * first + rest_kk * second


def to_core(x):
    return lax.ppermute(x, LAT, [(i, i ^ 1) for i in range(lax.axis_size(LAT))])


def to_inter(x):
    return lax.ppermute(x, LAT, [(i, ((i + 1) ^ 1) - 1) for i in range(1, lax.axis_size(LAT) - 1)])


def to_even(x):
    return lax.ppermute(x, "lon", [(i, i ^ 1) for i in range(LON)])


def to_odd(x):
    return lax.ppermute(x, "lon", [(i, (((i + 1) % LON ^ 1) - 1) % LON) for i in range(LON)])


def spread_out(x, axes, first):
    count = lax.axis_size(axes)
    group = [(i + first) % count for i in range(count)]
    return lax.all_to_all(x, axes, split_axis=0, concat_axis=0, tiled=True, axis_index_groups=[group])


def shards(courant, obs_matrix, obs_weight, innovation, block_owner, block_row, block_count):
    flow = courant.reshape(-1, LANES)
    owner, row, count = block_owner.reshape(-1), block_row.reshape(-1), block_count
    wholes = (obs_matrix[0], obs_weight[0], innovation[0])
    (parcels,) = call(
        prepare,
        [(LON * PARCEL, LANES)],
        (owner, row, count, *wholes),
        4_000_000,
        [pltpu.SMEM((CAP,), jnp.int32), pltpu.SMEM((CAP,), jnp.int32), pltpu.SMEM((1, 1), jnp.int32)]
        + [pltpu.VMEM(x.shape, F32) for x in wholes]
        + [pltpu.VMEM((OWN, LANES), F32), pltpu.SemaphoreType.DMA((6,))],
        [pl.BlockSpec(memory_space=pltpu.HBM)] * 6,
        62,
    )
    parcels = spread_out(parcels.reshape(LON, PARCEL, LANES), "lon", FIRST).reshape(LON * PARCEL, LANES)
    edge = (EDGE, LANES), (2 * OWN, LANES)
    for_core, for_inter, for_even, for_odd = call(halo, [edge[0], edge[0], edge[1], edge[1]], (flow,), 1_000_000)
    odd = to_odd(for_odd)
    even = to_even(for_even)
    inter = to_inter(for_inter)
    core = to_core(for_core)
    wide, strips = call(
        widen, [(WIDE * 2 * LEVELS, LANES), (2 * STRIP, LANES)], (flow, core, inter, even, odd), 4_000_000
    )
    for_core, for_inter = call(arrange, [(MESSAGE, LANES)] * 2, (parcels, even, odd), 1_000_000)
    core, inter = to_core(for_core), to_inter(for_inter)
    (grams,) = call(unpack, [(OWN * LANES, LANES)], (parcels,), 4_000_000)
    cells, listed = (ROWS * LEVELS, LANES), (OWN, LANES)
    work = [pltpu.VMEM((WIDE * LEVELS, LANES), F32)] * 2 + [pltpu.VMEM((WIDE * 8, LANES), F32)] * 2
    work_too = work + [pltpu.VMEM(cells, F32)]
    beside, spots, by_lane, right_side, seen, sums = call(
        first_half,
        [(2 * STRIP, LANES), (2 * LANES, LANES), (16, LANES), cells, listed, (8, LANES)],
        (wide, strips, core, for_core, inter),
        4_000_000,
        work_too,
    )
    rates = (wide, strips, beside)
    short = (HERALD, LANES)
    mine, sums = call(first_terms, [short, (8, LANES)], (grams, seen, sums), 2_000_000)
    core, inter = to_core(mine), to_inter(mine)
    (edges,) = call(edges_of, [(8, LANES)], (core, mine, inter), 10_000)
    lists = (core, mine, inter, to_even(edges), to_odd(edges))
    plane, towers = lax.axis_size(("lat_1", "lon")), lax.axis_size(("lat_0", "lat_2"))
    image, mine, parcels = call(
        second_half, [cells, short, (plane * 2, LANES)], (spots, by_lane, *lists, *rates, grams, sums), 4_000_000, work_too
    )
    parcels = spread_out(parcels.reshape(plane, 2, LANES), ("lat_1", "lon"), middle_of_plane()).reshape(plane * 2, LANES)
    sums, mine = call(gathered, [(towers, LANES), short], (parcels, mine), 10_000)
    core, inter = to_core(mine), to_inter(mine)
    parts = spread_out(sums.reshape(towers, 1, LANES), ("lat_0", "lat_2"), towers * 12 // 16 + 1).reshape(towers, LANES)
    increment, residual = call(
        finish, [cells, cells], (spots, by_lane, core, mine, inter, *rates, parts, right_side, image), 2_000_000, work
    )
    shape = courant.shape[1:]
    return increment.reshape(shape), residual.reshape(shape)


def solution(mesh):
    torus = Mesh(
        mesh.devices.reshape(-1, 4, 2, mesh.shape["lon"]), ("lat_0", "lat_1", "lat_2", "lon")
    )
    placed = (
        P(None, None, LAT, "lon"),
        P(LAT, "lon", None, None),
        P(LAT, "lon", None),
        P(LAT, "lon", None),
        P(LAT, "lon", None),
        P(LAT, "lon"),
        P(LAT, "lon"),
    )
    return jax.shard_map(
        shards,
        mesh=torus,
        in_specs=placed,
        out_specs=(P(None, LAT, "lon"), P(None, LAT, "lon")),
        check_vma=False,
    )
```
